32 devices in a mesh: gx: 2 (over core), gy: 4 (over y, x), gz: 4 (over z).
Axes of the slice: x: 2, y: 2, z: 4, core: 2. Of those that a mesh axis runs over, the one named last changes fastest.
Arguments:
- raw_weight: float32 [128, 27, 128], P(('gx', 'gy')), may hold values from -6 to 6
- inputs: bfloat16 [16, 64, 64, 128], P('gx', 'gy', 'gz'), may hold values from -6 to 6
- cotangent: bfloat16 [16, 64, 64, 128], P('gx', 'gy', 'gz'), may hold values from -0.099609375 to 0.099609375
Outputs:
- input_grad: bfloat16 [16, 64, 64, 128], P('gx', 'gy', 'gz')
- weight_grad: float32 [128, 27, 128], P(('gx', 'gy'))
The draws below stay inside these ranges and needn't reach their ends.
All inputs are finite; a program needn't handle non-finite values.
Results may differ from the reference program's by a relative error of at most 0.0049.
Values may be sent and summed in bfloat16 or wider, within the bound.
A program may use at most 64 MiB of HBM per device.

```python
import math
import jax
import jax.numpy as jnp
from jax import lax

C = 128
KK = 27
NX = 16
NY = 64
NZ = 64


def draw_raw_weight(key, part):
    sub_keys = jax.random.split(key, 4)
    row_scale = jnp.exp(jax.random.uniform(sub_keys[0], (C, 1, 1), jnp.float32, math.log(0.1), 0.0))
    col_scale = jnp.exp(jax.random.uniform(sub_keys[1], (1, 1, C), jnp.float32, math.log(0.1), 0.0))
    col_mean = jax.random.uniform(sub_keys[2], (1, 1, C), jnp.float32, -0.5, 0.5)
    base_draw = jnp.clip(jax.random.normal(sub_keys[3], (C, KK, C), jnp.float32), -4.0, 4.0)
    return jnp.clip((base_draw * row_scale + col_mean) * col_scale, -6.0, 6.0)


def steps_of(rng, shape, cuts, smallest, top_value):
    def one(dim, parts):
        steps = jax.random.uniform(jax.random.fold_in(jax.random.fold_in(rng, 6), dim), (parts,), jnp.float32, smallest / len(cuts), top_value / len(cuts))
        return jnp.repeat(jnp.exp(steps), shape[dim] // parts).reshape((-1,) + (1,) * (len(shape) - dim - 1))

    level = one(*cuts[0])
    for cut in cuts[1:]:
        level = level * one(*cut)
    return level


def normal_values(rng, shape, scale, most, shards=(), dtype=jnp.bfloat16):
    array = jax.random.normal(rng, shape, jnp.float32) * scale
    if len(shards) > 0:
        array = steps_of(rng, shape, shards, -0.22, 0.18) * array
    return jnp.clip(array, min=-most, max=most).astype(dtype)


def setup_inputs(seed: int = 0) -> dict:
    key_of = jax.random.split(jax.random.key(seed), 4)
    raw_weight = draw_raw_weight(jax.random.fold_in(key_of[3], 71), 0)
    inputs = normal_values(key_of[1], (NX, NY, NZ, C), 1.0, 6.0, ((0, 2), (1, 4), (2, 4)))
    cotangent = normal_values(key_of[2], (NX, NY, NZ, C), 0.017, 0.099609375, ((0, 2), (1, 4), (2, 4)))
    return dict(raw_weight=raw_weight, inputs=inputs, cotangent=cotangent)


var_eps = 1e-05
norm_eps = 1e-06
clip_norm = 600.0

def tap_view(padded, tap_a, tap_b, tap_c, extent):
    view = padded[2 - tap_a:2 - tap_a + extent[0], 2 - tap_b:2 - tap_b + extent[1], 2 - tap_c:2 - tap_c + extent[2], :]
    return view.reshape(-1, view.shape[-1])

def reference(raw_weight, inputs, cotangent):
    extent = inputs.shape[:3]
    channels = inputs.shape[3]
    fan_count = raw_weight.shape[0] * raw_weight.shape[1]
    sum_first = lax.optimization_barrier(jnp.sum(raw_weight, axis=(0, 1)))
    sum_second = lax.optimization_barrier(jnp.sum(raw_weight * raw_weight, axis=(0, 1)))
    mean_out = sum_first / fan_count
    var_out = sum_second / fan_count - mean_out * mean_out
    inv_std = lax.rsqrt(var_out + var_eps)
    std_float = (raw_weight - mean_out) * inv_std
    std_half = lax.optimization_barrier(std_float.astype(jnp.bfloat16)).astype(jnp.float32)
    padded = jnp.pad(cotangent.astype(jnp.float32), ((1, 1), (1, 1), (1, 1), (0, 0)))
    flat_in = inputs.astype(jnp.float32).reshape(-1, channels)
    dx_total = jnp.zeros((flat_in.shape[0], channels), jnp.float32)
    pieces = []
    for tap_a in range(3):
        for tap_b in range(3):
            for tap_c in range(3):
                tap_index = tap_a * 9 + tap_b * 3 + tap_c
                view = tap_view(padded, tap_a, tap_b, tap_c, extent)
                dx_total = dx_total + jnp.dot(view, std_half[:, tap_index, :].T, precision=lax.Precision.HIGHEST)
                pieces.append(jnp.dot(flat_in.T, view, precision=lax.Precision.HIGHEST))
    input_grad = dx_total.reshape(extent[0], extent[1], extent[2], channels).astype(jnp.bfloat16)
    filter_grad = jnp.stack(pieces, axis=1)
    mean_grad = lax.optimization_barrier(jnp.sum(filter_grad, axis=(0, 1))) / fan_count
    mean_cross = lax.optimization_barrier(jnp.sum(filter_grad * std_float, axis=(0, 1))) / fan_count
    raw_grad = inv_std * (filter_grad - mean_grad - std_float * mean_cross)
    square_sum = jnp.sum(raw_grad * raw_grad)
    scale = jnp.minimum(1.0, clip_norm * lax.rsqrt(square_sum + norm_eps))
    return (input_grad, raw_grad * scale)
```

```python
import functools

import jax
import jax.numpy as jnp
from jax import lax
from jax.experimental import pallas as pl
from jax.experimental.pallas import tpu as pltpu
from jax.sharding import PartitionSpec as P

var_eps = 1e-05
norm_eps = 1e-06
clip_norm = 600.0
F32 = jnp.float32
BF16 = jnp.bfloat16
MESH = pl.DeviceIdType.MESH
AXES = ("gx", "gy", "gz")


def z_groups(taps, nz):
    chunk = taps // 3
    sizes = [-(-2 * chunk // nz), -(-chunk // nz)]
    return [(0, 0, 2 * chunk, sizes[0]), (sizes[0] * nz, 2 * chunk, chunk, sizes[1])]


def kernel(dims, raw_hbm, in_hbm, cot_hbm, dx_ref, full, std, coef_ref, *scratch):
    (raw_ref, in_ref, shifted, face_out, face_in, in_t, part, recv_x, send_y, recv_y, send_z, recv_z,
     std_all, w_cat, stats, stats_in, total_in, load_sem, halo_send, halo_recv, x_send, x_recv, y_send, y_recv,
     z_send, z_recv, g_send, g_recv, ay_send, ay_recv, ax_send, ax_recv, st_send, st_recv, t_send, t_recv) = scratch
    count = dict(zip(AXES, dims))
    nx, ny, nz = dims
    plane_peers = nx * ny - 1
    me = {axis: lax.axis_index(axis) for axis in AXES}
    taps, rows, chan = raw_ref.shape
    ex, ey, ez = in_ref.shape[:3]
    chunk = taps // 3
    groups = z_groups(taps, nz)
    fan_count = float(rows * nx * ny * taps)

    def peer(axis, k):
        return lax.rem(me[axis] + k, count[axis])

    def plane_peer(k):
        flat = lax.rem(me["gx"] * ny + me["gy"] + k, nx * ny)
        return {"gx": lax.div(flat, ny), "gy": lax.rem(flat, ny)}

    def remote(src, dst, send_sem, recv_sem, where):
        return pltpu.make_async_remote_copy(
            src_ref=src, dst_ref=dst, send_sem=send_sem, recv_sem=recv_sem,
            device_id=where, device_id_type=MESH,
        )

    def wait_all(copies):
        for copy in copies:
            copy.wait()

    body = pl.ds(1, ey)
    load_raw = pltpu.make_async_copy(raw_hbm, raw_ref, load_sem.at[0])
    load_cot = pltpu.make_async_copy(cot_hbm, shifted.at[1, pl.ds(1, ex), body], load_sem.at[1])
    load_in = pltpu.make_async_copy(in_hbm, in_ref, load_sem.at[2])
    load_raw.start()
    load_cot.start()
    load_in.start()

    barrier = pltpu.get_barrier_semaphore()
    for k in range(1, nx * ny):
        pl.semaphore_signal(barrier, inc=1, device_id=plane_peer(k), device_id_type=MESH)
    for k in range(1, nz):
        pl.semaphore_signal(barrier, inc=1, device_id={"gz": peer("gz", k)}, device_id_type=MESH)

    def exchange_start(slot, base, peers):
        copies = []
        for k, where in enumerate(peers):
            copy = remote(stats.at[slot], stats_in.at[base + k], st_send.at[base + k], st_recv.at[base + k], where)
            copy.start()
            copies.append(copy)
        return copies

    def exchange_sum(slot, base, copies):
        wait_all(copies)
        total = stats[slot]
        for k in range(len(copies)):
            total = total + stats_in[base + k]
        return total

    zero_plane = jnp.zeros((ey + 2, ez, chan), BF16)
    zero_col = jnp.zeros((ex + 2, ez, chan), BF16)
    zero_face = jnp.zeros((ex + 2, ey + 2, chan), BF16)

    @pl.when(me["gx"] == 0)
    def _():
        shifted[1, 0] = zero_plane

    @pl.when(me["gx"] == nx - 1)
    def _():
        shifted[1, ex + 1] = zero_plane

    @pl.when(me["gy"] == 0)
    def _():
        shifted[1, :, 0] = zero_col

    @pl.when(me["gy"] == ny - 1)
    def _():
        shifted[1, :, ey + 1] = zero_col

    @pl.when(me["gz"] == 0)
    def _():
        face_in[0] = zero_face

    @pl.when(me["gz"] == nz - 1)
    def _():
        face_in[1] = zero_face

    for t in [b + v for b, first, many, size in groups for v in range(many, size * nz)]:
        send_z[t] = jnp.zeros((rows, chan), BF16)
        std[t] = jnp.zeros((rows, chan), F32)

    load_raw.wait()

    def per_output(value):
        return jnp.sum(jnp.sum(value, axis=0), axis=0, keepdims=True)

    raw = raw_ref[...]
    stats[0] = jnp.concatenate([per_output(raw), per_output(raw * raw), jnp.zeros((6, chan), F32)], axis=0)
    pl.semaphore_wait(barrier, plane_peers + nz - 1)
    weight_sums = exchange_start(0, 0, [plane_peer(k) for k in range(1, nx * ny)])
    load_cot.wait()

    def halo(axis, number, low_src, high_dst, high_src, low_dst):
        lower, upper = lax.max(me[axis] - 1, 0), lax.min(me[axis] + 1, count[axis] - 1)
        down = remote(low_src, high_dst, halo_send.at[2 * number], halo_recv.at[2 * number], {axis: lower})
        up = remote(high_src, low_dst, halo_send.at[2 * number + 1], halo_recv.at[2 * number + 1], {axis: upper})

        @pl.when(me[axis] > 0)
        def _():
            down.start()

        @pl.when(me[axis] < count[axis] - 1)
        def _():
            up.start()

        def finish():
            @pl.when(me[axis] > 0)
            def _():
                down.wait_send()
                up.wait_recv()

            @pl.when(me[axis] < count[axis] - 1)
            def _():
                up.wait_send()
                down.wait_recv()

        return finish

    def inside(dx, dy):
        gx, gy = me["gx"] + dx, me["gy"] + dy
        within = jnp.logical_and(gx >= 0, gx < nx)
        return jnp.logical_and(within, jnp.logical_and(gy >= 0, gy < ny))

    plane_halo = []
    for dx, dy in [(0, -1), (0, 1), (-1, 0), (1, 0), (-1, -1), (-1, 1), (1, -1), (1, 1)]:
        src_x = {-1: 1, 0: pl.ds(1, ex), 1: ex}[dx]
        dst_x = {-1: ex + 1, 0: pl.ds(1, ex), 1: 0}[dx]
        src_y = {-1: 1, 0: body, 1: ey}[dy]
        dst_y = {-1: ey + 1, 0: body, 1: 0}[dy]
        where = {
            "gx": lax.min(lax.max(me["gx"] + dx, 0), nx - 1),
            "gy": lax.min(lax.max(me["gy"] + dy, 0), ny - 1),
        }
        number = 2 + len(plane_halo)
        copy = remote(shifted.at[1, src_x, src_y], shifted.at[1, dst_x, dst_y],
                      halo_send.at[number], halo_recv.at[number], where)
        pl.when(inside(dx, dy))(copy.start)
        plane_halo.append((dx, dy, copy))
    load_in.wait()
    for x in range(ex):
        in_t[:, x * ey * ez:(x + 1) * ey * ez] = in_ref[x].reshape(ey * ez, chan).T
    for dx, dy, copy in plane_halo:
        pl.when(inside(dx, dy))(copy.wait_send)
        pl.when(inside(-dx, -dy))(copy.wait_recv)
    for x in range(ex + 2):
        plane = shifted[1, x].astype(F32)
        face_out[0, x] = plane[:, 0, :].astype(BF16)
        face_out[1, x] = plane[:, ez - 1, :].astype(BF16)
    halo_z = halo("gz", 0, face_out.at[0], face_in.at[1], face_out.at[1], face_in.at[0])

    sums = exchange_sum(0, 0, weight_sums)
    mean_out = sums[0:1] / fan_count
    var_out = sums[1:2] / fan_count - mean_out * mean_out
    inv_std = lax.rsqrt(var_out + var_eps)
    order = [t for c in (1, 0, 2) for t in range(c, taps, 3)]
    slots = [b + v for b, first, many, size in groups for v in range(many)]
    own = std_all.at[me["gx"], me["gy"]]
    for u, t in enumerate(order):
        value = (raw_ref[t] - mean_out) * inv_std
        std[slots[u]] = value
        own[u] = value.astype(BF16)
    gather_y = []
    for k in range(1, ny):
        copy = remote(own, own, ay_send.at[k - 1], ay_recv.at[k - 1], {"gy": peer("gy", k)})
        copy.start()
        gather_y.append(copy)

    def view(t, start, planes):
        a, b, c = t // 9, (t // 3) % 3, t % 3
        block = shifted[2 - c, pl.ds(start + 2 - a, planes), 2 - b:2 - b + ey]
        return block.reshape(planes * ey * ez, chan)

    def filter_chunk(n):
        for u in range(n * chunk, (n + 1) * chunk, 2):
            group = list(range(u, min(u + 2, (n + 1) * chunk)))
            views = [view(order[v], 0, ex) for v in group]
            right = jnp.concatenate(views, axis=1) if len(views) > 1 else views[0]
            product = jnp.dot(in_t[...], right, preferred_element_type=F32)
            for j, v in enumerate(group):
                for gx in range(nx):
                    for gy in range(ny):
                        low = (gx * ny + gy) * rows
                        part[gx, gy, v] = product[low:low + rows, j * chan:(j + 1) * chan]
        copies = []
        span = pl.ds(n * chunk, chunk)
        for k in range(1, nx):
            index = n * (nx - 1) + k - 1
            copy = remote(part.at[peer("gx", k), :, span], recv_x.at[k - 1, :, span],
                          x_send.at[index], x_recv.at[index], {"gx": peer("gx", k)})
            copy.start()
            copies.append(copy)
        return copies

    def rows_chunk(n, copies):
        wait_all(copies)
        span = pl.ds(n * chunk, chunk)
        for gy in range(ny):
            total = part[me["gx"], gy, span]
            for k in range(1, nx):
                total = total + recv_x[k - 1, gy, span]
            send_y[gy, span] = total.astype(BF16)
        sent = []
        for k in range(1, ny):
            index = n * (ny - 1) + k - 1
            copy = remote(send_y.at[peer("gy", k), span], recv_y.at[k - 1, span],
                          y_send.at[index], y_recv.at[index], {"gy": peer("gy", k)})
            copy.start()
            sent.append(copy)
        return sent

    depth_index = lax.broadcasted_iota(jnp.int32, (ey + 2, ez, chan), 1)

    def shift(slot, side, amount, edge):
        for x in range(ex + 2):
            plane = shifted[1, x].astype(F32)
            outer = face_in[side, x].astype(F32)[:, None, :]
            shifted[slot, x] = jnp.where(depth_index == edge, outer, pltpu.roll(plane, amount, 1)).astype(BF16)

    copies_0 = filter_chunk(0)
    halo_z()
    shift(2, 1, ez - 1, ez - 1)
    copies_1 = filter_chunk(1)
    reduce_y = [rows_chunk(0, copies_0)]
    shift(0, 0, 1, 0)
    copies_2 = filter_chunk(2)
    reduce_y.append(rows_chunk(1, copies_1))
    reduce_y.append(rows_chunk(2, copies_2))
    wait_all(gather_y)
    gather_x = []
    for k in range(1, nx):
        copy = remote(std_all.at[me["gx"]], std_all.at[me["gx"]], ax_send.at[k - 1], ax_recv.at[k - 1],
                      {"gx": peer("gx", k)})
        copy.start()
        gather_x.append(copy)

    step = 2 if ex % 2 == 0 else 1

    def dx_step(n, carry):
        start = n * step
        left = jnp.concatenate([view(t, start, step) for t in order], axis=1)
        product = lax.dot_general(left, w_cat[...], (((1,), (1,)), ((), ())), preferred_element_type=F32)
        dx_ref[pl.ds(start, step)] = product.astype(BF16).reshape(step, ey, ez, chan)
        return carry

    steps = ex // step
    half = steps // 2

    def depth_start(g):
        base, first, many, size = groups[g]
        span = pl.ds(first, many)
        total = send_y[me["gy"], span].astype(F32)
        for k in range(1, ny):
            total = total + recv_y[k - 1, span].astype(F32)
        send_z[base:base + many] = total.astype(BF16)
        copies = []
        for k in range(1, nz):
            index = g * (nz - 1) + k - 1
            copy = remote(send_z.at[pl.ds(base + peer("gz", k) * size, size)],
                          recv_z.at[k - 1, pl.ds(base // nz, size)],
                          z_send.at[index], z_recv.at[index], {"gz": peer("gz", k)})
            copy.start()
            copies.append(copy)
        return copies

    def depth_sum(g, copies):
        wait_all(copies)
        base, first, many, size = groups[g]
        mine = pl.ds(base + me["gz"] * size, size)
        grad = send_z[mine].astype(F32)
        for k in range(1, nz):
            grad = grad + recv_z[k - 1, pl.ds(base // nz, size)].astype(F32)
        full[mine] = grad.astype(BF16)
        sums = [per_output(grad), per_output(grad * std[mine]), per_output(grad * grad)]
        return jnp.concatenate(sums + [jnp.zeros((5, chan), F32)], axis=0)

    def gather_start(g):
        base, first, many, size = groups[g]
        mine = pl.ds(base + me["gz"] * size, size)
        copies = []
        for k in range(1, nz):
            index = g * (nz - 1) + k - 1
            copy = remote(full.at[mine], full.at[mine], g_send.at[index], g_recv.at[index], {"gz": peer("gz", k)})
            copy.start()
            copies.append(copy)
        return copies

    wait_all(reduce_y[0] + reduce_y[1])
    reduce_0 = depth_start(0)
    wait_all(gather_x)
    for u in range(taps):
        w_cat[:, u * chan:(u + 1) * chan] = std_all[:, :, u].reshape(nx * ny * rows, chan)
    lax.fori_loop(0, half, dx_step, 0)
    wait_all(reduce_y[2])
    reduce_1 = depth_start(1)
    lax.fori_loop(half, steps, dx_step, 0)
    first_sums = depth_sum(0, reduce_0)
    gather_z = gather_start(0)
    stats[1] = first_sums + depth_sum(1, reduce_1)
    flat = (me["gx"] * ny + me["gy"]) * nz + me["gz"]
    total_in[flat] = stats[1]
    final_sums = []
    for k in range(1, nx * ny * nz):
        other = lax.rem(flat + k, nx * ny * nz)
        where = {
            "gx": lax.div(other, ny * nz),
            "gy": lax.rem(lax.div(other, nz), ny),
            "gz": lax.rem(other, nz),
        }
        copy = remote(stats.at[1], total_in.at[flat], t_send.at[k - 1], t_recv.at[k - 1], where)
        copy.start()
        final_sums.append(copy)
    gather_z += gather_start(1)
    wait_all(final_sums)
    sums = total_in[0]
    for k in range(1, nx * ny * nz):
        sums = sums + total_in[k]
    wait_all(gather_z)
    sum_grad, sum_cross, sum_square = sums[0:1], sums[1:2], sums[2:3]
    mean_grad = sum_grad / fan_count
    mean_cross = sum_cross / fan_count
    spread = sum_square - 2.0 * mean_grad * sum_grad - 2.0 * mean_cross * sum_cross
    spread = (
        spread
        + fan_count * mean_grad * mean_grad
        + fan_count * mean_cross * mean_cross * var_out / (var_out + var_eps)
    )
    square_sum = jnp.sum(inv_std * inv_std * spread, axis=1, keepdims=True)
    scale = jnp.minimum(1.0, clip_norm * lax.rsqrt(square_sum + norm_eps))
    coef_ref[0:1] = inv_std * scale
    coef_ref[1:2] = mean_grad
    coef_ref[2:3] = mean_cross


def tap_slots(taps, nz):
    order = [t for c in (1, 0, 2) for t in range(c, taps, 3)]
    slots = [b + v for b, first, many, size in z_groups(taps, nz) for v in range(many)]
    return list(zip(order, slots))


def finish_kernel(nz, taps, dx_in, full, std, coef_ref, dx_hbm, wg_hbm, wg_ref, sem):
    out_dx = pltpu.make_async_copy(dx_in, dx_hbm, sem.at[0])
    out_dx.start()
    factor, mean_grad, mean_cross = coef_ref[0:1], coef_ref[1:2], coef_ref[2:3]
    for t, slot in tap_slots(taps, nz):
        wg_ref[t] = factor * (full[slot].astype(F32) - mean_grad - std[slot] * mean_cross)
    out_wg = pltpu.make_async_copy(wg_ref, wg_hbm, sem.at[1])
    out_wg.start()
    out_wg.wait()
    out_dx.wait()


def on_device(dims, raw_weight, inputs, cotangent):
    nx, ny, nz = dims
    rows, taps, chan = raw_weight.shape
    ex, ey, ez = inputs.shape[:3]
    groups = z_groups(taps, nz)
    piece = sum(size for base, first, many, size in groups)
    padded_taps = piece * nz
    stat_slots = nx * ny - 1
    dma = pltpu.SemaphoreType.DMA

    def pair(n):
        return [dma((max(n, 1),)), dma((max(n, 1),))]

    scratch = [
        pltpu.VMEM((taps, rows, chan), F32),
        pltpu.VMEM(inputs.shape, BF16),
        pltpu.VMEM((3, ex + 2, ey + 2, ez, chan), BF16),
        pltpu.VMEM((2, ex + 2, ey + 2, chan), BF16),
        pltpu.VMEM((2, ex + 2, ey + 2, chan), BF16),
        pltpu.VMEM((chan, ex * ey * ez), BF16),
        pltpu.VMEM((nx, ny, taps, rows, chan), F32),
        pltpu.VMEM((nx - 1, ny, taps, rows, chan), F32),
        pltpu.VMEM((ny, taps, rows, chan), BF16),
        pltpu.VMEM((ny - 1, taps, rows, chan), BF16),
        pltpu.VMEM((padded_taps, rows, chan), BF16),
        pltpu.VMEM((nz - 1, piece, rows, chan), BF16),
        pltpu.VMEM((nx, ny, taps, rows, chan), BF16),
        pltpu.VMEM((chan, taps * chan), BF16),
        pltpu.VMEM((2, 8, chan), F32),
        pltpu.VMEM((stat_slots, 8, chan), F32),
        pltpu.VMEM((nx * ny * nz, 8, chan), F32),
        dma((3,)), *pair(10), *pair(3 * (nx - 1)), *pair(3 * (ny - 1)), *pair(2 * (nz - 1)), *pair(2 * (nz - 1)),
        *pair(ny - 1), *pair(nx - 1), *pair(stat_slots), *pair(nx * ny * nz - 1),
    ]
    vmem = pl.BlockSpec(memory_space=pltpu.VMEM)
    anywhere = pl.BlockSpec(memory_space=pl.ANY)
    dx, full, std, coef = pl.pallas_call(
        functools.partial(kernel, dims),
        out_shape=(
            pltpu.VMEM(cotangent.shape, BF16),
            pltpu.VMEM((padded_taps, rows, chan), BF16),
            pltpu.VMEM((padded_taps, rows, chan), F32),
            pltpu.VMEM((8, chan), F32),
        ),
        in_specs=[anywhere] * 3,
        out_specs=(vmem,) * 4,
        scratch_shapes=scratch,
        compiler_params=pltpu.CompilerParams(
            collective_id=0, has_side_effects=True, vmem_limit_bytes=40 * 1024 * 1024
        ),
    )(*[pltpu.with_memory_space_constraint(v, pltpu.HBM) for v in (jnp.transpose(raw_weight, (1, 0, 2)), inputs, cotangent)])
    input_grad, weight_grad = pl.pallas_call(
        functools.partial(finish_kernel, nz, taps),
        out_shape=(
            jax.ShapeDtypeStruct(cotangent.shape, BF16),
            jax.ShapeDtypeStruct((taps, rows, chan), F32),
        ),
        in_specs=[vmem] * 4,
        out_specs=(anywhere,) * 2,
        scratch_shapes=[pltpu.VMEM((taps, rows, chan), F32), dma((2,))],
        compiler_params=pltpu.CompilerParams(vmem_limit_bytes=8 * 1024 * 1024),
    )(dx, full, std, coef)
    return input_grad, jnp.transpose(weight_grad, (1, 0, 2))


def solution(mesh):
    dims = tuple(mesh.shape[axis] for axis in AXES)
    in_specs = (P(("gx", "gy"), None, None), P("gx", "gy", "gz", None), P("gx", "gy", "gz", None))
    out_specs = (P("gx", "gy", "gz", None), P(("gx", "gy"), None, None))
    return jax.shard_map(
        functools.partial(on_device, dims), mesh=mesh, in_specs=in_specs, out_specs=out_specs, check_vma=False
    )
```

```python
import functools

import jax
import jax.numpy as jnp
from jax import lax
from jax.experimental import pallas as pl
from jax.experimental.pallas import tpu as pltpu
from jax.sharding import PartitionSpec as P

var_eps = 1e-05
norm_eps = 1e-06
clip_norm = 600.0
F32 = jnp.float32
BF16 = jnp.bfloat16
MESH = pl.DeviceIdType.MESH
AXES = ("gx", "gy", "gz")


def z_groups(taps, nz):
    most = nz * max(1, 8 // nz)
    groups, first, base = [], 0, 0
    while first < taps:
        many = min(most, taps - first)
        size = -(-many // nz)
        groups.append((base, first, many, size))
        first, base = first + many, base + size * nz
    return groups


def tap_slots(taps, nz):
    order = [t for c in (1, 0, 2) for t in range(c, taps, 3)]
    slots = [base + v for base, first, many, size in z_groups(taps, nz) for v in range(many)]
    return list(zip(order, slots))


def first_taps(taps):
    return taps // 3


def kernel(dims, raw_hbm, in_hbm, cot_hbm, dx_ref, full, std, coef_ref, *scratch):
    (raw_ref, in_ref, shifted, face_out, face_in, in_t, part, recv_x, send_y, recv_y, send_z, total_z, recv_z,
     std_all, w_cat, dx_part, stats, stats_in, total_in, load_sem, halo_send, halo_recv, x_send, x_recv, y_send, y_recv,
     z_send, z_recv, g_send, g_recv, ay_send, ay_recv, ax_send, ax_recv, st_send, st_recv, t_send, t_recv) = scratch
    count = dict(zip(AXES, dims))
    nx, ny, nz = dims
    me = {axis: lax.axis_index(axis) for axis in AXES}
    taps, rows, chan = raw_ref.shape
    ex, ey, ez = in_ref.shape[:3]
    groups = z_groups(taps, nz)
    order = [t for t, slot in tap_slots(taps, nz)]
    slots = [slot for t, slot in tap_slots(taps, nz)]
    early = first_taps(taps)
    fan_count = float(rows * nx * ny * taps)

    def peer(axis, k):
        return lax.rem(me[axis] + k, count[axis])

    def plane_peer(k):
        flat = lax.rem(me["gx"] * ny + me["gy"] + k, nx * ny)
        return {"gx": lax.div(flat, ny), "gy": lax.rem(flat, ny)}

    def remote(src, dst, send_sem, recv_sem, where):
        return pltpu.make_async_remote_copy(
            src_ref=src, dst_ref=dst, send_sem=send_sem, recv_sem=recv_sem,
            device_id=where, device_id_type=MESH,
        )

    def wait_all(copies):
        for copy in copies:
            copy.wait()

    def inside(step):
        within = None
        for axis, d in zip(AXES, step):
            if d:
                near = me[axis] + d
                ok = near >= 0 if d < 0 else near < count[axis]
                within = ok if within is None else jnp.logical_and(within, ok)
        return within

    def neighbour(step):
        return {axis: lax.min(lax.max(me[axis] + d, 0), count[axis] - 1) for axis, d in zip(AXES, step)}

    body = pl.ds(1, ey)
    load_cot = pltpu.make_async_copy(cot_hbm, shifted.at[1, pl.ds(1, ex), body], load_sem.at[1])
    load_raw = pltpu.make_async_copy(raw_hbm, raw_ref, load_sem.at[0])
    load_in = pltpu.make_async_copy(in_hbm, in_ref, load_sem.at[2])
    load_cot.start()
    load_raw.start()
    load_in.start()

    barrier = pltpu.get_barrier_semaphore()
    greeted = jnp.int32(nx * ny - 1 + nz - 1)
    for k in range(1, nx * ny):
        pl.semaphore_signal(barrier, inc=1, device_id=plane_peer(k), device_id_type=MESH)
    for k in range(1, nz):
        pl.semaphore_signal(barrier, inc=1, device_id={"gz": peer("gz", k)}, device_id_type=MESH)
    plane_steps = [(0, -1, 0), (0, 1, 0), (-1, -1, 0), (-1, 1, 0), (1, -1, 0), (1, 1, 0), (-1, 0, 0), (1, 0, 0)]
    depth_steps = [(dx, dy, dz) for dz in (-1, 1)
                   for dx, dy in [(0, 0), (-1, 0), (1, 0), (0, -1), (0, 1), (-1, -1), (-1, 1), (1, -1), (1, 1)]]
    for step in depth_steps:
        if step[0] or step[1]:
            near = inside(step)

            @pl.when(near)
            def _(step=step):
                pl.semaphore_signal(barrier, inc=1, device_id=neighbour(step), device_id_type=MESH)

            greeted = greeted + near.astype(jnp.int32)

    def exchange_start(slot, base, peers):
        copies = []
        for k, where in enumerate(peers):
            copy = remote(stats.at[slot], stats_in.at[base + k], st_send.at[base + k], st_recv.at[base + k], where)
            copy.start()
            copies.append(copy)
        return copies

    zero_plane = jnp.zeros((ey + 2, ez, chan), BF16)
    zero_col = jnp.zeros((ex + 2, ez, chan), BF16)
    for axis, edge, x in [("gx", 0, 0), ("gx", nx - 1, ex + 1)]:
        @pl.when(me[axis] == edge)
        def _(x=x):
            shifted[1, x] = zero_plane
            for side in range(2):
                face_in[side, x] = jnp.zeros((ey + 2, 1, chan), F32)

    for axis, edge, y in [("gy", 0, 0), ("gy", ny - 1, ey + 1)]:
        @pl.when(me[axis] == edge)
        def _(y=y):
            shifted[1, :, y] = zero_col
            for side in range(2):
                face_in[side, :, y] = jnp.zeros((ex + 2, 1, chan), F32)

    for side, edge in [(0, 0), (1, nz - 1)]:
        @pl.when(me["gz"] == edge)
        def _(side=side):
            face_in[side] = jnp.zeros((ex + 2, ey + 2, 1, chan), F32)

    for base, first, many, size in groups:
        for v in range(base + many, base + size * nz):
            send_z[v] = jnp.zeros((rows, chan), BF16)
            total_z[v] = jnp.zeros((rows, chan), F32)
            std[v] = jnp.zeros((rows, chan), F32)

    def per_output(value):
        return jnp.sum(jnp.sum(value, axis=0), axis=0, keepdims=True)

    load_raw.wait()
    raw = raw_ref[...]
    stats[0, 0] = per_output(raw)
    stats[0, 1] = per_output(raw * raw)
    stats[0, 2] = jnp.zeros((1, chan), F32)
    load_cot.wait()
    for x in range(ex):
        plane = shifted[1, x + 1, 1:ey + 1].astype(F32)
        face_out[0, x] = plane[:, 0:1, :]
        face_out[1, x] = plane[:, ez - 1:ez, :]
    pl.semaphore_wait(barrier, greeted)
    weight_sums = exchange_start(0, 0, [plane_peer(k) for k in range(1, nx * ny)])

    def halo_start(steps, base, source, target):
        copies = []
        for number, step in enumerate(steps, base):
            copy = remote(source(step), target(step), halo_send.at[number], halo_recv.at[number], neighbour(step))
            pl.when(inside(step))(copy.start)
            copies.append((step, copy))
        return copies

    def halo_wait(copies):
        for step, copy in copies:
            pl.when(inside(step))(copy.wait_send)
            pl.when(inside([-d for d in step]))(copy.wait_recv)

    def plane_source(step):
        return shifted.at[1, {-1: 1, 0: pl.ds(1, ex), 1: ex}[step[0]], {-1: 1, 0: body, 1: ey}[step[1]]]

    def plane_target(step):
        return shifted.at[1, {-1: ex + 1, 0: pl.ds(1, ex), 1: 0}[step[0]], {-1: ey + 1, 0: body, 1: 0}[step[1]]]

    def depth_source(step):
        return face_out.at[{-1: 0, 1: 1}[step[2]], {-1: pl.ds(0, 1), 0: pl.ds(0, ex), 1: pl.ds(ex - 1, 1)}[step[0]],
                           {-1: pl.ds(0, 1), 0: pl.ds(0, ey), 1: pl.ds(ey - 1, 1)}[step[1]]]

    def depth_target(step):
        return face_in.at[{-1: 1, 1: 0}[step[2]], {-1: pl.ds(ex + 1, 1), 0: pl.ds(1, ex), 1: pl.ds(0, 1)}[step[0]],
                          {-1: pl.ds(ey + 1, 1), 0: pl.ds(1, ey), 1: pl.ds(0, 1)}[step[1]]]

    plane_halo = halo_start(plane_steps, 0, plane_source, plane_target)
    depth_halo = halo_start(depth_steps, len(plane_steps), depth_source, depth_target)
    load_in.wait()
    for x in range(ex):
        in_t[:, x * ey * ez:(x + 1) * ey * ez] = in_ref[x].reshape(ey * ez, chan).T

    wait_all(weight_sums)
    sums = stats[0]
    for k in range(len(weight_sums)):
        sums = sums + stats_in[k]
    mean_out = sums[0] / fan_count
    var_out = sums[1] / fan_count - mean_out * mean_out
    inv_std = lax.rsqrt(var_out + var_eps)
    own = std_all.at[me["gx"], me["gy"]]
    for u, t in enumerate(order):
        value = (raw_ref[t] - mean_out) * inv_std
        std[slots[u]] = value
        own[u] = value.astype(BF16)

    def gather_y_start(part_number):
        span = [pl.ds(0, early), pl.ds(early, taps - early)][part_number]
        copies = []
        for k in range(1, ny):
            index = part_number * (ny - 1) + k - 1
            copy = remote(own.at[span], own.at[span], ay_send.at[index], ay_recv.at[index], {"gy": peer("gy", k)})
            copy.start()
            copies.append(copy)
        return copies

    def gather_x_start(part_number):
        span = [pl.ds(0, early), pl.ds(early, taps - early)][part_number]
        copies = []
        for k in range(1, nx):
            index = part_number * (nx - 1) + k - 1
            mine = std_all.at[me["gx"], :, span]
            copy = remote(mine, mine, ax_send.at[index], ax_recv.at[index], {"gx": peer("gx", k)})
            copy.start()
            copies.append(copy)
        return copies

    gather_y = [gather_y_start(0)]
    halo_wait(plane_halo)

    def view(t, start, planes):
        a, b, c = t // 9, (t // 3) % 3, t % 3
        block = shifted[2 - c, pl.ds(start + 2 - a, planes), 2 - b:2 - b + ey]
        return block.reshape(planes * ey * ez, chan)

    def filter_chunk(g):
        base, first, many, size = groups[g]
        for u in range(first, first + many, 2):
            group = list(range(u, min(u + 2, first + many)))
            views = [view(order[v], 0, ex) for v in group]
            right = jnp.concatenate(views, axis=1) if len(views) > 1 else views[0]
            product = jnp.dot(in_t[...], right, preferred_element_type=F32)
            for j, v in enumerate(group):
                for gx in range(nx):
                    for gy in range(ny):
                        low = (gx * ny + gy) * rows
                        part[gx, gy, v] = product[low:low + rows, j * chan:(j + 1) * chan]
        copies = []
        span = pl.ds(first, many)
        for k in range(1, nx):
            index = g * (nx - 1) + k - 1
            copy = remote(part.at[peer("gx", k), :, span], recv_x.at[k - 1, :, span],
                          x_send.at[index], x_recv.at[index], {"gx": peer("gx", k)})
            copy.start()
            copies.append(copy)
        return copies

    def rows_total(gy, span):
        total = part[me["gx"], gy, span]
        for k in range(1, nx):
            total = total + recv_x[k - 1, gy, span]
        return total

    def rows_chunk(g, copies):
        wait_all(copies)
        base, first, many, size = groups[g]
        span = pl.ds(first, many)
        for gy in range(ny):
            send_y[gy, span] = rows_total(gy, span).astype(BF16)
        sent = []
        for k in range(1, ny):
            index = g * (ny - 1) + k - 1
            copy = remote(send_y.at[peer("gy", k), span], recv_y.at[k - 1, span],
                          y_send.at[index], y_recv.at[index], {"gy": peer("gy", k)})
            copy.start()
            sent.append(copy)
        return sent

    depth_index = lax.broadcasted_iota(jnp.int32, (ey + 2, ez, chan), 1)

    def shift(slot, side, amount, edge):
        for x in range(ex + 2):
            plane = shifted[1, x].astype(F32)
            outer = face_in[side, x]
            shifted[slot, x] = jnp.where(depth_index == edge, outer, pltpu.roll(plane, amount, 1)).astype(BF16)

    reduce_x, reduce_y = [filter_chunk(0)], []
    halo_wait(depth_halo)
    shift(2, 1, ez - 1, ez - 1)
    shift(0, 0, 1, 0)
    for g in range(1, len(groups)):
        reduce_x.append(filter_chunk(g))
        reduce_y.append(rows_chunk(g - 1, reduce_x[g - 1]))
    reduce_y.append(rows_chunk(len(groups) - 1, reduce_x[-1]))
    gather_y.append(gather_y_start(1))
    wait_all(gather_y[0])
    gather_x = [gather_x_start(0)]

    step = 2 if ex % 2 == 0 else 1

    def dx_pass(low, high, last):
        for u in range(low, high):
            w_cat[:, u * chan:(u + 1) * chan] = std_all[:, :, u].reshape(nx * ny * rows, chan)

        def dx_step(n, carry):
            start = n * step
            left = jnp.concatenate([view(t, start, step) for t in order[low:high]], axis=1)
            right = w_cat[:, low * chan:high * chan]
            product = lax.dot_general(left, right, (((1,), (1,)), ((), ())), preferred_element_type=F32)
            product = product.reshape(step, ey, ez, chan)
            if last:
                dx_ref[pl.ds(start, step)] = (product + dx_part[pl.ds(start, step)]).astype(BF16)
            else:
                dx_part[pl.ds(start, step)] = product
            return carry

        lax.fori_loop(0, ex // step, dx_step, 0)

    def depth_start(g):
        wait_all(reduce_y[g])
        base, first, many, size = groups[g]
        span = pl.ds(first, many)
        total = rows_total(me["gy"], span)
        for k in range(1, ny):
            total = total + recv_y[k - 1, span].astype(F32)
        total_z[base:base + many] = total
        send_z[base:base + many] = total.astype(BF16)
        copies = []
        for k in range(1, nz):
            index = g * (nz - 1) + k - 1
            copy = remote(send_z.at[pl.ds(base + peer("gz", k) * size, size)],
                          recv_z.at[k - 1, pl.ds(base // nz, size)],
                          z_send.at[index], z_recv.at[index], {"gz": peer("gz", k)})
            copy.start()
            copies.append(copy)
        return copies

    def depth_sum(g, copies):
        wait_all(copies)
        base, first, many, size = groups[g]
        mine = pl.ds(base + me["gz"] * size, size)
        grad = total_z[mine]
        for k in range(1, nz):
            grad = grad + recv_z[k - 1, pl.ds(base // nz, size)].astype(F32)
        full[mine] = grad.astype(BF16)
        return [per_output(grad), per_output(grad * std[mine]), per_output(grad * grad)]

    def gather_start(g):
        base, first, many, size = groups[g]
        mine = pl.ds(base + me["gz"] * size, size)
        copies = []
        for k in range(1, nz):
            index = g * (nz - 1) + k - 1
            copy = remote(full.at[mine], full.at[mine], g_send.at[index], g_recv.at[index], {"gz": peer("gz", k)})
            copy.start()
            copies.append(copy)
        return copies

    wait_all(gather_x[0])
    dx_pass(0, early, False)
    reduce_z = [depth_start(g) for g in range(len(groups))]
    sums, gather_z = [None] * 3, []
    for g in range(len(groups)):
        if g == len(groups) - 2:
            wait_all(gather_y[1])
            gather_x.append(gather_x_start(1))
        new = depth_sum(g, reduce_z[g])
        sums = new if g == 0 else [a + b for a, b in zip(sums, new)]
        if g < len(groups) - 1:
            gather_z += gather_start(g)
    for n in range(3):
        stats[1, n] = sums[n]
    flat = (me["gx"] * ny + me["gy"]) * nz + me["gz"]
    total_in[flat] = stats[1]
    final_sums = []
    for k in range(1, nx * ny * nz):
        other = lax.rem(flat + k, nx * ny * nz)
        where = {
            "gx": lax.div(other, ny * nz),
            "gy": lax.rem(lax.div(other, nz), ny),
            "gz": lax.rem(other, nz),
        }
        copy = remote(stats.at[1], total_in.at[flat], t_send.at[k - 1], t_recv.at[k - 1], where)
        copy.start()
        final_sums.append(copy)
    gather_z += gather_start(len(groups) - 1)
    wait_all(gather_x[1])
    dx_pass(early, taps, True)
    wait_all(final_sums)
    sums = total_in[0]
    for k in range(1, nx * ny * nz):
        sums = sums + total_in[k]
    sum_grad, sum_cross, sum_square = sums[0], sums[1], sums[2]
    mean_grad = sum_grad / fan_count
    mean_cross = sum_cross / fan_count
    spread = sum_square - 2.0 * mean_grad * sum_grad - 2.0 * mean_cross * sum_cross
    spread = (
        spread
        + fan_count * mean_grad * mean_grad
        + fan_count * mean_cross * mean_cross * var_out / (var_out + var_eps)
    )
    square_sum = jnp.sum(inv_std * inv_std * spread, axis=1, keepdims=True)
    scale = jnp.minimum(1.0, clip_norm * lax.rsqrt(square_sum + norm_eps))
    coef_ref[0:1] = inv_std * scale
    coef_ref[1:2] = mean_grad
    coef_ref[2:3] = mean_cross
    wait_all(gather_z)


def finish_kernel(nz, taps, dx_in, full, std, coef_ref, dx_hbm, wg_hbm, wg_ref, sem):
    out_dx = pltpu.make_async_copy(dx_in, dx_hbm, sem.at[0])
    out_dx.start()
    factor, mean_grad, mean_cross = coef_ref[0:1], coef_ref[1:2], coef_ref[2:3]
    for t, slot in tap_slots(taps, nz):
        wg_ref[t] = factor * (full[slot].astype(F32) - mean_grad - std[slot] * mean_cross)
    out_wg = pltpu.make_async_copy(wg_ref, wg_hbm, sem.at[1])
    out_wg.start()
    out_wg.wait()
    out_dx.wait()


def on_device(dims, raw_weight, inputs, cotangent):
    nx, ny, nz = dims
    rows, taps, chan = raw_weight.shape
    ex, ey, ez = inputs.shape[:3]
    groups = z_groups(taps, nz)
    many = len(groups)
    piece = sum(size for base, first, number, size in groups)
    padded_taps = piece * nz
    stat_slots = nx * ny - 1
    dma = pltpu.SemaphoreType.DMA

    def pair(n):
        return [dma((max(n, 1),)), dma((max(n, 1),))]

    scratch = [
        pltpu.VMEM((taps, rows, chan), F32),
        pltpu.VMEM(inputs.shape, BF16),
        pltpu.VMEM((3, ex + 2, ey + 2, ez, chan), BF16),
        pltpu.VMEM((2, ex, ey, 1, chan), F32),
        pltpu.VMEM((2, ex + 2, ey + 2, 1, chan), F32),
        pltpu.VMEM((chan, ex * ey * ez), BF16),
        pltpu.VMEM((nx, ny, taps, rows, chan), F32),
        pltpu.VMEM((nx - 1, ny, taps, rows, chan), F32),
        pltpu.VMEM((ny, taps, rows, chan), BF16),
        pltpu.VMEM((ny - 1, taps, rows, chan), BF16),
        pltpu.VMEM((padded_taps, rows, chan), BF16),
        pltpu.VMEM((padded_taps, rows, chan), F32),
        pltpu.VMEM((nz - 1, piece, rows, chan), BF16),
        pltpu.VMEM((nx, ny, taps, rows, chan), BF16),
        pltpu.VMEM((chan, taps * chan), BF16),
        pltpu.VMEM((ex, ey, ez, chan), F32),
        pltpu.VMEM((2, 3, 1, chan), F32),
        pltpu.VMEM((stat_slots, 3, 1, chan), F32),
        pltpu.VMEM((nx * ny * nz, 3, 1, chan), F32),
        dma((3,)), *pair(26), *pair(many * (nx - 1)), *pair(many * (ny - 1)), *pair(many * (nz - 1)),
        *pair(many * (nz - 1)), *pair(2 * (ny - 1)), *pair(2 * (nx - 1)), *pair(stat_slots), *pair(nx * ny * nz - 1),
    ]
    vmem = pl.BlockSpec(memory_space=pltpu.VMEM)
    anywhere = pl.BlockSpec(memory_space=pl.ANY)
    operands = (jnp.transpose(raw_weight, (1, 0, 2)), inputs, cotangent)
    dx, full, std, coef = pl.pallas_call(
        functools.partial(kernel, dims),
        out_shape=(
            pltpu.VMEM(cotangent.shape, BF16),
            pltpu.VMEM((padded_taps, rows, chan), BF16),
            pltpu.VMEM((padded_taps, rows, chan), F32),
            pltpu.VMEM((8, chan), F32),
        ),
        in_specs=[anywhere] * 3,
        out_specs=(vmem,) * 4,
        scratch_shapes=scratch,
        compiler_params=pltpu.CompilerParams(
            collective_id=0, has_side_effects=True, vmem_limit_bytes=40 * 1024 * 1024
        ),
    )(*[pltpu.with_memory_space_constraint(v, pltpu.HBM) for v in operands])
    input_grad, weight_grad = pl.pallas_call(
        functools.partial(finish_kernel, nz, taps),
        out_shape=(
            jax.ShapeDtypeStruct(cotangent.shape, BF16),
            jax.ShapeDtypeStruct((taps, rows, chan), F32),
        ),
        in_specs=[vmem] * 4,
        out_specs=(anywhere,) * 2,
        scratch_shapes=[pltpu.VMEM((taps, rows, chan), F32), dma((2,))],
        compiler_params=pltpu.CompilerParams(vmem_limit_bytes=8 * 1024 * 1024),
    )(dx, full, std, coef)
    return input_grad, jnp.transpose(weight_grad, (1, 0, 2))


def solution(mesh):
    dims = tuple(mesh.shape[axis] for axis in AXES)
    in_specs = (P(("gx", "gy"), None, None), P("gx", "gy", "gz", None), P("gx", "gy", "gz", None))
    out_specs = (P("gx", "gy", "gz", None), P(("gx", "gy"), None, None))
    return jax.shard_map(
        functools.partial(on_device, dims), mesh=mesh, in_specs=in_specs, out_specs=out_specs, check_vma=False
    )
```

```python
import functools

import jax
import jax.numpy as jnp
from jax import lax
from jax.experimental import pallas as pl
from jax.experimental.pallas import tpu as pltpu
from jax.sharding import PartitionSpec as P

var_eps = 1e-05
norm_eps = 1e-06
clip_norm = 600.0
F32 = jnp.float32
BF16 = jnp.bfloat16
MESH = pl.DeviceIdType.MESH
AXES = ("gx", "gy", "gz")


def z_groups(taps, nz):
    most = nz * max(1, 8 // nz)
    groups, first, base = [], 0, 0
    while first < taps:
        many = min(most, taps - first)
        size = -(-many // nz)
        groups.append((base, first, many, size))
        first, base = first + many, base + size * nz
    return groups


def tap_slots(taps, nz):
    order = [t for c in (1, 0, 2) for t in range(c, taps, 3)]
    slots = [base + v for base, first, many, size in z_groups(taps, nz) for v in range(many)]
    return list(zip(order, slots))


def first_taps(taps):
    return 2 * (taps // 3)


def kernel(dims, raw_hbm, in_hbm, cot_hbm, dx_ref, full, std, coef_ref, *scratch):
    (raw_ref, in_ref, shifted, face_out, face_in, in_t, part, recv_x, send_y, recv_y, send_z, total_z, recv_z,
     std_all, w_cat, dx_part, stats, stats_in, total_in, load_sem, halo_send, halo_recv, x_send, x_recv, y_send, y_recv,
     z_send, z_recv, g_send, g_recv, ay_send, ay_recv, ax_send, ax_recv, st_send, st_recv, t_send, t_recv) = scratch
    count = dict(zip(AXES, dims))
    nx, ny, nz = dims
    me = {axis: lax.axis_index(axis) for axis in AXES}
    taps, rows, chan = raw_ref.shape
    ex, ey, ez = in_ref.shape[:3]
    groups = z_groups(taps, nz)
    order = [t for t, slot in tap_slots(taps, nz)]
    slots = [slot for t, slot in tap_slots(taps, nz)]
    early = first_taps(taps)
    fan_count = float(rows * nx * ny * taps)

    def peer(axis, k):
        return lax.rem(me[axis] + k, count[axis])

    def plane_peer(k):
        flat = lax.rem(me["gx"] * ny + me["gy"] + k, nx * ny)
        return {"gx": lax.div(flat, ny), "gy": lax.rem(flat, ny)}

    def remote(src, dst, send_sem, recv_sem, where):
        return pltpu.make_async_remote_copy(
            src_ref=src, dst_ref=dst, send_sem=send_sem, recv_sem=recv_sem,
            device_id=where, device_id_type=MESH,
        )

    def arrived(ref, sem):
        remote(ref, ref, sem, sem, plane_peer(1)).wait_recv()

    def departed(ref, sem):
        remote(ref, ref, sem, sem, plane_peer(1)).wait_send()

    def inside(step):
        within = None
        for axis, d in zip(AXES, step):
            if d:
                near = me[axis] + d
                ok = near >= 0 if d < 0 else near < count[axis]
                within = ok if within is None else jnp.logical_and(within, ok)
        return within

    def neighbour(step):
        return {axis: lax.min(lax.max(me[axis] + d, 0), count[axis] - 1) for axis, d in zip(AXES, step)}

    body = pl.ds(1, ey)
    barrier = pltpu.get_barrier_semaphore()
    greeted = jnp.int32(nx * ny - 1 + nz - 1)
    plane_steps = [(0, -1, 0), (0, 1, 0), (-1, -1, 0), (-1, 1, 0), (1, -1, 0), (1, 1, 0), (-1, 0, 0), (1, 0, 0)]
    depth_steps = [(dx, dy, dz) for dz in (-1, 1)
                   for dx, dy in [(0, 0), (-1, 0), (1, 0), (0, -1), (0, 1), (-1, -1), (-1, 1), (1, -1), (1, 1)]]
    for step in reversed(depth_steps):
        if step[0] or step[1]:
            near = inside(step)

            @pl.when(near)
            def _(step=step):
                pl.semaphore_signal(barrier, inc=1, device_id=neighbour(step), device_id_type=MESH)

            greeted = greeted + near.astype(jnp.int32)

    for k in range(1, nz):
        pl.semaphore_signal(barrier, inc=1, device_id={"gz": peer("gz", k)}, device_id_type=MESH)
    for k in range(1, nx * ny):
        pl.semaphore_signal(barrier, inc=1, device_id=plane_peer(k), device_id_type=MESH)
    load_cot = pltpu.make_async_copy(cot_hbm, shifted.at[1, pl.ds(1, ex), body], load_sem.at[1])
    load_raw = pltpu.make_async_copy(raw_hbm, raw_ref, load_sem.at[0])
    load_in = pltpu.make_async_copy(in_hbm, in_ref, load_sem.at[2])
    load_cot.start()
    load_raw.start()
    load_in.start()

    zero_plane = jnp.zeros((ey + 2, ez, chan), BF16)
    zero_col = jnp.zeros((ex + 2, ez, chan), BF16)
    for axis, edge, x in [("gx", 0, 0), ("gx", nx - 1, ex + 1)]:
        @pl.when(me[axis] == edge)
        def _(x=x):
            shifted[1, x] = zero_plane
            for side in range(2):
                face_in[side, x] = jnp.zeros((ey + 2, 1, chan), F32)

    for axis, edge, y in [("gy", 0, 0), ("gy", ny - 1, ey + 1)]:
        @pl.when(me[axis] == edge)
        def _(y=y):
            shifted[1, :, y] = zero_col
            for side in range(2):
                face_in[side, :, y] = jnp.zeros((ex + 2, 1, chan), F32)

    for side, edge in [(0, 0), (1, nz - 1)]:
        @pl.when(me["gz"] == edge)
        def _(side=side):
            face_in[side] = jnp.zeros((ex + 2, ey + 2, 1, chan), F32)

    for base, first, many, size in groups:
        for v in range(base + many, base + size * nz):
            send_z[v] = jnp.zeros((rows, chan), BF16)
            total_z[v] = jnp.zeros((rows, chan), F32)
            std[v] = jnp.zeros((rows, chan), F32)

    def per_output(value):
        return jnp.sum(jnp.sum(value, axis=0), axis=0, keepdims=True)

    load_raw.wait()
    raw = raw_ref[...]
    stats[0, 0] = per_output(raw)
    stats[0, 1] = per_output(raw * raw)
    stats[0, 2] = jnp.zeros((1, chan), F32)
    load_cot.wait()
    for x in range(ex):
        plane = shifted[1, x + 1, 1:ey + 1].astype(F32)
        face_out[0, x] = plane[:, 0:1, :]
        face_out[1, x] = plane[:, ez - 1:ez, :]
    pl.semaphore_wait(barrier, greeted)
    for k in range(1, nx * ny):
        remote(stats.at[0], stats_in.at[k - 1], st_send.at[0], st_recv.at[0], plane_peer(k)).start()

    odd = lax.rem(me["gy"], 2) == 1

    def halo_start(steps, base, source, target):
        copies = []
        for number, step in enumerate(steps, base):
            copies.append((step, remote(source(step), target(step), halo_send.at[number], halo_recv.at[number],
                                        neighbour(step))))
        for far in (True, False):
            for step, copy in copies:
                up = odd if step[1] > 0 else jnp.logical_not(odd)
                if step[1]:
                    pl.when(jnp.logical_and(inside(step), up if far else jnp.logical_not(up)))(copy.start)
                elif not far:
                    pl.when(inside(step))(copy.start)
        return copies

    def halo_wait(copies):
        for step, copy in copies:
            pl.when(inside(step))(copy.wait_send)
            pl.when(inside([-d for d in step]))(copy.wait_recv)

    def plane_source(step):
        return shifted.at[1, {-1: 1, 0: pl.ds(1, ex), 1: ex}[step[0]], {-1: 1, 0: body, 1: ey}[step[1]]]

    def plane_target(step):
        return shifted.at[1, {-1: ex + 1, 0: pl.ds(1, ex), 1: 0}[step[0]], {-1: ey + 1, 0: body, 1: 0}[step[1]]]

    def depth_source(step):
        return face_out.at[{-1: 0, 1: 1}[step[2]], {-1: pl.ds(0, 1), 0: pl.ds(0, ex), 1: pl.ds(ex - 1, 1)}[step[0]],
                           {-1: pl.ds(0, 1), 0: pl.ds(0, ey), 1: pl.ds(ey - 1, 1)}[step[1]]]

    def depth_target(step):
        return face_in.at[{-1: 1, 1: 0}[step[2]], {-1: pl.ds(ex + 1, 1), 0: pl.ds(1, ex), 1: pl.ds(0, 1)}[step[0]],
                          {-1: pl.ds(ey + 1, 1), 0: pl.ds(1, ey), 1: pl.ds(0, 1)}[step[1]]]

    plane_halo = halo_start(plane_steps, 0, plane_source, plane_target)
    depth_halo = halo_start(depth_steps, len(plane_steps), depth_source, depth_target)
    load_in.wait()
    for x in range(ex):
        in_t[:, x * ey * ez:(x + 1) * ey * ez] = in_ref[x].reshape(ey * ez, chan).T

    arrived(stats_in, st_recv.at[0])
    sums = stats[0]
    for k in range(nx * ny - 1):
        sums = sums + stats_in[k]
    mean_out = sums[0] / fan_count
    var_out = sums[1] / fan_count - mean_out * mean_out
    inv_std = lax.rsqrt(var_out + var_eps)
    own = std_all.at[me["gx"], me["gy"]]
    for u, t in enumerate(order):
        value = (raw_ref[t] - mean_out) * inv_std
        std[slots[u]] = value
        own[u] = value.astype(BF16)

    spans = [pl.ds(0, early), pl.ds(early, taps - early)]

    def gather_y_start(n):
        mine = own.at[spans[n]]
        for k in range(1, ny):
            remote(mine, mine, ay_send.at[0], ay_recv.at[n], {"gy": peer("gy", k)}).start()

    def gather_x_start(n):
        arrived(std_all.at[0, pl.ds(0, ny - 1), spans[n]], ay_recv.at[n])
        mine = std_all.at[me["gx"], :, spans[n]]
        for k in range(1, nx):
            remote(mine, mine, ax_send.at[0], ax_recv.at[n], {"gx": peer("gx", k)}).start()

    def gather_wait(n):
        arrived(std_all.at[pl.ds(0, nx - 1), :, spans[n]], ax_recv.at[n])

    gather_y_start(0)
    halo_wait(plane_halo)

    def view(t, start, planes):
        a, b, c = t // 9, (t // 3) % 3, t % 3
        block = shifted[2 - c, pl.ds(start + 2 - a, planes), 2 - b:2 - b + ey]
        return block.reshape(planes * ey * ez, chan)

    def filter_chunk(g):
        base, first, many, size = groups[g]
        for u in range(first, first + many, 2):
            group = list(range(u, min(u + 2, first + many)))
            views = [view(order[v], 0, ex) for v in group]
            right = jnp.concatenate(views, axis=1) if len(views) > 1 else views[0]
            product = jnp.dot(in_t[...], right, preferred_element_type=F32)
            for j, v in enumerate(group):
                for gx in range(nx):
                    for gy in range(ny):
                        low = (gx * ny + gy) * rows
                        part[gx, gy, v] = product[low:low + rows, j * chan:(j + 1) * chan]
        span = pl.ds(first, many)
        for k in range(1, nx):
            remote(part.at[peer("gx", k), :, span], recv_x.at[k - 1, :, span], x_send.at[0], x_recv.at[g],
                   {"gx": peer("gx", k)}).start()

    def rows_total(gy, span):
        total = part[me["gx"], gy, span]
        for k in range(1, nx):
            total = total + recv_x[k - 1, gy, span]
        return total

    def rows_chunk(g):
        base, first, many, size = groups[g]
        span = pl.ds(first, many)
        arrived(recv_x.at[:, :, span], x_recv.at[g])
        for gy in range(ny):
            send_y[gy, span] = rows_total(gy, span).astype(BF16)
        for k in range(1, ny):
            remote(send_y.at[peer("gy", k), span], recv_y.at[k - 1, span], y_send.at[0], y_recv.at[g],
                   {"gy": peer("gy", k)}).start()

    depth_index = lax.broadcasted_iota(jnp.int32, (ey + 2, ez, chan), 1)

    def shift(slot, side, amount, edge):
        for x in range(ex + 2):
            plane = shifted[1, x].astype(F32)
            outer = face_in[side, x]
            shifted[slot, x] = jnp.where(depth_index == edge, outer, pltpu.roll(plane, amount, 1)).astype(BF16)

    filter_chunk(0)
    halo_wait(depth_halo)
    shift(2, 1, ez - 1, ez - 1)
    shift(0, 0, 1, 0)
    for g in range(1, len(groups)):
        filter_chunk(g)
        rows_chunk(g - 1)
    rows_chunk(len(groups) - 1)
    gather_y_start(1)
    gather_x_start(0)

    step = 2 if ex % 2 == 0 else 1

    def dx_pass(low, high, last):
        for u in range(low, high):
            w_cat[:, u * chan:(u + 1) * chan] = std_all[:, :, u].reshape(nx * ny * rows, chan)

        def dx_step(n, carry):
            start = n * step
            left = jnp.concatenate([view(t, start, step) for t in order[low:high]], axis=1)
            right = w_cat[:, low * chan:high * chan]
            product = lax.dot_general(left, right, (((1,), (1,)), ((), ())), preferred_element_type=F32)
            product = product.reshape(step, ey, ez, chan)
            if last:
                dx_ref[pl.ds(start, step)] = (product + dx_part[pl.ds(start, step)]).astype(BF16)
            else:
                dx_part[pl.ds(start, step)] = product
            return carry

        lax.fori_loop(0, ex // step, dx_step, 0)

    def depth_start(g):
        base, first, many, size = groups[g]
        span = pl.ds(first, many)
        arrived(recv_y.at[:, span], y_recv.at[g])
        total = rows_total(me["gy"], span)
        for k in range(1, ny):
            total = total + recv_y[k - 1, span].astype(F32)
        total_z[base:base + many] = total
        send_z[base:base + many] = total.astype(BF16)
        for k in range(1, nz):
            remote(send_z.at[pl.ds(base + peer("gz", k) * size, size)], recv_z.at[k - 1, pl.ds(base // nz, size)],
                   z_send.at[0], z_recv.at[g], {"gz": peer("gz", k)}).start()

    def depth_sum(g):
        base, first, many, size = groups[g]
        mine = pl.ds(base + me["gz"] * size, size)
        arrived(recv_z.at[:, pl.ds(base // nz, size)], z_recv.at[g])
        grad = total_z[mine]
        for k in range(1, nz):
            grad = grad + recv_z[k - 1, pl.ds(base // nz, size)].astype(F32)
        full[mine] = grad.astype(BF16)
        return [per_output(grad), per_output(grad * std[mine]), per_output(grad * grad)]

    def gather_start(g):
        base, first, many, size = groups[g]
        mine = pl.ds(base + me["gz"] * size, size)
        for k in range(1, nz):
            remote(full.at[mine], full.at[mine], g_send.at[0], g_recv.at[0], {"gz": peer("gz", k)}).start()

    gather_wait(0)
    dx_pass(0, early, False)
    for g in range(len(groups)):
        depth_start(g)
    sums = None
    for g in range(len(groups)):
        if g == len(groups) - 2:
            gather_x_start(1)
        new = depth_sum(g)
        sums = new if g == 0 else [a + b for a, b in zip(sums, new)]
        if g < len(groups) - 1:
            gather_start(g)
    for n in range(3):
        stats[1, n] = sums[n]
    flat = (me["gx"] * ny + me["gy"]) * nz + me["gz"]
    total_in[flat] = stats[1]
    for k in range(1, nx * ny * nz):
        other = lax.rem(flat + k, nx * ny * nz)
        where = {
            "gx": lax.div(other, ny * nz),
            "gy": lax.rem(lax.div(other, nz), ny),
            "gz": lax.rem(other, nz),
        }
        remote(stats.at[1], total_in.at[flat], t_send.at[0], t_recv.at[0], where).start()
    gather_start(len(groups) - 1)
    gather_wait(1)
    dx_pass(early, taps, True)
    departed(stats_in, st_send.at[0])
    departed(part.at[pl.ds(0, nx - 1)], x_send.at[0])
    departed(send_y.at[pl.ds(0, ny - 1)], y_send.at[0])
    departed(recv_z, z_send.at[0])
    departed(recv_z, g_send.at[0])
    departed(std_all.at[0, pl.ds(0, ny - 1)], ay_send.at[0])
    departed(std_all.at[pl.ds(0, nx - 1)], ax_send.at[0])
    others = total_in.at[pl.ds(0, nx * ny * nz - 1)]
    departed(others, t_send.at[0])
    arrived(others, t_recv.at[0])
    sums = total_in[0]
    for k in range(1, nx * ny * nz):
        sums = sums + total_in[k]
    sum_grad, sum_cross, sum_square = sums[0], sums[1], sums[2]
    mean_grad = sum_grad / fan_count
    mean_cross = sum_cross / fan_count
    spread = sum_square - 2.0 * mean_grad * sum_grad - 2.0 * mean_cross * sum_cross
    spread = (
        spread
        + fan_count * mean_grad * mean_grad
        + fan_count * mean_cross * mean_cross * var_out / (var_out + var_eps)
    )
    square_sum = jnp.sum(inv_std * inv_std * spread, axis=1, keepdims=True)
    scale = jnp.minimum(1.0, clip_norm * lax.rsqrt(square_sum + norm_eps))
    coef_ref[0:1] = inv_std * scale
    coef_ref[1:2] = mean_grad
    coef_ref[2:3] = mean_cross
    arrived(recv_z, g_recv.at[0])


def finish_kernel(nz, taps, dx_in, full, std, coef_ref, dx_hbm, wg_hbm, wg_ref, sem):
    out_dx = pltpu.make_async_copy(dx_in, dx_hbm, sem.at[0])
    out_dx.start()
    factor, mean_grad, mean_cross = coef_ref[0:1], coef_ref[1:2], coef_ref[2:3]
    for t, slot in tap_slots(taps, nz):
        wg_ref[t] = factor * (full[slot].astype(F32) - mean_grad - std[slot] * mean_cross)
    out_wg = pltpu.make_async_copy(wg_ref, wg_hbm, sem.at[1])
    out_wg.start()
    out_wg.wait()
    out_dx.wait()


def on_device(dims, raw_weight, inputs, cotangent):
    nx, ny, nz = dims
    rows, taps, chan = raw_weight.shape
    ex, ey, ez = inputs.shape[:3]
    groups = z_groups(taps, nz)
    many = len(groups)
    piece = sum(size for base, first, number, size in groups)
    padded_taps = piece * nz
    stat_slots = nx * ny - 1
    dma = pltpu.SemaphoreType.DMA

    def pair(n, m):
        return [dma((n,)), dma((m,))]

    scratch = [
        pltpu.VMEM((taps, rows, chan), F32),
        pltpu.VMEM(inputs.shape, BF16),
        pltpu.VMEM((3, ex + 2, ey + 2, ez, chan), BF16),
        pltpu.VMEM((2, ex, ey, 1, chan), F32),
        pltpu.VMEM((2, ex + 2, ey + 2, 1, chan), F32),
        pltpu.VMEM((chan, ex * ey * ez), BF16),
        pltpu.VMEM((nx, ny, taps, rows, chan), F32),
        pltpu.VMEM((nx - 1, ny, taps, rows, chan), F32),
        pltpu.VMEM((ny, taps, rows, chan), BF16),
        pltpu.VMEM((ny - 1, taps, rows, chan), BF16),
        pltpu.VMEM((padded_taps, rows, chan), BF16),
        pltpu.VMEM((padded_taps, rows, chan), F32),
        pltpu.VMEM((nz - 1, piece, rows, chan), BF16),
        pltpu.VMEM((nx, ny, taps, rows, chan), BF16),
        pltpu.VMEM((chan, taps * chan), BF16),
        pltpu.VMEM((ex, ey, ez, chan), F32),
        pltpu.VMEM((2, 3, 1, chan), F32),
        pltpu.VMEM((stat_slots, 3, 1, chan), F32),
        pltpu.VMEM((nx * ny * nz, 3, 1, chan), F32),
        dma((3,)), *pair(26, 26), *pair(1, many), *pair(1, many), *pair(1, many), *pair(1, 1), *pair(1, 2), *pair(1, 2),
        *pair(1, 1), *pair(1, 1),
    ]
    vmem = pl.BlockSpec(memory_space=pltpu.VMEM)
    anywhere = pl.BlockSpec(memory_space=pl.ANY)
    operands = (jnp.transpose(raw_weight, (1, 0, 2)), inputs, cotangent)
    dx, full, std, coef = pl.pallas_call(
        functools.partial(kernel, dims),
        out_shape=(
            pltpu.VMEM(cotangent.shape, BF16),
            pltpu.VMEM((padded_taps, rows, chan), BF16),
            pltpu.VMEM((padded_taps, rows, chan), F32),
            pltpu.VMEM((8, chan), F32),
        ),
        in_specs=[anywhere] * 3,
        out_specs=(vmem,) * 4,
        scratch_shapes=scratch,
        compiler_params=pltpu.CompilerParams(
            collective_id=0, has_side_effects=True, vmem_limit_bytes=40 * 1024 * 1024
        ),
    )(*[pltpu.with_memory_space_constraint(v, pltpu.HBM) for v in operands])
    input_grad, weight_grad = pl.pallas_call(
        functools.partial(finish_kernel, nz, taps),
        out_shape=(
            jax.ShapeDtypeStruct(cotangent.shape, BF16),
            jax.ShapeDtypeStruct((taps, rows, chan), F32),
        ),
        in_specs=[vmem] * 4,
        out_specs=(anywhere,) * 2,
        scratch_shapes=[pltpu.VMEM((taps, rows, chan), F32), dma((2,))],
        compiler_params=pltpu.CompilerParams(vmem_limit_bytes=8 * 1024 * 1024),
    )(dx, full, std, coef)
    return input_grad, jnp.transpose(weight_grad, (1, 0, 2))


def solution(mesh):
    dims = tuple(mesh.shape[axis] for axis in AXES)
    in_specs = (P(("gx", "gy"), None, None), P("gx", "gy", "gz", None), P("gx", "gy", "gz", None))
    out_specs = (P("gx", "gy", "gz", None), P(("gx", "gy"), None, None))
    return jax.shard_map(
        functools.partial(on_device, dims), mesh=mesh, in_specs=in_specs, out_specs=out_specs, check_vma=False
    )
```

```python
import functools
import itertools

import jax
import jax.numpy as jnp
from jax import lax
from jax.experimental import pallas as pl
from jax.experimental.pallas import tpu as pltpu
from jax.sharding import PartitionSpec as P

var_eps = 1e-05
norm_eps = 1e-06
clip_norm = 600.0
F32 = jnp.float32
BF16 = jnp.bfloat16
MESH = pl.DeviceIdType.MESH
AXES = ("gx", "gy", "gz")


def tap_phases():
    phases = [[(1, 1)], [(1, 0), (1, 2)], [(0, 1), (2, 1)], [(0, 0), (2, 0), (0, 2), (2, 2)]]
    return [[9 * a + 3 * b + c for b, c in phase for a in range(3)] for phase in phases]


def z_groups(nz):
    groups, first, base = [], 0, 0
    for phase in tap_phases():
        left = len(phase)
        while left:
            many = min(8, left)
            size = -(-many // nz)
            groups.append((base, first, many, size))
            first, base, left = first + many, base + size * nz, left - many
    return groups


def tap_slots(nz):
    order = [t for phase in tap_phases() for t in phase]
    slots = [base + v for base, first, many, size in z_groups(nz) for v in range(many)]
    return list(zip(order, slots))


def kernel(dims, raw_hbm, in_hbm, cot_hbm, dx_ref, full, std, coef_ref, *scratch):
    (raw_ref, in_ref, shifted, face_out, face_in, edge_out, edge_in, in_t, part, recv_x, send_y, recv_y, send_z, total_z, recv_z,
     std_all, w_cat, dx_part, stats, stats_in, total_in, load_sem, halo_send, halo_recv, x_send, x_recv, y_send, y_recv,
     z_send, z_recv, g_send, g_recv, ay_send, ay_recv, ax_send, ax_recv, st_send, st_recv, t_send, t_recv) = scratch
    count = dict(zip(AXES, dims))
    nx, ny, nz = dims
    me = {axis: lax.axis_index(axis) for axis in AXES}
    taps, rows, chan = raw_ref.shape
    ex, ey, ez = in_ref.shape[:3]
    groups = z_groups(nz)
    order = [t for t, slot in tap_slots(nz)]
    slots = [slot for t, slot in tap_slots(nz)]
    early = len(tap_phases()[0]) + len(tap_phases()[1])
    fan_count = float(rows * nx * ny * taps)
    wide = 2 if ex % 2 == 0 else 1
    reach = wide + 2
    planes = 2 * wide if ex % (2 * wide) == 0 else wide

    def peer(axis, k):
        return lax.rem(me[axis] + k, count[axis])

    def plane_peer(k):
        flat = lax.rem(me["gx"] * ny + me["gy"] + k, nx * ny)
        return {"gx": lax.div(flat, ny), "gy": lax.rem(flat, ny)}

    def remote(src, dst, send_sem, recv_sem, where):
        return pltpu.make_async_remote_copy(
            src_ref=src, dst_ref=dst, send_sem=send_sem, recv_sem=recv_sem,
            device_id=where, device_id_type=MESH,
        )

    def arrived(ref, sem):
        remote(ref, ref, sem, sem, plane_peer(1)).wait_recv()

    def departed(ref, sem):
        remote(ref, ref, sem, sem, plane_peer(1)).wait_send()

    def inside(step):
        within = None
        for axis, d in zip(AXES, step):
            if d:
                near = me[axis] + d
                ok = near >= 0 if d < 0 else near < count[axis]
                within = ok if within is None else jnp.logical_and(within, ok)
        return within

    def neighbour(step):
        return {axis: lax.min(lax.max(me[axis] + d, 0), count[axis] - 1) for axis, d in zip(AXES, step)}

    body = pl.ds(1, ey)
    load_cot = pltpu.make_async_copy(cot_hbm, shifted.at[1, pl.ds(1, ex), body], load_sem.at[1])
    load_raw = pltpu.make_async_copy(raw_hbm, raw_ref, load_sem.at[0])
    load_in = pltpu.make_async_copy(in_hbm, in_ref, load_sem.at[2])
    load_cot.start()
    load_raw.start()
    load_in.start()

    barrier = pltpu.get_barrier_semaphore()
    greeted = jnp.int32(nx * ny - 1 + nz - 1)
    steps = [[(dx, dy, dz) for dx in xs for dy in ys for dz in zs]
             for xs, ys, zs in [((-1, 1), (0,), (0,)), ((0, -1, 1), (0,), (-1, 1)), ((0, -1, 1), (-1, 1), (0,)),
                                ((0, -1, 1), (-1, 1), (-1, 1))]]
    for step in reversed(steps[1] + steps[3]):
        if step[0] or step[1]:
            near = inside(step)

            @pl.when(near)
            def _(step=step):
                pl.semaphore_signal(barrier, inc=1, device_id=neighbour(step), device_id_type=MESH)

            greeted = greeted + near.astype(jnp.int32)

    for k in range(1, nz):
        pl.semaphore_signal(barrier, inc=1, device_id={"gz": peer("gz", k)}, device_id_type=MESH)
    for k in range(1, nx * ny):
        pl.semaphore_signal(barrier, inc=1, device_id=plane_peer(k), device_id_type=MESH)
    for u in range(0, taps, 3):
        for j in range(wide):
            for p in range(reach):
                if not 0 <= p - j <= 2:
                    w_cat[j * chan:(j + 1) * chan, (u // 3 * reach + p) * chan:(u // 3 * reach + p + 1) * chan] = (
                        jnp.zeros((chan, chan), BF16))
    zero_plane = jnp.zeros((ey + 2, ez, chan), BF16)
    zero_col = jnp.zeros((ex + 2, ez, chan), BF16)
    for axis, edge, x in [("gx", 0, 0), ("gx", nx - 1, ex + 1)]:
        @pl.when(me[axis] == edge)
        def _(x=x):
            shifted[1, x] = zero_plane
            face_in[0, x] = jnp.zeros((ey, chan), BF16)
            face_in[1, x] = jnp.zeros((ey, chan), BF16)
            edge_in[:, :, x] = jnp.zeros((2, 2, 1, chan), F32)

    for axis, edge, y, side in [("gy", 0, 0, 0), ("gy", ny - 1, ey + 1, 1)]:
        @pl.when(me[axis] == edge)
        def _(y=y, side=side):
            shifted[1, :, y] = zero_col
            edge_in[:, side] = jnp.zeros((2, ex + 2, 1, chan), F32)

    for side, edge in [(0, 0), (1, nz - 1)]:
        @pl.when(me["gz"] == edge)
        def _(side=side):
            face_in[side] = jnp.zeros((ex + 2, ey, chan), BF16)
            edge_in[side] = jnp.zeros((2, ex + 2, 1, chan), F32)

    for base, first, many, size in groups:
        for v in range(base + many, base + size * nz):
            send_z[v] = jnp.zeros((rows, chan), BF16)
            total_z[v] = jnp.zeros((rows, chan), F32)
            std[v] = jnp.zeros((rows, chan), F32)

    def per_output(value):
        return jnp.sum(jnp.sum(value, axis=0), axis=0, keepdims=True)

    load_raw.wait()
    raw = raw_ref[...]
    stats[0, 0] = per_output(raw)
    stats[0, 1] = per_output(raw * raw)
    stats[0, 2] = jnp.zeros((1, chan), F32)
    load_cot.wait()
    for x in range(ex):
        plane = shifted[1, x + 1, 1:ey + 1].astype(F32)
        for side, z in [(0, 0), (1, ez - 1)]:
            face_out[side, x] = plane[:, z, :].astype(BF16)
            edge_out[side, 0, x] = plane[0, z:z + 1, :]
            edge_out[side, 1, x] = plane[ey - 1, z:z + 1, :]
    pl.semaphore_wait(barrier, greeted)
    for k in range(1, nx * ny):
        remote(stats.at[0], stats_in.at[k - 1], st_send.at[0], st_recv.at[0], plane_peer(k)).start()

    odd = lax.rem(me["gy"], 2) == 1

    def own_cells(d, extent, base):
        return {-1: pl.ds(base, 1), 0: pl.ds(base, extent), 1: pl.ds(base + extent - 1, 1)}[d]

    def beyond(d, extent):
        return {-1: pl.ds(extent + 1, 1), 0: pl.ds(1, extent), 1: pl.ds(0, 1)}[d]

    def halo_copy(phase, step):
        dx, dy, dz = step
        side = {-1: 0, 0: None, 1: 1}
        if phase == 1:
            pair = face_out.at[side[dz], own_cells(dx, ex, 0)], face_in.at[1 - side[dz], beyond(dx, ex)]
        elif phase == 3:
            pair = (edge_out.at[side[dz], side[dy], own_cells(dx, ex, 0)],
                    edge_in.at[1 - side[dz], 1 - side[dy], beyond(dx, ex)])
        else:
            pair = (shifted.at[1, own_cells(dx, ex, 1), own_cells(dy, ey, 1)],
                    shifted.at[1, beyond(dx, ex), beyond(dy, ey)])
        return remote(*pair, halo_send.at[phase], halo_recv.at[phase], neighbour(step))

    def halo_start(phase, far):
        for step in steps[phase]:
            near = inside(step)
            if far is not None:
                up = odd if step[1] > 0 else jnp.logical_not(odd)
                near = jnp.logical_and(near, up if far else jnp.logical_not(up))
            pl.when(near)(halo_copy(phase, step).start)

    def neighbours(axis):
        total = (me[axis] > 0).astype(jnp.int32) + (me[axis] < count[axis] - 1).astype(jnp.int32)
        return [(n, total == n) for n in ([count[axis] - 1] if count[axis] < 3 else [1, 2])]

    def halo_wait(phase):
        for (i, on_x), (j, on_y), (k, on_z) in itertools.product(*[neighbours(axis) for axis in AXES]):
            along = pl.ds(0, ex + i)
            if phase == 0:
                size, active, others = i, on_x, j == neighbours("gy")[0][0] and k == neighbours("gz")[0][0]
                ref = shifted.at[1, pl.ds(0, i), body]
            elif phase == 1:
                size, active, others = k, jnp.logical_and(on_x, on_z), j == neighbours("gy")[0][0]
                ref = face_in.at[pl.ds(0, k), along]
            elif phase == 2:
                size, active, others = j, jnp.logical_and(on_x, on_y), k == neighbours("gz")[0][0]
                ref = shifted.at[1, along, pl.ds(0, j)]
            else:
                size, active, others = j * k, jnp.logical_and(on_x, jnp.logical_and(on_y, on_z)), True
                ref = edge_in.at[pl.ds(0, k), pl.ds(0, j), along]
            if size and others:
                @pl.when(active)
                def _(ref=ref):
                    departed(ref, halo_send.at[phase])
                    arrived(ref, halo_recv.at[phase])

    halo_start(2, True)
    halo_start(2, False)
    halo_start(0, None)
    halo_start(1, None)
    halo_start(3, True)
    halo_start(3, False)
    load_in.wait()
    for x in range(ex):
        in_t[:, x * ey * ez:(x + 1) * ey * ez] = in_ref[x].reshape(ey * ez, chan).T

    own = std_all.at[me["gx"], me["gy"]]
    spans = [pl.ds(0, early), pl.ds(early, taps - early)]

    def gather_y_start(n):
        mine = own.at[spans[n]]
        for k in range(1, ny):
            remote(mine, mine, ay_send.at[0], ay_recv.at[n], {"gy": peer("gy", k)}).start()

    def gather_x_start(n):
        arrived(std_all.at[0, pl.ds(0, ny - 1), spans[n]], ay_recv.at[n])
        mine = std_all.at[me["gx"], :, spans[n]]
        for k in range(1, nx):
            remote(mine, mine, ax_send.at[0], ax_recv.at[n], {"gx": peer("gx", k)}).start()

    def gather_wait(n):
        arrived(std_all.at[pl.ds(0, nx - 1), :, spans[n]], ax_recv.at[n])


    def view(t, start, planes):
        a, b, c = t // 9, (t // 3) % 3, t % 3
        block = shifted[2 - c, pl.ds(start + 2 - a, planes), 2 - b:2 - b + ey]
        return block.reshape(planes * ey * ez, chan)

    def filter_chunk(g):
        base, first, many, size = groups[g]
        for u in range(first, first + many, 2):
            group = list(range(u, min(u + 2, first + many)))
            views = [view(order[v], 0, ex) for v in group]
            right = jnp.concatenate(views, axis=1) if len(views) > 1 else views[0]
            product = jnp.dot(in_t[...], right, preferred_element_type=F32)
            for j, v in enumerate(group):
                for gx in range(nx):
                    for gy in range(ny):
                        low = (gx * ny + gy) * rows
                        part[gx, gy, v] = product[low:low + rows, j * chan:(j + 1) * chan]
        span = pl.ds(first, many)
        for k in range(1, nx):
            remote(part.at[peer("gx", k), :, span], recv_x.at[k - 1, :, span], x_send.at[0], x_recv.at[g],
                   {"gx": peer("gx", k)}).start()

    def rows_total(gy, span):
        total = part[me["gx"], gy, span]
        for k in range(1, nx):
            total = total + recv_x[k - 1, gy, span]
        return total

    def rows_chunk(g):
        base, first, many, size = groups[g]
        span = pl.ds(first, many)
        arrived(recv_x.at[:, :, span], x_recv.at[g])
        for gy in range(ny):
            send_y[gy, span] = rows_total(gy, span).astype(BF16)
        for k in range(1, ny):
            remote(send_y.at[peer("gy", k), span], recv_y.at[k - 1, span], y_send.at[0], y_recv.at[g],
                   {"gy": peer("gy", k)}).start()

    depth_index = lax.broadcasted_iota(jnp.int32, (ey, ez, chan), 1)
    edge_index = lax.broadcasted_iota(jnp.int32, (ex + 2, ez, chan), 1)
    turns = [(2, 1, ez - 1, ez - 1), (0, 0, 1, 0)]

    def shift_faces():
        for slot, side, amount, last in turns:
            for x in range(ex + 2):
                plane = pltpu.roll(shifted[1, x, 1:ey + 1].astype(F32), amount, 1)
                outer = face_in[side, x].astype(F32)[:, None, :]
                shifted[slot, x, 1:ey + 1] = jnp.where(depth_index == last, outer, plane).astype(BF16)

    def shift_edges():
        for slot, side, amount, last in turns:
            for end, y in [(0, 0), (1, ey + 1)]:
                plane = pltpu.roll(shifted[1, :, y].astype(F32), amount, 1)
                shifted[slot, :, y] = jnp.where(edge_index == last, edge_in[side, end], plane).astype(BF16)

    def depth_start(g):
        base, first, many, size = groups[g]
        span = pl.ds(first, many)
        arrived(recv_y.at[:, span], y_recv.at[g])
        total = rows_total(me["gy"], span)
        for k in range(1, ny):
            total = total + recv_y[k - 1, span].astype(F32)
        total_z[base:base + many] = total
        send_z[base:base + many] = total.astype(BF16)
        for k in range(1, nz):
            remote(send_z.at[pl.ds(base + peer("gz", k) * size, size)], recv_z.at[k - 1, pl.ds(base // nz, size)],
                   z_send.at[0], z_recv.at[g], {"gz": peer("gz", k)}).start()

    def depth_sum(g):
        base, first, many, size = groups[g]
        mine = pl.ds(base + me["gz"] * size, size)
        arrived(recv_z.at[:, pl.ds(base // nz, size)], z_recv.at[g])
        grad = total_z[mine]
        for k in range(1, nz):
            grad = grad + recv_z[k - 1, pl.ds(base // nz, size)].astype(F32)
        full[mine] = grad.astype(BF16)
        return [per_output(grad), per_output(grad * std[mine]), per_output(grad * grad)]

    def gather_start(g):
        base, first, many, size = groups[g]
        mine = pl.ds(base + me["gz"] * size, size)
        for k in range(1, nz):
            remote(full.at[mine], full.at[mine], g_send.at[0], g_recv.at[0], {"gz": peer("gz", k)}).start()

    halo_wait(0)
    filter_chunk(0)
    rows_chunk(0)
    arrived(stats_in, st_recv.at[0])
    sums = stats[0]
    for k in range(nx * ny - 1):
        sums = sums + stats_in[k]
    mean_out = sums[0] / fan_count
    var_out = sums[1] / fan_count - mean_out * mean_out
    inv_std = lax.rsqrt(var_out + var_eps)
    for u, t in enumerate(order):
        value = (raw_ref[t] - mean_out) * inv_std
        std[slots[u]] = value
        own[u] = value.astype(BF16)

    gather_y_start(0)
    halo_wait(1)
    shift_faces()
    filter_chunk(1)
    halo_wait(2)
    filter_chunk(2)
    rows_chunk(1)
    halo_wait(3)
    shift_edges()
    for g in range(3, len(groups)):
        filter_chunk(g)
        rows_chunk(g - 1)
    rows_chunk(len(groups) - 1)
    gather_y_start(1)
    depth_start(0)
    gather_x_start(0)

    def dx_pass(low, high, last):
        span = slice(low * reach * chan // 3, high * reach * chan // 3)
        for u in range(low, high):
            a = order[u] // 9
            for j in range(wide):
                at = (u // 3 * reach + j + 2 - a) * chan
                w_cat[j * chan:(j + 1) * chan, at:at + chan] = std_all[:, :, u].reshape(nx * ny * rows, chan)

        def dx_step(n, carry):
            start = n * planes
            left = []
            for x in range(0, planes, wide):
                strips = []
                for t in order[low:high:3]:
                    b, c = (t // 3) % 3, t % 3
                    for p in range(reach):
                        strips.append(shifted[2 - c, start + x + p, 2 - b:2 - b + ey].reshape(ey * ez, chan))
                left.append(jnp.concatenate(strips, axis=1))
            left = jnp.concatenate(left, axis=0)
            product = lax.dot_general(left, w_cat[:, span], (((1,), (1,)), ((), ())), preferred_element_type=F32)
            for x in range(0, planes, wide):
                for j in range(wide):
                    plane = product[x // wide * ey * ez:(x // wide + 1) * ey * ez, j * chan:(j + 1) * chan]
                    plane = plane.reshape(ey, ez, chan)
                    if last:
                        dx_ref[start + x + j] = (plane + dx_part[start + x + j]).astype(BF16)
                    else:
                        dx_part[start + x + j] = plane
            return carry

        lax.fori_loop(0, ex // planes, dx_step, 0)

    gather_wait(0)
    dx_pass(0, early, False)
    for g in range(1, len(groups)):
        depth_start(g)
    sums = None
    for g in range(len(groups)):
        if g == len(groups) - 1:
            gather_x_start(1)
        new = depth_sum(g)
        sums = new if g == 0 else [a + b for a, b in zip(sums, new)]
        if g < len(groups) - 1:
            gather_start(g)
    for n in range(3):
        stats[1, n] = sums[n]
    flat = (me["gx"] * ny + me["gy"]) * nz + me["gz"]
    total_in[flat] = stats[1]
    for k in range(1, nx * ny * nz):
        other = lax.rem(flat + k, nx * ny * nz)
        where = {
            "gx": lax.div(other, ny * nz),
            "gy": lax.rem(lax.div(other, nz), ny),
            "gz": lax.rem(other, nz),
        }
        remote(stats.at[1], total_in.at[flat], t_send.at[0], t_recv.at[0], where).start()
    gather_start(len(groups) - 1)
    gather_wait(1)
    dx_pass(early, taps, True)
    departed(stats_in, st_send.at[0])
    departed(part.at[pl.ds(0, nx - 1)], x_send.at[0])
    departed(send_y.at[pl.ds(0, ny - 1)], y_send.at[0])
    departed(recv_z, z_send.at[0])
    departed(recv_z, g_send.at[0])
    departed(std_all.at[0, pl.ds(0, ny - 1)], ay_send.at[0])
    departed(std_all.at[pl.ds(0, nx - 1)], ax_send.at[0])
    others = total_in.at[pl.ds(0, nx * ny * nz - 1)]
    departed(others, t_send.at[0])
    arrived(others, t_recv.at[0])
    sums = total_in[0]
    for k in range(1, nx * ny * nz):
        sums = sums + total_in[k]
    sum_grad, sum_cross, sum_square = sums[0], sums[1], sums[2]
    mean_grad = sum_grad / fan_count
    mean_cross = sum_cross / fan_count
    spread = sum_square - 2.0 * mean_grad * sum_grad - 2.0 * mean_cross * sum_cross
    spread = (
        spread
        + fan_count * mean_grad * mean_grad
        + fan_count * mean_cross * mean_cross * var_out / (var_out + var_eps)
    )
    square_sum = jnp.sum(inv_std * inv_std * spread, axis=1, keepdims=True)
    scale = jnp.minimum(1.0, clip_norm * lax.rsqrt(square_sum + norm_eps))
    coef_ref[0:1] = inv_std * scale
    coef_ref[1:2] = mean_grad
    coef_ref[2:3] = mean_cross
    arrived(recv_z, g_recv.at[0])


def finish_kernel(nz, dx_in, full, std, coef_ref, dx_hbm, wg_hbm, wg_ref, sem):
    out_dx = pltpu.make_async_copy(dx_in, dx_hbm, sem.at[0])
    out_dx.start()
    factor, mean_grad, mean_cross = coef_ref[0:1], coef_ref[1:2], coef_ref[2:3]
    for t, slot in tap_slots(nz):
        wg_ref[t] = factor * (full[slot].astype(F32) - mean_grad - std[slot] * mean_cross)
    out_wg = pltpu.make_async_copy(wg_ref, wg_hbm, sem.at[1])
    out_wg.start()
    out_wg.wait()
    out_dx.wait()


def on_device(dims, raw_weight, inputs, cotangent):
    nx, ny, nz = dims
    rows, taps, chan = raw_weight.shape
    ex, ey, ez = inputs.shape[:3]
    groups = z_groups(nz)
    wide = 2 if ex % 2 == 0 else 1
    many = len(groups)
    piece = sum(size for base, first, number, size in groups)
    padded_taps = piece * nz
    stat_slots = nx * ny - 1
    dma = pltpu.SemaphoreType.DMA

    def pair(n, m):
        return [dma((n,)), dma((m,))]

    scratch = [
        pltpu.VMEM((taps, rows, chan), F32),
        pltpu.VMEM(inputs.shape, BF16),
        pltpu.VMEM((3, ex + 2, ey + 2, ez, chan), BF16),
        pltpu.VMEM((2, ex, ey, chan), BF16),
        pltpu.VMEM((2, ex + 2, ey, chan), BF16),
        pltpu.VMEM((2, 2, ex, 1, chan), F32),
        pltpu.VMEM((2, 2, ex + 2, 1, chan), F32),
        pltpu.VMEM((chan, ex * ey * ez), BF16),
        pltpu.VMEM((nx, ny, taps, rows, chan), F32),
        pltpu.VMEM((nx - 1, ny, taps, rows, chan), F32),
        pltpu.VMEM((ny, taps, rows, chan), BF16),
        pltpu.VMEM((ny - 1, taps, rows, chan), BF16),
        pltpu.VMEM((padded_taps, rows, chan), BF16),
        pltpu.VMEM((padded_taps, rows, chan), F32),
        pltpu.VMEM((nz - 1, piece, rows, chan), BF16),
        pltpu.VMEM((nx, ny, taps, rows, chan), BF16),
        pltpu.VMEM((wide * chan, taps // 3 * (wide + 2) * chan), BF16),
        pltpu.VMEM((ex, ey, ez, chan), F32),
        pltpu.VMEM((2, 3, 1, chan), F32),
        pltpu.VMEM((stat_slots, 3, 1, chan), F32),
        pltpu.VMEM((nx * ny * nz, 3, 1, chan), F32),
        dma((3,)), *pair(4, 4), *pair(1, many), *pair(1, many), *pair(1, many), *pair(1, 1), *pair(1, 2), *pair(1, 2),
        *pair(1, 1), *pair(1, 1),
    ]
    vmem = pl.BlockSpec(memory_space=pltpu.VMEM)
    anywhere = pl.BlockSpec(memory_space=pl.ANY)
    operands = (jnp.transpose(raw_weight, (1, 0, 2)), inputs, cotangent)
    dx, full, std, coef = pl.pallas_call(
        functools.partial(kernel, dims),
        out_shape=(
            pltpu.VMEM(cotangent.shape, BF16),
            pltpu.VMEM((padded_taps, rows, chan), BF16),
            pltpu.VMEM((padded_taps, rows, chan), F32),
            pltpu.VMEM((8, chan), F32),
        ),
        in_specs=[anywhere] * 3,
        out_specs=(vmem,) * 4,
        scratch_shapes=scratch,
        compiler_params=pltpu.CompilerParams(
            collective_id=0, has_side_effects=True, vmem_limit_bytes=40 * 1024 * 1024
        ),
    )(*[pltpu.with_memory_space_constraint(v, pltpu.HBM) for v in operands])
    input_grad, weight_grad = pl.pallas_call(
        functools.partial(finish_kernel, nz),
        out_shape=(
            jax.ShapeDtypeStruct(cotangent.shape, BF16),
            jax.ShapeDtypeStruct((taps, rows, chan), F32),
        ),
        in_specs=[vmem] * 4,
        out_specs=(anywhere,) * 2,
        scratch_shapes=[pltpu.VMEM((taps, rows, chan), F32), dma((2,))],
        compiler_params=pltpu.CompilerParams(vmem_limit_bytes=8 * 1024 * 1024),
    )(dx, full, std, coef)
    return input_grad, jnp.transpose(weight_grad, (1, 0, 2))


def solution(mesh):
    dims = tuple(mesh.shape[axis] for axis in AXES)
    in_specs = (P(("gx", "gy"), None, None), P("gx", "gy", "gz", None), P("gx", "gy", "gz", None))
    out_specs = (P("gx", "gy", "gz", None), P(("gx", "gy"), None, None))
    return jax.shard_map(
        functools.partial(on_device, dims), mesh=mesh, in_specs=in_specs, out_specs=out_specs, check_vma=False
    )
```

```python
import functools
import itertools

import jax
import jax.numpy as jnp
from jax import lax
from jax.experimental import pallas as pl
from jax.experimental.pallas import tpu as pltpu
from jax.sharding import PartitionSpec as P

var_eps = 1e-05
norm_eps = 1e-06
clip_norm = 600.0
F32 = jnp.float32
BF16 = jnp.bfloat16
MESH = pl.DeviceIdType.MESH
AXES = ("gx", "gy", "gz")


def tap_order():
    pairs = [(1, 1), (1, 0), (1, 2), (0, 1), (2, 1), (0, 0), (2, 0), (0, 2), (2, 2)]
    return [9 * a + 3 * b + c for b, c in pairs for a in range(3)]


def z_groups(nz):
    groups, first, base = [], 0, 0
    for many in (3, 8, 8, 4, 4):
        size = -(-many // nz)
        groups.append((base, first, many, size))
        first, base = first + many, base + size * nz
    return groups


depth_first = 1


def tap_slots(nz):
    order = tap_order()
    slots = [base + v for base, first, many, size in z_groups(nz) for v in range(many)]
    return list(zip(order, slots))


def kernel(dims, raw_hbm, in_hbm, cot_hbm, dx_ref, full, std, coef_ref, *scratch):
    (raw_ref, in_ref, plain, shifted, in_y, in_z, face_turn, send_a, recv_a, send_b, recv_b, own_b, face_out, face_in, edge_out, edge_in, in_t, part, recv_x, send_y, recv_y, send_z, total_z, recv_z,
     std_all, w_cat, dx_part, stats, stats_in, total_in, load_sem, halo_send, halo_recv, x_send, x_recv, y_send, y_recv,
     z_send, z_recv, g_send, g_recv, ay_send, ay_recv, ax_send, ax_recv, st_send, st_recv, t_send, t_recv) = scratch
    count = dict(zip(AXES, dims))
    nx, ny, nz = dims
    me = {axis: lax.axis_index(axis) for axis in AXES}
    taps, rows, chan = raw_ref.shape
    ex, ey, ez = in_ref.shape[:3]
    groups = z_groups(nz)
    order = [t for t, slot in tap_slots(nz)]
    slots = [slot for t, slot in tap_slots(nz)]
    parts = [(0, taps // 3), (taps // 3, 2 * (taps // 3)), (2 * (taps // 3), taps)]
    fan_count = float(rows * nx * ny * taps)
    wide = 2 if ex % 2 == 0 else 1
    reach = wide + 2
    planes = 2 * wide if ex % (2 * wide) == 0 else wide

    def peer(axis, k):
        return lax.rem(me[axis] + k, count[axis])

    def plane_peer(k):
        flat = lax.rem(me["gx"] * ny + me["gy"] + k, nx * ny)
        return {"gx": lax.div(flat, ny), "gy": lax.rem(flat, ny)}

    def remote(src, dst, send_sem, recv_sem, where):
        return pltpu.make_async_remote_copy(
            src_ref=src, dst_ref=dst, send_sem=send_sem, recv_sem=recv_sem,
            device_id=where, device_id_type=MESH,
        )

    def arrived(ref, sem):
        remote(ref, ref, sem, sem, plane_peer(1)).wait_recv()

    def departed(ref, sem):
        remote(ref, ref, sem, sem, plane_peer(1)).wait_send()

    def inside(step):
        within = None
        for axis, d in zip(AXES, step):
            if d:
                near = me[axis] + d
                ok = near >= 0 if d < 0 else near < count[axis]
                within = ok if within is None else jnp.logical_and(within, ok)
        return within

    def neighbour(step):
        return {axis: lax.min(lax.max(me[axis] + d, 0), count[axis] - 1) for axis, d in zip(AXES, step)}

    body = pl.ds(1, ey)
    load_cot = pltpu.make_async_copy(cot_hbm, plain.at[1, pl.ds(1, ex), body], load_sem.at[1])
    load_more = pltpu.make_async_copy(cot_hbm, shifted.at[1, pl.ds(1, ex), body], load_sem.at[3])
    load_raw = pltpu.make_async_copy(raw_hbm, raw_ref, load_sem.at[0])
    load_in = pltpu.make_async_copy(in_hbm, in_ref, load_sem.at[2])
    load_cot.start()
    load_raw.start()
    load_in.start()
    load_more.start()

    barrier = pltpu.get_barrier_semaphore()
    greeted = jnp.int32(nx * ny - 1 + nz - 1)
    steps = [[(dx, dy, dz) for dx in xs for dy in ys for dz in zs]
             for xs, ys, zs in [((-1, 1), (0,), (0,)), ((0, -1, 1), (0,), (-1, 1)), ((0, -1, 1), (-1, 1), (0,)),
                                ((0, -1, 1), (-1, 1), (-1, 1))]]
    for step in reversed(steps[1] + steps[3]):
        if step[0] or step[1]:
            near = inside(step)

            @pl.when(near)
            def _(step=step):
                pl.semaphore_signal(barrier, inc=1, device_id=neighbour(step), device_id_type=MESH)

            greeted = greeted + near.astype(jnp.int32)

    for k in range(1, nz):
        pl.semaphore_signal(barrier, inc=1, device_id={"gz": peer("gz", k)}, device_id_type=MESH)
    for k in range(1, nx * ny):
        pl.semaphore_signal(barrier, inc=1, device_id=plane_peer(k), device_id_type=MESH)
    for u in range(0, taps, 3):
        for j in range(wide):
            for p in range(reach):
                if not 0 <= p - j <= 2:
                    w_cat[j * chan:(j + 1) * chan, (u // 3 * reach + p) * chan:(u // 3 * reach + p + 1) * chan] = (
                        jnp.zeros((chan, chan), BF16))
    for slot in range(3):
        plain[slot, :, 0] = jnp.zeros((ex + 2, ez, chan), BF16)
        plain[slot, :, ey + 1] = jnp.zeros((ex + 2, ez, chan), BF16)
    zero_col = jnp.zeros((ex + 2, ez, chan), BF16)
    for axis, edge, x in [("gx", 0, 0), ("gx", nx - 1, ex + 1)]:
        @pl.when(me[axis] == edge)
        def _(x=x):
            plain[1, x, 1:ey + 1] = jnp.zeros((ey, ez, chan), BF16)
            shifted[1, x, 0] = jnp.zeros((ez, chan), BF16)
            shifted[1, x, ey + 1] = jnp.zeros((ez, chan), BF16)
            face_in[0, x] = jnp.zeros((ey, chan), BF16)
            face_in[1, x] = jnp.zeros((ey, chan), BF16)
            edge_in[:, :, x] = jnp.zeros((2, 2, 1, chan), F32)

    for axis, edge, y, side in [("gy", 0, 0, 0), ("gy", ny - 1, ey + 1, 1)]:
        @pl.when(me[axis] == edge)
        def _(y=y, side=side):
            shifted[1, :, y] = zero_col
            edge_in[:, side] = jnp.zeros((2, ex + 2, 1, chan), F32)

    for side, edge in [(0, 0), (1, nz - 1)]:
        @pl.when(me["gz"] == edge)
        def _(side=side):
            face_in[side] = jnp.zeros((ex + 2, ey, chan), BF16)
            edge_in[side] = jnp.zeros((2, ex + 2, 1, chan), F32)

    for base, first, many, size in groups:
        for v in range(base + many, base + size * nz):
            send_z[v] = jnp.zeros((rows, chan), BF16)
            total_z[v] = jnp.zeros((rows, chan), F32)
            std[v] = jnp.zeros((rows, chan), F32)

    def per_output(value):
        return jnp.sum(jnp.sum(value, axis=0), axis=0, keepdims=True)

    load_raw.wait()
    raw = raw_ref[...]
    stats[0, 0] = per_output(raw)
    stats[0, 1] = per_output(raw * raw)
    stats[0, 2] = jnp.zeros((1, chan), F32)
    load_cot.wait()
    for x in range(ex):
        plane = plain[1, x + 1, 1:ey + 1].astype(F32)
        for side, z in [(0, 0), (1, ez - 1)]:
            face_out[side, x] = plane[:, z, :].astype(BF16)
            edge_out[side, 0, x] = plane[0, z:z + 1, :]
            edge_out[side, 1, x] = plane[ey - 1, z:z + 1, :]
    pl.semaphore_wait(barrier, greeted)
    for k in range(1, nx * ny):
        remote(stats.at[0], stats_in.at[k - 1], st_send.at[0], st_recv.at[0], plane_peer(k)).start()

    odd = lax.rem(me["gy"], 2) == 1

    def own_cells(d, extent, base):
        return {-1: pl.ds(base, 1), 0: pl.ds(base, extent), 1: pl.ds(base + extent - 1, 1)}[d]

    def beyond(d, extent):
        return {-1: pl.ds(extent + 1, 1), 0: pl.ds(1, extent), 1: pl.ds(0, 1)}[d]

    def halo_copy(phase, step):
        dx, dy, dz = step
        side = {-1: 0, 0: None, 1: 1}
        if phase == 1:
            pair = face_out.at[side[dz], own_cells(dx, ex, 0)], face_in.at[1 - side[dz], beyond(dx, ex)]
        elif phase == 3:
            pair = (edge_out.at[side[dz], side[dy], own_cells(dx, ex, 0)],
                    edge_in.at[1 - side[dz], 1 - side[dy], beyond(dx, ex)])
        else:
            land = plain if phase == 0 else shifted
            pair = (plain.at[1, own_cells(dx, ex, 1), own_cells(dy, ey, 1)],
                    land.at[1, beyond(dx, ex), beyond(dy, ey)])
        return remote(*pair, halo_send.at[phase], halo_recv.at[phase], neighbour(step))

    def halo_start(phase, far):
        for step in steps[phase]:
            near = inside(step)
            if far is not None:
                up = odd if step[1] > 0 else jnp.logical_not(odd)
                near = jnp.logical_and(near, up if far else jnp.logical_not(up))
            pl.when(near)(halo_copy(phase, step).start)

    def neighbours(axis):
        total = (me[axis] > 0).astype(jnp.int32) + (me[axis] < count[axis] - 1).astype(jnp.int32)
        return [(n, total == n) for n in ([count[axis] - 1] if count[axis] < 3 else [1, 2])]

    def halo_wait(phase):
        for (i, on_x), (j, on_y), (k, on_z) in itertools.product(*[neighbours(axis) for axis in AXES]):
            along = pl.ds(0, ex + i)
            if phase == 0:
                size, active, others = i, on_x, j == neighbours("gy")[0][0] and k == neighbours("gz")[0][0]
                ref = plain.at[1, pl.ds(0, i), body]
            elif phase == 1:
                size, active, others = k, jnp.logical_and(on_x, on_z), j == neighbours("gy")[0][0]
                ref = face_in.at[pl.ds(0, k), along]
            elif phase == 2:
                size, active, others = j, jnp.logical_and(on_x, on_y), k == neighbours("gz")[0][0]
                ref = shifted.at[1, along, pl.ds(0, j)]
            else:
                size, active, others = j * k, jnp.logical_and(on_x, jnp.logical_and(on_y, on_z)), True
                ref = edge_in.at[pl.ds(0, k), pl.ds(0, j), along]
            if size and others:
                @pl.when(active)
                def _(ref=ref):
                    departed(ref, halo_send.at[phase])
                    arrived(ref, halo_recv.at[phase])

    halo_start(2, True)
    halo_start(2, False)
    halo_start(0, None)
    halo_start(1, None)
    halo_start(3, True)
    halo_start(3, False)
    load_in.wait()
    for x in range(ex):
        in_t[:, x * ey * ez:(x + 1) * ey * ez] = in_ref[x].reshape(ey * ez, chan).T

    own = std_all.at[me["gx"], me["gy"]]
    spans = [pl.ds(low, high - low) for low, high in parts]

    def gather_y_start(n):
        mine = own.at[spans[n]]
        for k in range(1, ny):
            remote(mine, mine, ay_send.at[0], ay_recv.at[n], {"gy": peer("gy", k)}).start()

    def gather_x_start(n):
        arrived(std_all.at[0, pl.ds(0, ny - 1), spans[n]], ay_recv.at[n])
        mine = std_all.at[me["gx"], :, spans[n]]
        for k in range(1, nx):
            remote(mine, mine, ax_send.at[0], ax_recv.at[n], {"gx": peer("gx", k)}).start()

    def gather_wait(n):
        arrived(std_all.at[pl.ds(0, nx - 1), :, spans[n]], ax_recv.at[n])


    def view(t):
        a, b, c = t // 9, (t // 3) % 3, t % 3
        return plain[2 - c, 2 - a:2 - a + ex, 2 - b:2 - b + ey].reshape(ex * ey * ez, chan)

    def blocks():
        return [(gx, gy, (gx * ny + gy) * rows) for gx in range(nx) for gy in range(ny)]

    def interior(first, last):
        for u in range(first, last, 2):
            group = list(range(u, min(u + 2, last)))
            views = [view(order[v]) for v in group]
            right = jnp.concatenate(views, axis=1) if len(views) > 1 else views[0]
            product = jnp.dot(in_t[...], right, preferred_element_type=F32)
            for j, v in enumerate(group):
                for gx, gy, low in blocks():
                    part[gx, gy, v] = product[low:low + rows, j * chan:(j + 1) * chan]

    def correct(triple):
        b, c = (order[3 * triple] // 3) % 3, order[3 * triple] % 3
        left, right = [], [[] for a in range(3)]
        if b != 1:
            end = b // 2
            left.append(in_y[1 - end])
            for a in range(3):
                right[a].append(shifted[2 - c, 2 - a:2 - a + ex, (1 - end) * (ey + 1)].reshape(ex * ez, chan))
        if c != 1:
            end = c // 2
            left.append(in_z[1 - end])
            for a in range(3):
                face = face_in[1 - end, 2 - a:2 - a + ex] if b == 1 else face_turn[1 - end, b // 2, 2 - a:2 - a + ex]
                right[a].append(face.reshape(ex * ey, chan))
        left = jnp.concatenate(left, axis=1)
        right = jnp.concatenate([jnp.concatenate(strip, axis=0) for strip in right], axis=1)
        product = jnp.dot(left, right, preferred_element_type=F32)
        for a in range(3):
            for gx, gy, low in blocks():
                part[gx, gy, 3 * triple + a] += product[low:low + rows, a * chan:(a + 1) * chan]

    def rows_send(g):
        base, first, many, size = groups[g]
        span = pl.ds(first, many)
        for k in range(1, nx):
            remote(part.at[peer("gx", k), :, span], recv_x.at[k - 1, :, span], x_send.at[0], x_recv.at[g],
                   {"gx": peer("gx", k)}).start()

    def rows_total(gy, span):
        total = part[me["gx"], gy, span]
        for k in range(1, nx):
            total = total + recv_x[k - 1, gy, span]
        return total

    def rows_chunk(g):
        base, first, many, size = groups[g]
        span = pl.ds(first, many)
        arrived(recv_x.at[:, :, span], x_recv.at[g])
        if g == depth_first:
            for gy in range(ny):
                send_a[gy, 0:many] = rows_total(gy, span).astype(BF16)
                for v in range(many, size * nz):
                    send_a[gy, v] = jnp.zeros((rows, chan), BF16)
            for k in range(1, nz):
                remote(send_a.at[:, pl.ds(peer("gz", k) * size, size)], recv_a.at[k - 1], y_send.at[1], y_recv.at[g],
                       {"gz": peer("gz", k)}).start()
            return
        for gy in range(ny):
            send_y[gy, span] = rows_total(gy, span).astype(BF16)
        for k in range(1, ny):
            remote(send_y.at[peer("gy", k), span], recv_y.at[k - 1, span], y_send.at[0], y_recv.at[g],
                   {"gy": peer("gy", k)}).start()

    def depth_middle():
        g = depth_first
        base, first, many, size = groups[g]
        arrived(recv_a, y_recv.at[g])
        mine = pl.ds(me["gz"] * size, size)
        for gy in range(ny):
            total = send_a[gy, mine].astype(F32)
            for k in range(1, nz):
                total = total + recv_a[k - 1, gy].astype(F32)
            own_b[gy] = total
            send_b[gy] = total.astype(BF16)
        for k in range(1, ny):
            remote(send_b.at[peer("gy", k)], recv_b.at[k - 1], z_send.at[1], z_recv.at[g], {"gy": peer("gy", k)}).start()

    depth_index = lax.broadcasted_iota(jnp.int32, (ey, ez, chan), 1)
    edge_index = lax.broadcasted_iota(jnp.int32, (ex + 2, ez, chan), 1)
    row_index = lax.broadcasted_iota(jnp.int32, (ex + 2, ey, chan), 1)
    turns = [(2, 1, ez - 1, ez - 1), (0, 0, 1, 0)]

    def turn_plain(xs):
        for x in xs:
            value = plain[1, x, 1:ey + 1].astype(F32)
            for slot, side, amount, last in turns:
                plane = pltpu.roll(value, amount, 1)
                plain[slot, x, 1:ey + 1] = jnp.where(depth_index == last, 0.0, plane).astype(BF16)

    def turn_faces():
        for side in range(2):
            face = face_in[side].astype(F32)
            for n, amount, last in [(0, ey - 1, ey - 1), (1, 1, 0)]:
                face_turn[side, n] = jnp.where(row_index == last, 0.0, pltpu.roll(face, amount, 1)).astype(BF16)

    def shift_faces():
        for x in (0, ex + 1):
            shifted[1, x, 1:ey + 1] = plain[1, x, 1:ey + 1]
        for slot, side, amount, last in turns:
            for x in range(ex + 2):
                outer = face_in[side, x].astype(F32)[:, None, :]
                plane = plain[slot, x, 1:ey + 1].astype(F32)
                shifted[slot, x, 1:ey + 1] = jnp.where(depth_index == last, outer, plane).astype(BF16)

    def shift_edges():
        for slot, side, amount, last in turns:
            for end, y in [(0, 0), (1, ey + 1)]:
                plane = pltpu.roll(shifted[1, :, y].astype(F32), amount, 1)
                shifted[slot, :, y] = jnp.where(edge_index == last, edge_in[side, end], plane).astype(BF16)

    def depth_start(g):
        base, first, many, size = groups[g]
        span = pl.ds(first, many)
        arrived(recv_y.at[:, span], y_recv.at[g])
        total = rows_total(me["gy"], span)
        for k in range(1, ny):
            total = total + recv_y[k - 1, span].astype(F32)
        total_z[base:base + many] = total
        send_z[base:base + many] = total.astype(BF16)
        for k in range(1, nz):
            remote(send_z.at[pl.ds(base + peer("gz", k) * size, size)], recv_z.at[k - 1, pl.ds(base // nz, size)],
                   z_send.at[0], z_recv.at[g], {"gz": peer("gz", k)}).start()

    def depth_sum(g):
        base, first, many, size = groups[g]
        mine = pl.ds(base + me["gz"] * size, size)
        if g == depth_first:
            arrived(recv_b, z_recv.at[g])
            grad = own_b[me["gy"]]
            for k in range(1, ny):
                grad = grad + recv_b[k - 1].astype(F32)
        else:
            arrived(recv_z.at[:, pl.ds(base // nz, size)], z_recv.at[g])
            grad = total_z[mine]
            for k in range(1, nz):
                grad = grad + recv_z[k - 1, pl.ds(base // nz, size)].astype(F32)
        full[mine] = grad.astype(BF16)
        return [per_output(grad), per_output(grad * std[mine]), per_output(grad * grad)]

    def gather_start(g):
        base, first, many, size = groups[g]
        mine = pl.ds(base + me["gz"] * size, size)
        for k in range(1, nz):
            remote(full.at[mine], full.at[mine], g_send.at[0], g_recv.at[0], {"gz": peer("gz", k)}).start()

    turn_plain(range(1, ex + 1))
    for end, y, z in [(0, 0, 0), (1, ey - 1, ez - 1)]:
        in_y[end] = in_ref[:, y].reshape(ex * ez, chan).T
        in_z[end] = jnp.concatenate([in_ref[x].astype(F32)[:, z, :] for x in range(ex)], axis=0).astype(BF16).T
    halo_wait(0)
    interior(0, 3)
    rows_send(0)
    turn_plain((0, ex + 1))
    interior(3, taps)
    rows_chunk(0)
    arrived(stats_in, st_recv.at[0])
    sums = stats[0]
    for k in range(nx * ny - 1):
        sums = sums + stats_in[k]
    mean_out = sums[0] / fan_count
    var_out = sums[1] / fan_count - mean_out * mean_out
    inv_std = lax.rsqrt(var_out + var_eps)
    for u, t in enumerate(order):
        value = (raw_ref[t] - mean_out) * inv_std
        std[slots[u]] = value
        own[u] = value.astype(BF16)
    gather_y_start(0)
    halo_wait(1)
    turn_faces()
    halo_wait(2)
    load_more.wait()
    halo_wait(3)
    shift_edges()
    done = 3
    for g in range(1, len(groups)):
        base, first, many, size = groups[g]
        while done < first + many:
            correct(done // 3)
            done += 3
        rows_send(g)
    for g in range(1, len(groups)):
        rows_chunk(g)
    gather_y_start(1)
    depth_start(0)
    gather_x_start(0)
    shift_faces()

    def dx_pass(n):
        low, high = parts[n]
        span = slice(low * reach * chan // 3, high * reach * chan // 3)
        for u in range(low, high):
            a = order[u] // 9
            for j in range(wide):
                at = (u // 3 * reach + j + 2 - a) * chan
                w_cat[j * chan:(j + 1) * chan, at:at + chan] = std_all[:, :, u].reshape(nx * ny * rows, chan)

        def dx_step(m, carry):
            start = m * planes
            left = []
            for x in range(0, planes, wide):
                strips = []
                for t in order[low:high:3]:
                    b, c = (t // 3) % 3, t % 3
                    for p in range(reach):
                        strips.append(shifted[2 - c, start + x + p, 2 - b:2 - b + ey].reshape(ey * ez, chan))
                left.append(jnp.concatenate(strips, axis=1))
            left = jnp.concatenate(left, axis=0)
            product = lax.dot_general(left, w_cat[:, span], (((1,), (1,)), ((), ())), preferred_element_type=F32)
            for x in range(0, planes, wide):
                for j in range(wide):
                    plane = product[x // wide * ey * ez:(x // wide + 1) * ey * ez, j * chan:(j + 1) * chan]
                    plane = plane.reshape(ey, ez, chan)
                    if n > 0:
                        plane = plane + dx_part[start + x + j]
                    if n == len(parts) - 1:
                        dx_ref[start + x + j] = plane.astype(BF16)
                    else:
                        dx_part[start + x + j] = plane
            return carry

        lax.fori_loop(0, ex // planes, dx_step, 0)

    gather_wait(0)
    dx_pass(0)
    for g in range(1, len(groups)):
        if g == 3:
            depth_middle()
            gather_y_start(2)
        if g != depth_first:
            depth_start(g)
    late = [g for g in range(len(groups)) if g != depth_first]
    late.insert(len(late) - 1, depth_first)
    sums = None
    for g in late:
        if g == late[-1]:
            gather_x_start(1)
        new = depth_sum(g)
        sums = new if sums is None else [a + b for a, b in zip(sums, new)]
        if g != late[-1]:
            gather_start(g)
    for n in range(3):
        stats[1, n] = sums[n]
    flat = (me["gx"] * ny + me["gy"]) * nz + me["gz"]
    total_in[flat] = stats[1]
    for k in range(1, nx * ny * nz):
        other = lax.rem(flat + k, nx * ny * nz)
        where = {
            "gx": lax.div(other, ny * nz),
            "gy": lax.rem(lax.div(other, nz), ny),
            "gz": lax.rem(other, nz),
        }
        remote(stats.at[1], total_in.at[flat], t_send.at[0], t_recv.at[0], where).start()
    gather_start(late[-1])
    gather_wait(1)
    dx_pass(1)
    gather_x_start(2)
    gather_wait(2)
    dx_pass(2)
    departed(stats_in, st_send.at[0])
    departed(part.at[pl.ds(0, nx - 1)], x_send.at[0])
    base, first, many, size = groups[depth_first]
    departed(recv_a, y_send.at[1])
    departed(recv_b, z_send.at[1])
    departed(send_y.at[pl.ds(0, ny - 1), pl.ds(0, taps - many)], y_send.at[0])
    departed(recv_z.at[:, pl.ds(0, recv_z.shape[1] - size)], z_send.at[0])
    departed(recv_z, g_send.at[0])
    departed(std_all.at[0, pl.ds(0, ny - 1)], ay_send.at[0])
    departed(std_all.at[pl.ds(0, nx - 1)], ax_send.at[0])
    others = total_in.at[pl.ds(0, nx * ny * nz - 1)]
    departed(others, t_send.at[0])
    arrived(others, t_recv.at[0])
    sums = total_in[0]
    for k in range(1, nx * ny * nz):
        sums = sums + total_in[k]
    sum_grad, sum_cross, sum_square = sums[0], sums[1], sums[2]
    mean_grad = sum_grad / fan_count
    mean_cross = sum_cross / fan_count
    spread = sum_square - 2.0 * mean_grad * sum_grad - 2.0 * mean_cross * sum_cross
    spread = (
        spread
        + fan_count * mean_grad * mean_grad
        + fan_count * mean_cross * mean_cross * var_out / (var_out + var_eps)
    )
    square_sum = jnp.sum(inv_std * inv_std * spread, axis=1, keepdims=True)
    scale = jnp.minimum(1.0, clip_norm * lax.rsqrt(square_sum + norm_eps))
    coef_ref[0:1] = inv_std * scale
    coef_ref[1:2] = mean_grad
    coef_ref[2:3] = mean_cross
    arrived(recv_z, g_recv.at[0])


def finish_kernel(nz, dx_in, full, std, coef_ref, dx_hbm, wg_hbm, wg_ref, sem):
    out_dx = pltpu.make_async_copy(dx_in, dx_hbm, sem.at[0])
    out_dx.start()
    factor, mean_grad, mean_cross = coef_ref[0:1], coef_ref[1:2], coef_ref[2:3]
    for t, slot in tap_slots(nz):
        wg_ref[t] = factor * (full[slot].astype(F32) - mean_grad - std[slot] * mean_cross)
    out_wg = pltpu.make_async_copy(wg_ref, wg_hbm, sem.at[1])
    out_wg.start()
    out_wg.wait()
    out_dx.wait()


def on_device(dims, raw_weight, inputs, cotangent):
    nx, ny, nz = dims
    rows, taps, chan = raw_weight.shape
    ex, ey, ez = inputs.shape[:3]
    groups = z_groups(nz)
    wide = 2 if ex % 2 == 0 else 1
    many = len(groups)
    piece = sum(size for base, first, number, size in groups)
    padded_taps = piece * nz
    alone = groups[depth_first][3]
    stat_slots = nx * ny - 1
    dma = pltpu.SemaphoreType.DMA

    def pair(n, m):
        return [dma((n,)), dma((m,))]

    scratch = [
        pltpu.VMEM((taps, rows, chan), F32),
        pltpu.VMEM(inputs.shape, BF16),
        pltpu.VMEM((3, ex + 2, ey + 2, ez, chan), BF16),
        pltpu.VMEM((3, ex + 2, ey + 2, ez, chan), BF16),
        pltpu.VMEM((2, chan, ex * ez), BF16),
        pltpu.VMEM((2, chan, ex * ey), BF16),
        pltpu.VMEM((2, 2, ex + 2, ey, chan), BF16),
        pltpu.VMEM((ny, alone * nz, rows, chan), BF16),
        pltpu.VMEM((nz - 1, ny, alone, rows, chan), BF16),
        pltpu.VMEM((ny, alone, rows, chan), BF16),
        pltpu.VMEM((ny - 1, alone, rows, chan), BF16),
        pltpu.VMEM((ny, alone, rows, chan), F32),
        pltpu.VMEM((2, ex, ey, chan), BF16),
        pltpu.VMEM((2, ex + 2, ey, chan), BF16),
        pltpu.VMEM((2, 2, ex, 1, chan), F32),
        pltpu.VMEM((2, 2, ex + 2, 1, chan), F32),
        pltpu.VMEM((chan, ex * ey * ez), BF16),
        pltpu.VMEM((nx, ny, taps, rows, chan), F32),
        pltpu.VMEM((nx - 1, ny, taps, rows, chan), F32),
        pltpu.VMEM((ny, taps, rows, chan), BF16),
        pltpu.VMEM((ny - 1, taps, rows, chan), BF16),
        pltpu.VMEM((padded_taps, rows, chan), BF16),
        pltpu.VMEM((padded_taps, rows, chan), F32),
        pltpu.VMEM((nz - 1, piece, rows, chan), BF16),
        pltpu.VMEM((nx, ny, taps, rows, chan), BF16),
        pltpu.VMEM((wide * chan, taps // 3 * (wide + 2) * chan), BF16),
        pltpu.VMEM((ex, ey, ez, chan), F32),
        pltpu.VMEM((2, 3, 1, chan), F32),
        pltpu.VMEM((stat_slots, 3, 1, chan), F32),
        pltpu.VMEM((nx * ny * nz, 3, 1, chan), F32),
        dma((4,)), *pair(4, 4), *pair(1, many), *pair(2, many), *pair(2, many), *pair(1, 1), *pair(1, 3), *pair(1, 3),
        *pair(1, 1), *pair(1, 1),
    ]
    vmem = pl.BlockSpec(memory_space=pltpu.VMEM)
    anywhere = pl.BlockSpec(memory_space=pl.ANY)
    operands = (jnp.transpose(raw_weight, (1, 0, 2)), inputs, cotangent)
    dx, full, std, coef = pl.pallas_call(
        functools.partial(kernel, dims),
        out_shape=(
            pltpu.VMEM(cotangent.shape, BF16),
            pltpu.VMEM((padded_taps, rows, chan), BF16),
            pltpu.VMEM((padded_taps, rows, chan), F32),
            pltpu.VMEM((8, chan), F32),
        ),
        in_specs=[anywhere] * 3,
        out_specs=(vmem,) * 4,
        scratch_shapes=scratch,
        compiler_params=pltpu.CompilerParams(
            collective_id=0, has_side_effects=True, vmem_limit_bytes=40 * 1024 * 1024
        ),
    )(*[pltpu.with_memory_space_constraint(v, pltpu.HBM) for v in operands])
    input_grad, weight_grad = pl.pallas_call(
        functools.partial(finish_kernel, nz),
        out_shape=(
            jax.ShapeDtypeStruct(cotangent.shape, BF16),
            jax.ShapeDtypeStruct((taps, rows, chan), F32),
        ),
        in_specs=[vmem] * 4,
        out_specs=(anywhere,) * 2,
        scratch_shapes=[pltpu.VMEM((taps, rows, chan), F32), dma((2,))],
        compiler_params=pltpu.CompilerParams(vmem_limit_bytes=8 * 1024 * 1024),
    )(dx, full, std, coef)
    return input_grad, jnp.transpose(weight_grad, (1, 0, 2))


def solution(mesh):
    dims = tuple(mesh.shape[axis] for axis in AXES)
    in_specs = (P(("gx", "gy"), None, None), P("gx", "gy", "gz", None), P("gx", "gy", "gz", None))
    out_specs = (P("gx", "gy", "gz", None), P(("gx", "gy"), None, None))
    return jax.shard_map(
        functools.partial(on_device, dims), mesh=mesh, in_specs=in_specs, out_specs=out_specs, check_vma=False
    )
```

```python
import functools
import itertools

import jax
import jax.numpy as jnp
from jax import lax
from jax.experimental import pallas as pl
from jax.experimental.pallas import tpu as pltpu
from jax.sharding import PartitionSpec as P

var_eps = 1e-05
norm_eps = 1e-06
clip_norm = 600.0
F32 = jnp.float32
BF16 = jnp.bfloat16
MESH = pl.DeviceIdType.MESH
AXES = ("gx", "gy", "gz")


def tap_order():
    pairs = [(1, 1), (1, 0), (1, 2), (0, 1), (2, 1), (0, 0), (2, 0), (0, 2), (2, 2)]
    return [9 * a + 3 * b + c for b, c in pairs for a in range(3)]


def z_groups(nz):
    groups, first, base = [], 0, 0
    for many in (3, 6, 8, 6, 4):
        size = -(-many // nz)
        groups.append((base, first, many, size))
        first, base = first + many, base + size * nz
    return groups


depth_first = 2


def tap_slots(nz):
    order = tap_order()
    slots = [base + v for base, first, many, size in z_groups(nz) for v in range(many)]
    return list(zip(order, slots))


def kernel(dims, raw_hbm, in_hbm, cot_hbm, dx_ref, full, std, coef_ref, *scratch):
    (raw_ref, in_ref, plain, shifted, in_y, in_z, face_turn, send_a, recv_a, send_b, recv_b, own_b, face_out, face_in, edge_out, edge_in, in_t, part, part_x, recv_x, send_y, recv_y, send_z, total_z, recv_z,
     std_all, w_cat, dx_part, stats, stats_in, total_in, load_sem, halo_send, halo_recv, x_send, x_recv, y_send, y_recv,
     z_send, z_recv, g_send, g_recv, ay_send, ay_recv, ax_send, ax_recv, st_send, st_recv, t_send, t_recv) = scratch
    count = dict(zip(AXES, dims))
    nx, ny, nz = dims
    me = {axis: lax.axis_index(axis) for axis in AXES}
    taps, rows, chan = raw_ref.shape
    ex, ey, ez = in_ref.shape[:3]
    groups = z_groups(nz)
    order = [t for t, slot in tap_slots(nz)]
    slots = [slot for t, slot in tap_slots(nz)]
    parts = [(0, 6), (6, 15), (15, taps)]
    fan_count = float(rows * nx * ny * taps)
    wide = 2 if ex % 2 == 0 else 1
    reach = wide + 2
    planes = 2 * wide if ex % (2 * wide) == 0 else wide

    turned = {axis: [lax.rem(me[axis] + k, count[axis]) for k in range(count[axis])] for axis in AXES}

    def peer(axis, k):
        return turned[axis][k]

    def plane_peer(k):
        flat = lax.rem(me["gx"] * ny + me["gy"] + k, nx * ny)
        return {"gx": lax.div(flat, ny), "gy": lax.rem(flat, ny)}

    def remote(src, dst, send_sem, recv_sem, where):
        return pltpu.make_async_remote_copy(
            src_ref=src, dst_ref=dst, send_sem=send_sem, recv_sem=recv_sem,
            device_id=where, device_id_type=MESH,
        )

    def arrived(ref, sem):
        remote(ref, ref, sem, sem, plane_peer(1)).wait_recv()

    def departed(ref, sem):
        remote(ref, ref, sem, sem, plane_peer(1)).wait_send()

    def inside(step):
        within = None
        for axis, d in zip(AXES, step):
            if d:
                near = me[axis] + d
                ok = near >= 0 if d < 0 else near < count[axis]
                within = ok if within is None else jnp.logical_and(within, ok)
        return within

    def neighbour(step):
        return {axis: lax.min(lax.max(me[axis] + d, 0), count[axis] - 1) for axis, d in zip(AXES, step)}

    body = pl.ds(1, ey)
    load_cot = pltpu.make_async_copy(cot_hbm, plain.at[1, pl.ds(1, ex), body], load_sem.at[1])
    load_more = pltpu.make_async_copy(cot_hbm, shifted.at[1, pl.ds(1, ex), body], load_sem.at[3])
    load_raw = pltpu.make_async_copy(raw_hbm, raw_ref, load_sem.at[0])
    load_in = pltpu.make_async_copy(in_hbm, in_ref, load_sem.at[2])
    load_cot.start()
    load_raw.start()
    load_in.start()
    load_more.start()

    barrier = pltpu.get_barrier_semaphore()
    greeted = jnp.int32(nx * ny - 1 + nz - 1)
    steps = [[(dx, dy, dz) for dx in xs for dy in ys for dz in zs]
             for xs, ys, zs in [((-1, 1), (0,), (0,)), ((0, -1, 1), (0,), (-1, 1)), ((0, -1, 1), (-1, 1), (0,)),
                                ((0, -1, 1), (-1, 1), (-1, 1))]]
    for step in reversed(steps[1] + steps[3]):
        if step[0] or step[1]:
            near = inside(step)

            @pl.when(near)
            def _(step=step):
                pl.semaphore_signal(barrier, inc=1, device_id=neighbour(step), device_id_type=MESH)

            greeted = greeted + near.astype(jnp.int32)

    for k in range(1, nz):
        pl.semaphore_signal(barrier, inc=1, device_id={"gz": peer("gz", k)}, device_id_type=MESH)
    for k in range(1, nx * ny):
        pl.semaphore_signal(barrier, inc=1, device_id=plane_peer(k), device_id_type=MESH)
    for u in range(0, taps, 3):
        for j in range(wide):
            for p in range(reach):
                if not 0 <= p - j <= 2:
                    w_cat[j * chan:(j + 1) * chan, (u // 3 * reach + p) * chan:(u // 3 * reach + p + 1) * chan] = (
                        jnp.zeros((chan, chan), BF16))
    for slot in range(3):
        plain[slot, :, 0] = jnp.zeros((ex + 2, ez, chan), BF16)
        plain[slot, :, ey + 1] = jnp.zeros((ex + 2, ez, chan), BF16)
    zero_col = jnp.zeros((ex + 2, ez, chan), BF16)
    for axis, edge, x in [("gx", 0, 0), ("gx", nx - 1, ex + 1)]:
        @pl.when(me[axis] == edge)
        def _(x=x):
            plain[1, x, 1:ey + 1] = jnp.zeros((ey, ez, chan), BF16)
            shifted[1, x, 0] = jnp.zeros((ez, chan), BF16)
            shifted[1, x, ey + 1] = jnp.zeros((ez, chan), BF16)
            face_in[0, x] = jnp.zeros((ey, chan), BF16)
            face_in[1, x] = jnp.zeros((ey, chan), BF16)
            edge_in[:, :, x] = jnp.zeros((2, 2, 1, chan), F32)

    for axis, edge, y, side in [("gy", 0, 0, 0), ("gy", ny - 1, ey + 1, 1)]:
        @pl.when(me[axis] == edge)
        def _(y=y, side=side):
            shifted[1, :, y] = zero_col
            edge_in[:, side] = jnp.zeros((2, ex + 2, 1, chan), F32)

    for side, edge in [(0, 0), (1, nz - 1)]:
        @pl.when(me["gz"] == edge)
        def _(side=side):
            face_in[side] = jnp.zeros((ex + 2, ey, chan), BF16)
            edge_in[side] = jnp.zeros((2, ex + 2, 1, chan), F32)

    for base, first, many, size in groups:
        for v in range(base + many, base + size * nz):
            send_z[v] = jnp.zeros((rows, chan), BF16)
            total_z[v] = jnp.zeros((rows, chan), F32)
            std[v] = jnp.zeros((rows, chan), F32)

    def per_output(value):
        return jnp.sum(jnp.sum(value, axis=0), axis=0, keepdims=True)

    load_raw.wait()
    raw = raw_ref[...]
    stats[0, 0] = per_output(raw)
    stats[0, 1] = per_output(raw * raw)
    stats[0, 2] = jnp.zeros((1, chan), F32)
    load_cot.wait()
    for x in range(ex):
        plane = plain[1, x + 1, 1:ey + 1].astype(F32)
        for side, z in [(0, 0), (1, ez - 1)]:
            face_out[side, x] = plane[:, z, :].astype(BF16)
            edge_out[side, 0, x] = plane[0, z:z + 1, :]
            edge_out[side, 1, x] = plane[ey - 1, z:z + 1, :]
    pl.semaphore_wait(barrier, greeted)
    for k in range(1, nx * ny):
        remote(stats.at[0], stats_in.at[k - 1], st_send.at[0], st_recv.at[0], plane_peer(k)).start()

    odd = lax.rem(me["gy"], 2) == 1

    def own_cells(d, extent, base):
        return {-1: pl.ds(base, 1), 0: pl.ds(base, extent), 1: pl.ds(base + extent - 1, 1)}[d]

    def beyond(d, extent):
        return {-1: pl.ds(extent + 1, 1), 0: pl.ds(1, extent), 1: pl.ds(0, 1)}[d]

    def halo_copy(phase, step):
        dx, dy, dz = step
        side = {-1: 0, 0: None, 1: 1}
        if phase == 1:
            pair = face_out.at[side[dz], own_cells(dx, ex, 0)], face_in.at[1 - side[dz], beyond(dx, ex)]
        elif phase == 3:
            pair = (edge_out.at[side[dz], side[dy], own_cells(dx, ex, 0)],
                    edge_in.at[1 - side[dz], 1 - side[dy], beyond(dx, ex)])
        else:
            land = plain if phase == 0 else shifted
            pair = (plain.at[1, own_cells(dx, ex, 1), own_cells(dy, ey, 1)],
                    land.at[1, beyond(dx, ex), beyond(dy, ey)])
        return remote(*pair, halo_send.at[phase], halo_recv.at[phase], neighbour(step))

    def halo_start(phase, far):
        for step in steps[phase]:
            near = inside(step)
            if far is not None:
                up = odd if step[1] > 0 else jnp.logical_not(odd)
                near = jnp.logical_and(near, up if far else jnp.logical_not(up))
            pl.when(near)(halo_copy(phase, step).start)

    def neighbours(axis):
        total = (me[axis] > 0).astype(jnp.int32) + (me[axis] < count[axis] - 1).astype(jnp.int32)
        return [(n, total == n) for n in ([count[axis] - 1] if count[axis] < 3 else [1, 2])]

    def halo_wait(phase):
        for (i, on_x), (j, on_y), (k, on_z) in itertools.product(*[neighbours(axis) for axis in AXES]):
            along = pl.ds(0, ex + i)
            if phase == 0:
                size, active, others = i, on_x, j == neighbours("gy")[0][0] and k == neighbours("gz")[0][0]
                ref = plain.at[1, pl.ds(0, i), body]
            elif phase == 1:
                size, active, others = k, jnp.logical_and(on_x, on_z), j == neighbours("gy")[0][0]
                ref = face_in.at[pl.ds(0, k), along]
            elif phase == 2:
                size, active, others = j, jnp.logical_and(on_x, on_y), k == neighbours("gz")[0][0]
                ref = shifted.at[1, along, pl.ds(0, j)]
            else:
                size, active, others = j * k, jnp.logical_and(on_x, jnp.logical_and(on_y, on_z)), True
                ref = edge_in.at[pl.ds(0, k), pl.ds(0, j), along]
            if size and others:
                @pl.when(active)
                def _(ref=ref):
                    departed(ref, halo_send.at[phase])
                    arrived(ref, halo_recv.at[phase])

    halo_start(2, True)
    halo_start(2, False)
    halo_start(0, None)
    halo_start(1, None)
    halo_start(3, True)
    halo_start(3, False)
    load_in.wait()
    for x in range(ex):
        in_t[:, x * ey * ez:(x + 1) * ey * ez] = in_ref[x].reshape(ey * ez, chan).T

    own = std_all.at[me["gx"], me["gy"]]
    spans = [pl.ds(low, high - low) for low, high in parts]

    def gather_y_start(n):
        mine = own.at[spans[n]]
        for k in range(1, ny):
            remote(mine, mine, ay_send.at[0], ay_recv.at[n], {"gy": peer("gy", k)}).start()

    def gather_x_start(n):
        arrived(std_all.at[0, pl.ds(0, ny - 1), spans[n]], ay_recv.at[n])
        mine = std_all.at[me["gx"], :, spans[n]]
        for k in range(1, nx):
            remote(mine, mine, ax_send.at[0], ax_recv.at[n], {"gx": peer("gx", k)}).start()

    def gather_wait(n):
        arrived(std_all.at[pl.ds(0, nx - 1), :, spans[n]], ax_recv.at[n])


    def view(t):
        a, b, c = t // 9, (t // 3) % 3, t % 3
        return plain[2 - c, 2 - a:2 - a + ex, 2 - b:2 - b + ey].reshape(ex * ey * ez, chan)

    def blocks():
        return [(gx, gy, (gx * ny + gy) * rows) for gx in range(nx) for gy in range(ny)]

    def interior(first, last):
        for u in range(first, last, 2):
            group = list(range(u, min(u + 2, last)))
            views = [view(order[v]) for v in group]
            right = jnp.concatenate(views, axis=1) if len(views) > 1 else views[0]
            product = jnp.dot(in_t[...], right, preferred_element_type=F32)
            for j, v in enumerate(group):
                for gx, gy, low in blocks():
                    value = product[low:low + rows, j * chan:(j + 1) * chan]
                    part[gx, gy, v] = value
                    if v < 3:
                        part_x[gx, gy, v] = value.astype(BF16)

    def correct(triple):
        b, c = (order[3 * triple] // 3) % 3, order[3 * triple] % 3
        left, right = [], [[] for a in range(3)]
        if b != 1:
            end = b // 2
            left.append(in_y[1 - end])
            for a in range(3):
                right[a].append(shifted[2 - c, 2 - a:2 - a + ex, (1 - end) * (ey + 1)].reshape(ex * ez, chan))
        if c != 1:
            end = c // 2
            left.append(in_z[1 - end])
            for a in range(3):
                face = face_in[1 - end, 2 - a:2 - a + ex] if b == 1 else face_turn[1 - end, b // 2, 2 - a:2 - a + ex]
                right[a].append(face.reshape(ex * ey, chan))
        left = jnp.concatenate(left, axis=1)
        right = jnp.concatenate([jnp.concatenate(strip, axis=0) for strip in right], axis=1)
        return jnp.dot(left, right, preferred_element_type=F32)

    def correct_all(triples):
        products = [correct(triple) for triple in triples]
        for triple, product in zip(triples, products):
            for a in range(3):
                for gx, gy, low in blocks():
                    value = part[gx, gy, 3 * triple + a] + product[low:low + rows, a * chan:(a + 1) * chan]
                    part[gx, gy, 3 * triple + a] = value
                    part_x[gx, gy, 3 * triple + a] = value.astype(BF16)

    def rows_send(g):
        base, first, many, size = groups[g]
        span = pl.ds(first, many)
        for k in range(1, nx):
            remote(part_x.at[peer("gx", k), :, span], recv_x.at[k - 1, :, span], x_send.at[0], x_recv.at[g],
                   {"gx": peer("gx", k)}).start()

    def rows_total(gy, span):
        total = part[me["gx"], gy, span]
        for k in range(1, nx):
            total = total + recv_x[k - 1, gy, span].astype(F32)
        return total

    def rows_chunk(g):
        base, first, many, size = groups[g]
        span = pl.ds(first, many)
        arrived(recv_x.at[:, :, span], x_recv.at[g])
        if g == depth_first:
            for gy in range(ny):
                send_a[gy, 0:many] = rows_total(gy, span).astype(BF16)
                for v in range(many, size * nz):
                    send_a[gy, v] = jnp.zeros((rows, chan), BF16)
            for k in range(1, nz):
                remote(send_a.at[:, pl.ds(peer("gz", k) * size, size)], recv_a.at[k - 1], y_send.at[1], y_recv.at[g],
                       {"gz": peer("gz", k)}).start()
            return
        for gy in range(ny):
            send_y[gy, span] = rows_total(gy, span).astype(BF16)
        for k in range(1, ny):
            remote(send_y.at[peer("gy", k), span], recv_y.at[k - 1, span], y_send.at[0], y_recv.at[g],
                   {"gy": peer("gy", k)}).start()

    def depth_middle():
        g = depth_first
        base, first, many, size = groups[g]
        arrived(recv_a, y_recv.at[g])
        mine = pl.ds(me["gz"] * size, size)
        for gy in range(ny):
            total = send_a[gy, mine].astype(F32)
            for k in range(1, nz):
                total = total + recv_a[k - 1, gy].astype(F32)
            own_b[gy] = total
            send_b[gy] = total.astype(BF16)
        for k in range(1, ny):
            remote(send_b.at[peer("gy", k)], recv_b.at[k - 1], z_send.at[1], z_recv.at[g], {"gy": peer("gy", k)}).start()

    depth_index = lax.broadcasted_iota(jnp.int32, (ey, ez, chan), 1)
    edge_index = lax.broadcasted_iota(jnp.int32, (ex + 2, ez, chan), 1)
    row_index = lax.broadcasted_iota(jnp.int32, (ex + 2, ey, chan), 1)
    turns = [(2, 1, ez - 1, ez - 1), (0, 0, 1, 0)]

    def turn_plain(xs):
        for x in xs:
            value = plain[1, x, 1:ey + 1].astype(F32)
            for slot, side, amount, last in turns:
                plane = pltpu.roll(value, amount, 1)
                plain[slot, x, 1:ey + 1] = jnp.where(depth_index == last, 0.0, plane).astype(BF16)

    def turn_faces():
        for side in range(2):
            face = face_in[side].astype(F32)
            for n, amount, last in [(0, ey - 1, ey - 1), (1, 1, 0)]:
                face_turn[side, n] = jnp.where(row_index == last, 0.0, pltpu.roll(face, amount, 1)).astype(BF16)

    def shift_faces():
        for x in (0, ex + 1):
            shifted[1, x, 1:ey + 1] = plain[1, x, 1:ey + 1]
        for slot, side, amount, last in turns:
            for x in range(ex + 2):
                outer = face_in[side, x].astype(F32)[:, None, :]
                plane = plain[slot, x, 1:ey + 1].astype(F32)
                shifted[slot, x, 1:ey + 1] = jnp.where(depth_index == last, outer, plane).astype(BF16)

    def shift_edges():
        for slot, side, amount, last in turns:
            for end, y in [(0, 0), (1, ey + 1)]:
                plane = pltpu.roll(shifted[1, :, y].astype(F32), amount, 1)
                shifted[slot, :, y] = jnp.where(edge_index == last, edge_in[side, end], plane).astype(BF16)

    def depth_start(g):
        base, first, many, size = groups[g]
        span = pl.ds(first, many)
        arrived(recv_y.at[:, span], y_recv.at[g])
        total = rows_total(me["gy"], span)
        for k in range(1, ny):
            total = total + recv_y[k - 1, span].astype(F32)
        total_z[base:base + many] = total
        send_z[base:base + many] = total.astype(BF16)
        for k in range(1, nz):
            remote(send_z.at[pl.ds(base + peer("gz", k) * size, size)], recv_z.at[k - 1, pl.ds(base // nz, size)],
                   z_send.at[0], z_recv.at[g], {"gz": peer("gz", k)}).start()

    def depth_sum(g):
        base, first, many, size = groups[g]
        mine = pl.ds(base + me["gz"] * size, size)
        if g == depth_first:
            arrived(recv_b, z_recv.at[g])
            grad = own_b[me["gy"]]
            for k in range(1, ny):
                grad = grad + recv_b[k - 1].astype(F32)
        else:
            arrived(recv_z.at[:, pl.ds(base // nz, size)], z_recv.at[g])
            grad = total_z[mine]
            for k in range(1, nz):
                grad = grad + recv_z[k - 1, pl.ds(base // nz, size)].astype(F32)
        full[mine] = grad.astype(BF16)
        return [per_output(grad), per_output(grad * std[mine]), per_output(grad * grad)]

    def gather_start(g):
        base, first, many, size = groups[g]
        mine = pl.ds(base + me["gz"] * size, size)
        for k in range(1, nz):
            remote(full.at[mine], full.at[mine], g_send.at[0], g_recv.at[0], {"gz": peer("gz", k)}).start()

    turn_plain(range(1, ex + 1))
    for end, y, z in [(0, 0, 0), (1, ey - 1, ez - 1)]:
        in_y[end] = in_ref[:, y].reshape(ex * ez, chan).T
        in_z[end] = jnp.concatenate([in_ref[x].astype(F32)[:, z, :] for x in range(ex)], axis=0).astype(BF16).T
    halo_wait(0)
    interior(0, 3)
    rows_send(0)
    turn_plain((0, ex + 1))
    interior(3, taps)
    rows_chunk(0)
    halo_wait(1)
    turn_faces()
    correct_all(range(1, 3))
    rows_send(1)
    arrived(stats_in, st_recv.at[0])
    sums = stats[0]
    for k in range(nx * ny - 1):
        sums = sums + stats_in[k]
    mean_out = sums[0] / fan_count
    var_out = sums[1] / fan_count - mean_out * mean_out
    inv_std = lax.rsqrt(var_out + var_eps)
    for u, t in enumerate(order):
        value = (raw_ref[t] - mean_out) * inv_std
        std[slots[u]] = value
        own[u] = value.astype(BF16)
    gather_y_start(0)
    halo_wait(2)
    correct_all(range(3, 5))
    halo_wait(3)
    shift_edges()
    correct_all(range(5, 9))
    for g in range(2, len(groups)):
        rows_send(g)
    for g in range(1, len(groups)):
        rows_chunk(g)
    gather_y_start(1)
    depth_start(0)
    gather_x_start(0)
    load_more.wait()
    shift_faces()

    def dx_pass(n):
        low, high = parts[n]
        span = slice(low * reach * chan // 3, high * reach * chan // 3)
        for u in range(low, high):
            a = order[u] // 9
            for j in range(wide):
                at = (u // 3 * reach + j + 2 - a) * chan
                w_cat[j * chan:(j + 1) * chan, at:at + chan] = std_all[:, :, u].reshape(nx * ny * rows, chan)

        def dx_step(m, carry):
            start = m * planes
            left = []
            for x in range(0, planes, wide):
                strips = []
                for t in order[low:high:3]:
                    b, c = (t // 3) % 3, t % 3
                    for p in range(reach):
                        strips.append(shifted[2 - c, start + x + p, 2 - b:2 - b + ey].reshape(ey * ez, chan))
                left.append(jnp.concatenate(strips, axis=1))
            left = jnp.concatenate(left, axis=0)
            product = lax.dot_general(left, w_cat[:, span], (((1,), (1,)), ((), ())), preferred_element_type=F32)
            for x in range(0, planes, wide):
                for j in range(wide):
                    plane = product[x // wide * ey * ez:(x // wide + 1) * ey * ez, j * chan:(j + 1) * chan]
                    plane = plane.reshape(ey, ez, chan)
                    if n > 0:
                        plane = plane + dx_part[start + x + j]
                    if n == len(parts) - 1:
                        dx_ref[start + x + j] = plane.astype(BF16)
                    else:
                        dx_part[start + x + j] = plane
            return carry

        lax.fori_loop(0, ex // planes, dx_step, 0)

    gather_wait(0)
    dx_pass(0)
    for g in range(1, len(groups)):
        if g != depth_first:
            depth_start(g)
    depth_middle()
    gather_y_start(2)
    late = [g for g in range(len(groups)) if g != depth_first]
    late.append(depth_first)
    sums = None
    for g in late:
        new = depth_sum(g)
        if g == 1:
            gather_x_start(1)
        sums = new if sums is None else [a + b for a, b in zip(sums, new)]
        if g != late[-1]:
            gather_start(g)
    for n in range(3):
        stats[1, n] = sums[n]
    flat = (me["gx"] * ny + me["gy"]) * nz + me["gz"]
    total_in[flat] = stats[1]
    for dz in sorted(range(nz), key=lambda k: -min(k, nz - k)):
        for dx in range(nx):
            for dy in range(ny):
                if dx or dy or dz:
                    where = {"gx": peer("gx", dx), "gy": peer("gy", dy), "gz": peer("gz", dz)}
                    remote(stats.at[1], total_in.at[flat], t_send.at[0], t_recv.at[0], where).start()
    gather_start(late[-1])
    gather_x_start(2)
    gather_wait(1)
    dx_pass(1)
    gather_wait(2)
    dx_pass(2)
    departed(stats_in, st_send.at[0])
    departed(part_x.at[pl.ds(0, nx - 1)], x_send.at[0])
    base, first, many, size = groups[depth_first]
    departed(recv_a, y_send.at[1])
    departed(recv_b, z_send.at[1])
    departed(send_y.at[pl.ds(0, ny - 1), pl.ds(0, taps - many)], y_send.at[0])
    departed(recv_z.at[:, pl.ds(0, recv_z.shape[1] - size)], z_send.at[0])
    departed(recv_z, g_send.at[0])
    departed(std_all.at[0, pl.ds(0, ny - 1)], ay_send.at[0])
    departed(std_all.at[pl.ds(0, nx - 1)], ax_send.at[0])
    others = total_in.at[pl.ds(0, nx * ny * nz - 1)]
    departed(others, t_send.at[0])
    arrived(others, t_recv.at[0])
    sums = total_in[0]
    for k in range(1, nx * ny * nz):
        sums = sums + total_in[k]
    sum_grad, sum_cross, sum_square = sums[0], sums[1], sums[2]
    mean_grad = sum_grad / fan_count
    mean_cross = sum_cross / fan_count
    spread = sum_square - 2.0 * mean_grad * sum_grad - 2.0 * mean_cross * sum_cross
    spread = (
        spread
        + fan_count * mean_grad * mean_grad
        + fan_count * mean_cross * mean_cross * var_out / (var_out + var_eps)
    )
    square_sum = jnp.sum(inv_std * inv_std * spread, axis=1, keepdims=True)
    scale = jnp.minimum(1.0, clip_norm * lax.rsqrt(square_sum + norm_eps))
    coef_ref[0:1] = inv_std * scale
    coef_ref[1:2] = mean_grad
    coef_ref[2:3] = mean_cross
    arrived(recv_z, g_recv.at[0])


def finish_kernel(nz, dx_in, full, std, coef_ref, dx_hbm, wg_hbm, wg_ref, sem):
    out_dx = pltpu.make_async_copy(dx_in, dx_hbm, sem.at[0])
    out_dx.start()
    factor, mean_grad, mean_cross = coef_ref[0:1], coef_ref[1:2], coef_ref[2:3]
    for t, slot in tap_slots(nz):
        wg_ref[t] = factor * (full[slot].astype(F32) - mean_grad - std[slot] * mean_cross)
    out_wg = pltpu.make_async_copy(wg_ref, wg_hbm, sem.at[1])
    out_wg.start()
    out_wg.wait()
    out_dx.wait()


def on_device(dims, raw_weight, inputs, cotangent):
    nx, ny, nz = dims
    rows, taps, chan = raw_weight.shape
    ex, ey, ez = inputs.shape[:3]
    groups = z_groups(nz)
    wide = 2 if ex % 2 == 0 else 1
    many = len(groups)
    piece = sum(size for base, first, number, size in groups)
    padded_taps = piece * nz
    alone = groups[depth_first][3]
    stat_slots = nx * ny - 1
    dma = pltpu.SemaphoreType.DMA

    def pair(n, m):
        return [dma((n,)), dma((m,))]

    scratch = [
        pltpu.VMEM((taps, rows, chan), F32),
        pltpu.VMEM(inputs.shape, BF16),
        pltpu.VMEM((3, ex + 2, ey + 2, ez, chan), BF16),
        pltpu.VMEM((3, ex + 2, ey + 2, ez, chan), BF16),
        pltpu.VMEM((2, chan, ex * ez), BF16),
        pltpu.VMEM((2, chan, ex * ey), BF16),
        pltpu.VMEM((2, 2, ex + 2, ey, chan), BF16),
        pltpu.VMEM((ny, alone * nz, rows, chan), BF16),
        pltpu.VMEM((nz - 1, ny, alone, rows, chan), BF16),
        pltpu.VMEM((ny, alone, rows, chan), BF16),
        pltpu.VMEM((ny - 1, alone, rows, chan), BF16),
        pltpu.VMEM((ny, alone, rows, chan), F32),
        pltpu.VMEM((2, ex, ey, chan), BF16),
        pltpu.VMEM((2, ex + 2, ey, chan), BF16),
        pltpu.VMEM((2, 2, ex, 1, chan), F32),
        pltpu.VMEM((2, 2, ex + 2, 1, chan), F32),
        pltpu.VMEM((chan, ex * ey * ez), BF16),
        pltpu.VMEM((nx, ny, taps, rows, chan), F32),
        pltpu.VMEM((nx, ny, taps, rows, chan), BF16),
        pltpu.VMEM((nx - 1, ny, taps, rows, chan), BF16),
        pltpu.VMEM((ny, taps, rows, chan), BF16),
        pltpu.VMEM((ny - 1, taps, rows, chan), BF16),
        pltpu.VMEM((padded_taps, rows, chan), BF16),
        pltpu.VMEM((padded_taps, rows, chan), F32),
        pltpu.VMEM((nz - 1, piece, rows, chan), BF16),
        pltpu.VMEM((nx, ny, taps, rows, chan), BF16),
        pltpu.VMEM((wide * chan, taps // 3 * (wide + 2) * chan), BF16),
        pltpu.VMEM((ex, ey, ez, chan), F32),
        pltpu.VMEM((2, 3, 1, chan), F32),
        pltpu.VMEM((stat_slots, 3, 1, chan), F32),
        pltpu.VMEM((nx * ny * nz, 3, 1, chan), F32),
        dma((4,)), *pair(4, 4), *pair(1, many), *pair(2, many), *pair(2, many), *pair(1, 1), *pair(1, 3), *pair(1, 3),
        *pair(1, 1), *pair(1, 1),
    ]
    vmem = pl.BlockSpec(memory_space=pltpu.VMEM)
    anywhere = pl.BlockSpec(memory_space=pl.ANY)
    operands = (jnp.transpose(raw_weight, (1, 0, 2)), inputs, cotangent)
    dx, full, std, coef = pl.pallas_call(
        functools.partial(kernel, dims),
        out_shape=(
            pltpu.VMEM(cotangent.shape, BF16),
            pltpu.VMEM((padded_taps, rows, chan), BF16),
            pltpu.VMEM((padded_taps, rows, chan), F32),
            pltpu.VMEM((8, chan), F32),
        ),
        in_specs=[anywhere] * 3,
        out_specs=(vmem,) * 4,
        scratch_shapes=scratch,
        compiler_params=pltpu.CompilerParams(
            collective_id=0, has_side_effects=True, vmem_limit_bytes=40 * 1024 * 1024
        ),
    )(*[pltpu.with_memory_space_constraint(v, pltpu.HBM) for v in operands])
    input_grad, weight_grad = pl.pallas_call(
        functools.partial(finish_kernel, nz),
        out_shape=(
            jax.ShapeDtypeStruct(cotangent.shape, BF16),
            jax.ShapeDtypeStruct((taps, rows, chan), F32),
        ),
        in_specs=[vmem] * 4,
        out_specs=(anywhere,) * 2,
        scratch_shapes=[pltpu.VMEM((taps, rows, chan), F32), dma((2,))],
        compiler_params=pltpu.CompilerParams(vmem_limit_bytes=8 * 1024 * 1024),
    )(dx, full, std, coef)
    return input_grad, jnp.transpose(weight_grad, (1, 0, 2))


def solution(mesh):
    dims = tuple(mesh.shape[axis] for axis in AXES)
    in_specs = (P(("gx", "gy"), None, None), P("gx", "gy", "gz", None), P("gx", "gy", "gz", None))
    out_specs = (P("gx", "gy", "gz", None), P(("gx", "gy"), None, None))
    return jax.shard_map(
        functools.partial(on_device, dims), mesh=mesh, in_specs=in_specs, out_specs=out_specs, check_vma=False
    )
```

```python
import functools
import itertools

import jax
import jax.numpy as jnp
from jax import lax
from jax.experimental import pallas as pl
from jax.experimental.pallas import tpu as pltpu
from jax.sharding import PartitionSpec as P

var_eps = 1e-05
norm_eps = 1e-06
clip_norm = 600.0
F32 = jnp.float32
BF16 = jnp.bfloat16
MESH = pl.DeviceIdType.MESH
AXES = ("gx", "gy", "gz")


def tap_order():
    pairs = [(1, 1), (1, 0), (1, 2), (0, 1), (2, 1), (0, 0), (2, 0), (0, 2), (2, 2)]
    return [9 * a + 3 * b + c for b, c in pairs for a in range(3)]


def z_groups(nz):
    groups, first, base = [], 0, 0
    for many in (3, 6, 8, 6, 4):
        size = -(-many // nz)
        groups.append((base, first, many, size))
        first, base = first + many, base + size * nz
    return groups


depth_first = 2


def tap_slots(nz):
    order = tap_order()
    slots = [base + v for base, first, many, size in z_groups(nz) for v in range(many)]
    return list(zip(order, slots))


def kernel(dims, raw_hbm, in_hbm, cot_hbm, dx_ref, full, std, coef_ref, *scratch):
    (raw_ref, in_ref, plain, shifted, in_y, in_z, face_turn, send_a, recv_a, send_b, recv_b, own_b, face_out, face_in, edge_out, edge_in, in_t, part, part_x, recv_x, send_y, recv_y, send_z, total_z, recv_z,
     std_all, w_cat, dx_part, stats, stats_in, total_in, load_sem, halo_send, halo_recv, x_send, x_recv, y_send, y_recv,
     z_send, z_recv, g_send, g_recv, ay_send, ay_recv, ax_send, ax_recv, st_send, st_recv, t_send, t_recv) = scratch
    count = dict(zip(AXES, dims))
    nx, ny, nz = dims
    me = {axis: lax.axis_index(axis) for axis in AXES}
    taps, rows, chan = raw_ref.shape
    ex, ey, ez = in_ref.shape[:3]
    groups = z_groups(nz)
    order = [t for t, slot in tap_slots(nz)]
    slots = [slot for t, slot in tap_slots(nz)]
    parts = [(0, 6), (6, 18), (18, taps)]
    fan_count = float(rows * nx * ny * taps)
    wide = 2 if ex % 2 == 0 else 1
    reach = wide + 2
    planes = 2 * wide if ex % (2 * wide) == 0 else wide

    turned = {axis: [lax.rem(me[axis] + k, count[axis]) for k in range(count[axis])] for axis in AXES}

    def peer(axis, k):
        return turned[axis][k]

    def plane_peer(k):
        flat = lax.rem(me["gx"] * ny + me["gy"] + k, nx * ny)
        return {"gx": lax.div(flat, ny), "gy": lax.rem(flat, ny)}

    def remote(src, dst, send_sem, recv_sem, where):
        return pltpu.make_async_remote_copy(
            src_ref=src, dst_ref=dst, send_sem=send_sem, recv_sem=recv_sem,
            device_id=where, device_id_type=MESH,
        )

    def arrived(ref, sem):
        remote(ref, ref, sem, sem, plane_peer(1)).wait_recv()

    def departed(ref, sem):
        remote(ref, ref, sem, sem, plane_peer(1)).wait_send()

    def inside(step):
        within = None
        for axis, d in zip(AXES, step):
            if d:
                near = me[axis] + d
                ok = near >= 0 if d < 0 else near < count[axis]
                within = ok if within is None else jnp.logical_and(within, ok)
        return within

    def neighbour(step):
        return {axis: lax.min(lax.max(me[axis] + d, 0), count[axis] - 1) for axis, d in zip(AXES, step)}

    body = pl.ds(1, ey)
    load_cot = pltpu.make_async_copy(cot_hbm, plain.at[1, pl.ds(1, ex), body], load_sem.at[1])
    load_more = pltpu.make_async_copy(cot_hbm, shifted.at[1, pl.ds(1, ex), body], load_sem.at[3])
    load_raw = pltpu.make_async_copy(raw_hbm, raw_ref, load_sem.at[0])
    load_in = pltpu.make_async_copy(in_hbm, in_ref, load_sem.at[2])
    load_cot.start()
    load_raw.start()
    load_in.start()
    load_more.start()

    barrier = pltpu.get_barrier_semaphore()
    greeted = jnp.int32(nx * ny - 1 + nz - 1)
    steps = [[(dx, dy, dz) for dx in xs for dy in ys for dz in zs]
             for xs, ys, zs in [((-1, 1), (0,), (0,)), ((0, -1, 1), (0,), (-1, 1)), ((0, -1, 1), (-1, 1), (0,)),
                                ((0, -1, 1), (-1, 1), (-1, 1))]]
    for step in reversed(steps[1] + steps[3]):
        if step[0] or step[1]:
            near = inside(step)

            @pl.when(near)
            def _(step=step):
                pl.semaphore_signal(barrier, inc=1, device_id=neighbour(step), device_id_type=MESH)

            greeted = greeted + near.astype(jnp.int32)

    for k in range(1, nz):
        pl.semaphore_signal(barrier, inc=1, device_id={"gz": peer("gz", k)}, device_id_type=MESH)
    for k in range(1, nx * ny):
        pl.semaphore_signal(barrier, inc=1, device_id=plane_peer(k), device_id_type=MESH)
    for u in range(0, taps, 3):
        for j in range(wide):
            for p in range(reach):
                if not 0 <= p - j <= 2:
                    w_cat[j * chan:(j + 1) * chan, (u // 3 * reach + p) * chan:(u // 3 * reach + p + 1) * chan] = (
                        jnp.zeros((chan, chan), BF16))
    for slot in range(3):
        plain[slot, :, 0] = jnp.zeros((ex + 2, ez, chan), BF16)
        plain[slot, :, ey + 1] = jnp.zeros((ex + 2, ez, chan), BF16)
    zero_col = jnp.zeros((ex + 2, ez, chan), BF16)
    for axis, edge, x in [("gx", 0, 0), ("gx", nx - 1, ex + 1)]:
        @pl.when(me[axis] == edge)
        def _(x=x):
            plain[1, x, 1:ey + 1] = jnp.zeros((ey, ez, chan), BF16)
            shifted[1, x, 0] = jnp.zeros((ez, chan), BF16)
            shifted[1, x, ey + 1] = jnp.zeros((ez, chan), BF16)
            face_in[0, x] = jnp.zeros((ey, chan), BF16)
            face_in[1, x] = jnp.zeros((ey, chan), BF16)
            edge_in[:, :, x] = jnp.zeros((2, 2, 1, chan), F32)

    for axis, edge, y, side in [("gy", 0, 0, 0), ("gy", ny - 1, ey + 1, 1)]:
        @pl.when(me[axis] == edge)
        def _(y=y, side=side):
            shifted[1, :, y] = zero_col
            edge_in[:, side] = jnp.zeros((2, ex + 2, 1, chan), F32)

    for side, edge in [(0, 0), (1, nz - 1)]:
        @pl.when(me["gz"] == edge)
        def _(side=side):
            face_in[side] = jnp.zeros((ex + 2, ey, chan), BF16)
            edge_in[side] = jnp.zeros((2, ex + 2, 1, chan), F32)

    for base, first, many, size in groups:
        for v in range(base + many, base + size * nz):
            send_z[v] = jnp.zeros((rows, chan), BF16)
            total_z[v] = jnp.zeros((rows, chan), F32)
            std[v] = jnp.zeros((rows, chan), F32)

    def per_output(value):
        return jnp.sum(jnp.sum(value, axis=0), axis=0, keepdims=True)

    load_raw.wait()
    raw = raw_ref[...]
    stats[0, 0] = per_output(raw)
    stats[0, 1] = per_output(raw * raw)
    stats[0, 2] = jnp.zeros((1, chan), F32)
    load_cot.wait()
    for x in range(ex):
        plane = plain[1, x + 1, 1:ey + 1].astype(F32)
        for side, z in [(0, 0), (1, ez - 1)]:
            face_out[side, x] = plane[:, z, :].astype(BF16)
            edge_out[side, 0, x] = plane[0, z:z + 1, :]
            edge_out[side, 1, x] = plane[ey - 1, z:z + 1, :]
    pl.semaphore_wait(barrier, greeted)
    for k in range(1, nx * ny):
        remote(stats.at[0], stats_in.at[k - 1], st_send.at[0], st_recv.at[0], plane_peer(k)).start()

    odd = lax.rem(me["gy"], 2) == 1

    def own_cells(d, extent, base):
        return {-1: pl.ds(base, 1), 0: pl.ds(base, extent), 1: pl.ds(base + extent - 1, 1)}[d]

    def beyond(d, extent):
        return {-1: pl.ds(extent + 1, 1), 0: pl.ds(1, extent), 1: pl.ds(0, 1)}[d]

    def halo_copy(phase, step):
        dx, dy, dz = step
        side = {-1: 0, 0: None, 1: 1}
        if phase == 1:
            pair = face_out.at[side[dz], own_cells(dx, ex, 0)], face_in.at[1 - side[dz], beyond(dx, ex)]
        elif phase == 3:
            pair = (edge_out.at[side[dz], side[dy], own_cells(dx, ex, 0)],
                    edge_in.at[1 - side[dz], 1 - side[dy], beyond(dx, ex)])
        else:
            land = plain if phase == 0 else shifted
            pair = (plain.at[1, own_cells(dx, ex, 1), own_cells(dy, ey, 1)],
                    land.at[1, beyond(dx, ex), beyond(dy, ey)])
        return remote(*pair, halo_send.at[phase], halo_recv.at[phase], neighbour(step))

    def halo_start(phase, far):
        for step in steps[phase]:
            near = inside(step)
            if far is not None:
                up = odd if step[1] > 0 else jnp.logical_not(odd)
                near = jnp.logical_and(near, up if far else jnp.logical_not(up))
            pl.when(near)(halo_copy(phase, step).start)

    def neighbours(axis):
        total = (me[axis] > 0).astype(jnp.int32) + (me[axis] < count[axis] - 1).astype(jnp.int32)
        return [(n, total == n) for n in ([count[axis] - 1] if count[axis] < 3 else [1, 2])]

    def halo_wait(phase):
        for (i, on_x), (j, on_y), (k, on_z) in itertools.product(*[neighbours(axis) for axis in AXES]):
            along = pl.ds(0, ex + i)
            if phase == 0:
                size, active, others = i, on_x, j == neighbours("gy")[0][0] and k == neighbours("gz")[0][0]
                ref = plain.at[1, pl.ds(0, i), body]
            elif phase == 1:
                size, active, others = k, jnp.logical_and(on_x, on_z), j == neighbours("gy")[0][0]
                ref = face_in.at[pl.ds(0, k), along]
            elif phase == 2:
                size, active, others = j, jnp.logical_and(on_x, on_y), k == neighbours("gz")[0][0]
                ref = shifted.at[1, along, pl.ds(0, j)]
            else:
                size, active, others = j * k, jnp.logical_and(on_x, jnp.logical_and(on_y, on_z)), True
                ref = edge_in.at[pl.ds(0, k), pl.ds(0, j), along]
            if size and others:
                @pl.when(active)
                def _(ref=ref):
                    departed(ref, halo_send.at[phase])
                    arrived(ref, halo_recv.at[phase])

    halo_start(2, True)
    halo_start(2, False)
    halo_start(0, None)
    halo_start(1, None)
    halo_start(3, True)
    halo_start(3, False)
    load_in.wait()
    for x in range(ex):
        in_t[:, x * ey * ez:(x + 1) * ey * ez] = in_ref[x].reshape(ey * ez, chan).T

    own = std_all.at[me["gx"], me["gy"]]
    spans = [pl.ds(low, high - low) for low, high in parts]

    def gather_y_start(n):
        mine = own.at[spans[n]]
        for k in range(1, ny):
            remote(mine, mine, ay_send.at[0], ay_recv.at[n], {"gy": peer("gy", k)}).start()

    def gather_x_start(n):
        arrived(std_all.at[0, pl.ds(0, ny - 1), spans[n]], ay_recv.at[n])
        mine = std_all.at[me["gx"], :, spans[n]]
        for k in range(1, nx):
            remote(mine, mine, ax_send.at[0], ax_recv.at[n], {"gx": peer("gx", k)}).start()

    def gather_wait(n):
        arrived(std_all.at[pl.ds(0, nx - 1), :, spans[n]], ax_recv.at[n])


    def view(t):
        a, b, c = t // 9, (t // 3) % 3, t % 3
        return plain[2 - c, 2 - a:2 - a + ex, 2 - b:2 - b + ey].reshape(ex * ey * ez, chan)

    def blocks():
        return [(gx, gy, (gx * ny + gy) * rows) for gx in range(nx) for gy in range(ny)]

    def interior(first, last):
        for u in range(first, last, 2):
            group = list(range(u, min(u + 2, last)))
            views = [view(order[v]) for v in group]
            right = jnp.concatenate(views, axis=1) if len(views) > 1 else views[0]
            product = jnp.dot(in_t[...], right, preferred_element_type=F32)
            for j, v in enumerate(group):
                for gx, gy, low in blocks():
                    value = product[low:low + rows, j * chan:(j + 1) * chan]
                    part[gx, gy, v] = value
                    if v < 3:
                        part_x[gx, gy, v] = value.astype(BF16)

    def correct(triple):
        b, c = (order[3 * triple] // 3) % 3, order[3 * triple] % 3
        left, right = [], [[] for a in range(3)]
        if b != 1:
            end = b // 2
            left.append(in_y[1 - end])
            for a in range(3):
                right[a].append(shifted[2 - c, 2 - a:2 - a + ex, (1 - end) * (ey + 1)].reshape(ex * ez, chan))
        if c != 1:
            end = c // 2
            left.append(in_z[1 - end])
            for a in range(3):
                face = face_in[1 - end, 2 - a:2 - a + ex] if b == 1 else face_turn[1 - end, b // 2, 2 - a:2 - a + ex]
                right[a].append(face.reshape(ex * ey, chan))
        left = jnp.concatenate(left, axis=1)
        right = jnp.concatenate([jnp.concatenate(strip, axis=0) for strip in right], axis=1)
        return jnp.dot(left, right, preferred_element_type=F32)

    def correct_all(triples):
        products = [correct(triple) for triple in triples]
        for triple, product in zip(triples, products):
            for a in range(3):
                for gx, gy, low in blocks():
                    value = part[gx, gy, 3 * triple + a] + product[low:low + rows, a * chan:(a + 1) * chan]
                    part[gx, gy, 3 * triple + a] = value
                    part_x[gx, gy, 3 * triple + a] = value.astype(BF16)

    def rows_send(g):
        base, first, many, size = groups[g]
        span = pl.ds(first, many)
        for k in range(1, nx):
            remote(part_x.at[peer("gx", k), :, span], recv_x.at[k - 1, :, span], x_send.at[0], x_recv.at[g],
                   {"gx": peer("gx", k)}).start()

    def rows_total(gy, span):
        total = part[me["gx"], gy, span]
        for k in range(1, nx):
            total = total + recv_x[k - 1, gy, span].astype(F32)
        return total

    def rows_chunk(g):
        base, first, many, size = groups[g]
        span = pl.ds(first, many)
        arrived(recv_x.at[:, :, span], x_recv.at[g])
        if g == depth_first:
            for gy in range(ny):
                send_a[gy, 0:many] = rows_total(gy, span).astype(BF16)
                for v in range(many, size * nz):
                    send_a[gy, v] = jnp.zeros((rows, chan), BF16)
            for k in range(1, nz):
                remote(send_a.at[:, pl.ds(peer("gz", k) * size, size)], recv_a.at[k - 1], y_send.at[1], y_recv.at[g],
                       {"gz": peer("gz", k)}).start()
            return
        for gy in range(ny):
            send_y[gy, span] = rows_total(gy, span).astype(BF16)
        for k in range(1, ny):
            remote(send_y.at[peer("gy", k), span], recv_y.at[k - 1, span], y_send.at[0], y_recv.at[g],
                   {"gy": peer("gy", k)}).start()

    def depth_middle():
        g = depth_first
        base, first, many, size = groups[g]
        arrived(recv_a, y_recv.at[g])
        mine = pl.ds(me["gz"] * size, size)
        for gy in range(ny):
            total = send_a[gy, mine].astype(F32)
            for k in range(1, nz):
                total = total + recv_a[k - 1, gy].astype(F32)
            own_b[gy] = total
            send_b[gy] = total.astype(BF16)
        for k in range(1, ny):
            remote(send_b.at[peer("gy", k)], recv_b.at[k - 1], z_send.at[1], z_recv.at[g], {"gy": peer("gy", k)}).start()

    def middle_sums():
        base, first, many, size = groups[depth_first]
        mine_std = pl.ds(first + me["gz"] * size, size)
        plain_sum, cross_sum = 0.0, 0.0
        for gy in range(ny):
            plain_sum = plain_sum + own_b[gy]
            cross_sum = cross_sum + own_b[gy] * std_all[me["gx"], gy, mine_std].astype(F32)
        return [per_output(plain_sum), per_output(cross_sum)]

    depth_index = lax.broadcasted_iota(jnp.int32, (ey, ez, chan), 1)
    edge_index = lax.broadcasted_iota(jnp.int32, (ex + 2, ez, chan), 1)
    row_index = lax.broadcasted_iota(jnp.int32, (ex + 2, ey, chan), 1)
    turns = [(2, 1, ez - 1, ez - 1), (0, 0, 1, 0)]

    def turn_plain(xs):
        for x in xs:
            value = plain[1, x, 1:ey + 1].astype(F32)
            for slot, side, amount, last in turns:
                plane = pltpu.roll(value, amount, 1)
                plain[slot, x, 1:ey + 1] = jnp.where(depth_index == last, 0.0, plane).astype(BF16)

    def turn_faces():
        for side in range(2):
            face = face_in[side].astype(F32)
            for n, amount, last in [(0, ey - 1, ey - 1), (1, 1, 0)]:
                face_turn[side, n] = jnp.where(row_index == last, 0.0, pltpu.roll(face, amount, 1)).astype(BF16)

    def shift_faces():
        for x in (0, ex + 1):
            shifted[1, x, 1:ey + 1] = plain[1, x, 1:ey + 1]
        for slot, side, amount, last in turns:
            for x in range(ex + 2):
                outer = face_in[side, x].astype(F32)[:, None, :]
                plane = plain[slot, x, 1:ey + 1].astype(F32)
                shifted[slot, x, 1:ey + 1] = jnp.where(depth_index == last, outer, plane).astype(BF16)

    def shift_edges():
        for slot, side, amount, last in turns:
            for end, y in [(0, 0), (1, ey + 1)]:
                plane = pltpu.roll(shifted[1, :, y].astype(F32), amount, 1)
                shifted[slot, :, y] = jnp.where(edge_index == last, edge_in[side, end], plane).astype(BF16)

    def depth_start(g):
        base, first, many, size = groups[g]
        span = pl.ds(first, many)
        arrived(recv_y.at[:, span], y_recv.at[g])
        total = rows_total(me["gy"], span)
        for k in range(1, ny):
            total = total + recv_y[k - 1, span].astype(F32)
        total_z[base:base + many] = total
        send_z[base:base + many] = total.astype(BF16)
        for k in range(1, nz):
            remote(send_z.at[pl.ds(base + peer("gz", k) * size, size)], recv_z.at[k - 1, pl.ds(base // nz, size)],
                   z_send.at[0], z_recv.at[g], {"gz": peer("gz", k)}).start()
        return [per_output(total), per_output(total * std[base:base + many])]

    def depth_sum(g):
        base, first, many, size = groups[g]
        mine = pl.ds(base + me["gz"] * size, size)
        if g == depth_first:
            arrived(recv_b, z_recv.at[g])
            grad = own_b[me["gy"]]
            for k in range(1, ny):
                grad = grad + recv_b[k - 1].astype(F32)
        else:
            arrived(recv_z.at[:, pl.ds(base // nz, size)], z_recv.at[g])
            grad = total_z[mine]
            for k in range(1, nz):
                grad = grad + recv_z[k - 1, pl.ds(base // nz, size)].astype(F32)
        full[mine] = grad.astype(BF16)
        return per_output(grad * grad)

    def gather_start(g):
        base, first, many, size = groups[g]
        mine = pl.ds(base + me["gz"] * size, size)
        for k in range(1, nz):
            remote(full.at[mine], full.at[mine], g_send.at[0], g_recv.at[0], {"gz": peer("gz", k)}).start()

    turn_plain(range(1, ex + 1))
    for end, y, z in [(0, 0, 0), (1, ey - 1, ez - 1)]:
        in_y[end] = in_ref[:, y].reshape(ex * ez, chan).T
        in_z[end] = jnp.concatenate([in_ref[x].astype(F32)[:, z, :] for x in range(ex)], axis=0).astype(BF16).T
    halo_wait(0)
    interior(0, 3)
    rows_send(0)
    turn_plain((0, ex + 1))
    interior(3, taps)
    rows_chunk(0)
    halo_wait(1)
    turn_faces()
    correct_all(range(1, 3))
    rows_send(1)
    arrived(stats_in, st_recv.at[0])
    sums = stats[0]
    for k in range(nx * ny - 1):
        sums = sums + stats_in[k]
    mean_out = sums[0] / fan_count
    var_out = sums[1] / fan_count - mean_out * mean_out
    inv_std = lax.rsqrt(var_out + var_eps)
    for u, t in enumerate(order):
        value = (raw_ref[t] - mean_out) * inv_std
        std[slots[u]] = value
        own[u] = value.astype(BF16)
    gather_y_start(0)
    halo_wait(2)
    correct_all(range(3, 5))
    halo_wait(3)
    shift_edges()
    correct_all(range(5, 9))
    for g in range(2, len(groups)):
        rows_send(g)
    for g in range(1, len(groups)):
        rows_chunk(g)
    gather_y_start(1)
    linear = [depth_start(0)]
    gather_x_start(0)
    load_more.wait()
    shift_faces()

    def dx_pass(n):
        low, high = parts[n]
        span = slice(low * reach * chan // 3, high * reach * chan // 3)
        for u in range(low, high):
            a = order[u] // 9
            for j in range(wide):
                at = (u // 3 * reach + j + 2 - a) * chan
                w_cat[j * chan:(j + 1) * chan, at:at + chan] = std_all[:, :, u].reshape(nx * ny * rows, chan)

        def dx_step(m, carry):
            start = m * planes
            left = []
            for x in range(0, planes, wide):
                strips = []
                for t in order[low:high:3]:
                    b, c = (t // 3) % 3, t % 3
                    for p in range(reach):
                        strips.append(shifted[2 - c, start + x + p, 2 - b:2 - b + ey].reshape(ey * ez, chan))
                left.append(jnp.concatenate(strips, axis=1))
            left = jnp.concatenate(left, axis=0)
            product = lax.dot_general(left, w_cat[:, span], (((1,), (1,)), ((), ())), preferred_element_type=F32)
            for x in range(0, planes, wide):
                for j in range(wide):
                    plane = product[x // wide * ey * ez:(x // wide + 1) * ey * ez, j * chan:(j + 1) * chan]
                    plane = plane.reshape(ey, ez, chan)
                    if n > 0:
                        plane = plane + dx_part[start + x + j]
                    if n == len(parts) - 1:
                        dx_ref[start + x + j] = plane.astype(BF16)
                    else:
                        dx_part[start + x + j] = plane
            return carry

        lax.fori_loop(0, ex // planes, dx_step, 0)

    for g in range(1, len(groups)):
        if g != depth_first:
            linear.append(depth_start(g))
    depth_middle()
    gather_y_start(2)
    gather_wait(0)
    dx_pass(0)
    late = [g for g in range(len(groups)) if g != depth_first]
    late.append(depth_first)
    flat = (me["gx"] * ny + me["gy"]) * nz + me["gz"]

    def everywhere(span, n):
        mine = total_in.at[flat, span]
        for dz in sorted(range(nz), key=lambda k: -min(k, nz - k)):
            for dx in range(nx):
                for dy in range(ny):
                    if dx or dy or dz:
                        where = {"gx": peer("gx", dx), "gy": peer("gy", dy), "gz": peer("gz", dz)}
                        remote(stats.at[1, span], mine, t_send.at[n], t_recv.at[n], where).start()

    squares = None
    for g in late:
        new = depth_sum(g)
        squares = new if squares is None else squares + new
        if g == 1:
            gather_x_start(1)
            linear.append(middle_sums())
            for n in range(2):
                stats[1, n] = sum(pair[n] for pair in linear)
            everywhere(pl.ds(0, 2), 0)
        if g != late[-1]:
            gather_start(g)
    stats[1, 2] = squares
    total_in[flat] = stats[1]
    everywhere(pl.ds(2, 1), 1)
    gather_start(late[-1])
    gather_x_start(2)
    gather_wait(1)
    dx_pass(1)
    gather_wait(2)
    dx_pass(2)
    departed(stats_in, st_send.at[0])
    departed(part_x.at[pl.ds(0, nx - 1)], x_send.at[0])
    base, first, many, size = groups[depth_first]
    departed(recv_a, y_send.at[1])
    departed(recv_b, z_send.at[1])
    departed(send_y.at[pl.ds(0, ny - 1), pl.ds(0, taps - many)], y_send.at[0])
    departed(recv_z.at[:, pl.ds(0, recv_z.shape[1] - size)], z_send.at[0])
    departed(recv_z, g_send.at[0])
    departed(std_all.at[0, pl.ds(0, ny - 1)], ay_send.at[0])
    departed(std_all.at[pl.ds(0, nx - 1)], ax_send.at[0])
    others = [total_in.at[pl.ds(0, nx * ny * nz - 1), pl.ds(0, 2)], total_in.at[pl.ds(0, nx * ny * nz - 1), pl.ds(2, 1)]]
    departed(others[0], t_send.at[0])
    departed(others[1], t_send.at[1])
    arrived(others[0], t_recv.at[0])
    sums = total_in[0, 0:2]
    for k in range(1, nx * ny * nz):
        sums = sums + total_in[k, 0:2]
    sum_grad, sum_cross = sums[0], sums[1]
    arrived(others[1], t_recv.at[1])
    sum_square = total_in[0, 2]
    for k in range(1, nx * ny * nz):
        sum_square = sum_square + total_in[k, 2]
    mean_grad = sum_grad / fan_count
    mean_cross = sum_cross / fan_count
    spread = sum_square - 2.0 * mean_grad * sum_grad - 2.0 * mean_cross * sum_cross
    spread = (
        spread
        + fan_count * mean_grad * mean_grad
        + fan_count * mean_cross * mean_cross * var_out / (var_out + var_eps)
    )
    square_sum = jnp.sum(inv_std * inv_std * spread, axis=1, keepdims=True)
    scale = jnp.minimum(1.0, clip_norm * lax.rsqrt(square_sum + norm_eps))
    coef_ref[0:1] = inv_std * scale
    coef_ref[1:2] = mean_grad
    coef_ref[2:3] = mean_cross
    arrived(recv_z, g_recv.at[0])


def finish_kernel(nz, dx_in, full, std, coef_ref, dx_hbm, wg_hbm, wg_ref, sem):
    out_dx = pltpu.make_async_copy(dx_in, dx_hbm, sem.at[0])
    out_dx.start()
    factor, mean_grad, mean_cross = coef_ref[0:1], coef_ref[1:2], coef_ref[2:3]
    for t, slot in tap_slots(nz):
        wg_ref[t] = factor * (full[slot].astype(F32) - mean_grad - std[slot] * mean_cross)
    out_wg = pltpu.make_async_copy(wg_ref, wg_hbm, sem.at[1])
    out_wg.start()
    out_wg.wait()
    out_dx.wait()


def on_device(dims, raw_weight, inputs, cotangent):
    nx, ny, nz = dims
    rows, taps, chan = raw_weight.shape
    ex, ey, ez = inputs.shape[:3]
    groups = z_groups(nz)
    wide = 2 if ex % 2 == 0 else 1
    many = len(groups)
    piece = sum(size for base, first, number, size in groups)
    padded_taps = piece * nz
    alone = groups[depth_first][3]
    stat_slots = nx * ny - 1
    dma = pltpu.SemaphoreType.DMA

    def pair(n, m):
        return [dma((n,)), dma((m,))]

    scratch = [
        pltpu.VMEM((taps, rows, chan), F32),
        pltpu.VMEM(inputs.shape, BF16),
        pltpu.VMEM((3, ex + 2, ey + 2, ez, chan), BF16),
        pltpu.VMEM((3, ex + 2, ey + 2, ez, chan), BF16),
        pltpu.VMEM((2, chan, ex * ez), BF16),
        pltpu.VMEM((2, chan, ex * ey), BF16),
        pltpu.VMEM((2, 2, ex + 2, ey, chan), BF16),
        pltpu.VMEM((ny, alone * nz, rows, chan), BF16),
        pltpu.VMEM((nz - 1, ny, alone, rows, chan), BF16),
        pltpu.VMEM((ny, alone, rows, chan), BF16),
        pltpu.VMEM((ny - 1, alone, rows, chan), BF16),
        pltpu.VMEM((ny, alone, rows, chan), F32),
        pltpu.VMEM((2, ex, ey, chan), BF16),
        pltpu.VMEM((2, ex + 2, ey, chan), BF16),
        pltpu.VMEM((2, 2, ex, 1, chan), F32),
        pltpu.VMEM((2, 2, ex + 2, 1, chan), F32),
        pltpu.VMEM((chan, ex * ey * ez), BF16),
        pltpu.VMEM((nx, ny, taps, rows, chan), F32),
        pltpu.VMEM((nx, ny, taps, rows, chan), BF16),
        pltpu.VMEM((nx - 1, ny, taps, rows, chan), BF16),
        pltpu.VMEM((ny, taps, rows, chan), BF16),
        pltpu.VMEM((ny - 1, taps, rows, chan), BF16),
        pltpu.VMEM((padded_taps, rows, chan), BF16),
        pltpu.VMEM((padded_taps, rows, chan), F32),
        pltpu.VMEM((nz - 1, piece, rows, chan), BF16),
        pltpu.VMEM((nx, ny, taps, rows, chan), BF16),
        pltpu.VMEM((wide * chan, taps // 3 * (wide + 2) * chan), BF16),
        pltpu.VMEM((ex, ey, ez, chan), F32),
        pltpu.VMEM((2, 3, 1, chan), F32),
        pltpu.VMEM((stat_slots, 3, 1, chan), F32),
        pltpu.VMEM((nx * ny * nz, 3, 1, chan), F32),
        dma((4,)), *pair(4, 4), *pair(1, many), *pair(2, many), *pair(2, many), *pair(1, 1), *pair(1, 3), *pair(1, 3),
        *pair(1, 1), *pair(2, 2),
    ]
    vmem = pl.BlockSpec(memory_space=pltpu.VMEM)
    anywhere = pl.BlockSpec(memory_space=pl.ANY)
    operands = (jnp.transpose(raw_weight, (1, 0, 2)), inputs, cotangent)
    dx, full, std, coef = pl.pallas_call(
        functools.partial(kernel, dims),
        out_shape=(
            pltpu.VMEM(cotangent.shape, BF16),
            pltpu.VMEM((padded_taps, rows, chan), BF16),
            pltpu.VMEM((padded_taps, rows, chan), F32),
            pltpu.VMEM((8, chan), F32),
        ),
        in_specs=[anywhere] * 3,
        out_specs=(vmem,) * 4,
        scratch_shapes=scratch,
        compiler_params=pltpu.CompilerParams(
            collective_id=0, has_side_effects=True, vmem_limit_bytes=40 * 1024 * 1024
        ),
    )(*[pltpu.with_memory_space_constraint(v, pltpu.HBM) for v in operands])
    input_grad, weight_grad = pl.pallas_call(
        functools.partial(finish_kernel, nz),
        out_shape=(
            jax.ShapeDtypeStruct(cotangent.shape, BF16),
            jax.ShapeDtypeStruct((taps, rows, chan), F32),
        ),
        in_specs=[vmem] * 4,
        out_specs=(anywhere,) * 2,
        scratch_shapes=[pltpu.VMEM((taps, rows, chan), F32), dma((2,))],
        compiler_params=pltpu.CompilerParams(vmem_limit_bytes=8 * 1024 * 1024),
    )(dx, full, std, coef)
    return input_grad, jnp.transpose(weight_grad, (1, 0, 2))


def solution(mesh):
    dims = tuple(mesh.shape[axis] for axis in AXES)
    in_specs = (P(("gx", "gy"), None, None), P("gx", "gy", "gz", None), P("gx", "gy", "gz", None))
    out_specs = (P("gx", "gy", "gz", None), P(("gx", "gy"), None, None))
    return jax.shard_map(
        functools.partial(on_device, dims), mesh=mesh, in_specs=in_specs, out_specs=out_specs, check_vma=False
    )
```

```python
import functools
import itertools

import jax
import jax.numpy as jnp
from jax import lax
from jax.experimental import pallas as pl
from jax.experimental.pallas import tpu as pltpu
from jax.sharding import PartitionSpec as P

var_eps = 1e-05
norm_eps = 1e-06
clip_norm = 600.0
F32 = jnp.float32
BF16 = jnp.bfloat16
MESH = pl.DeviceIdType.MESH
AXES = ("gx", "gy", "gz")


def tap_order():
    pairs = [(1, 1), (1, 0), (1, 2), (0, 1), (2, 1), (0, 0), (2, 0), (0, 2), (2, 2)]
    return [9 * a + 3 * b + c for b, c in pairs for a in range(3)]


def z_groups(nz):
    groups, first, base = [], 0, 0
    for many in (3, 6, 8, 6, 4):
        size = -(-many // nz)
        groups.append((base, first, many, size))
        first, base = first + many, base + size * nz
    return groups


depth_first = 2


def tap_slots(nz):
    order = tap_order()
    slots = [base + v for base, first, many, size in z_groups(nz) for v in range(many)]
    return list(zip(order, slots))


def kernel(dims, raw_hbm, in_hbm, cot_hbm, dx_ref, full, std, coef_ref, *scratch):
    (raw_ref, in_ref, plain, shifted, in_y, in_z, face_turn, send_a, recv_a, send_b, recv_b, own_b, face_out, face_in, edge_out, edge_in, in_t, part, part_x, recv_x, send_y, recv_y, send_z, total_z, recv_z,
     std_all, w_cat, dx_part, stats, stats_in, total_in, load_sem, halo_send, halo_recv, x_send, x_recv, y_send, y_recv,
     z_send, z_recv, g_send, g_recv, ay_send, ay_recv, ax_send, ax_recv, st_send, st_recv, t_send, t_recv) = scratch
    count = dict(zip(AXES, dims))
    nx, ny, nz = dims
    me = {axis: lax.axis_index(axis) for axis in AXES}
    taps, rows, chan = raw_ref.shape
    ex, ey, ez = in_ref.shape[:3]
    groups = z_groups(nz)
    order = [t for t, slot in tap_slots(nz)]
    slots = [slot for t, slot in tap_slots(nz)]
    parts = [(0, 6), (6, 18), (18, taps)]
    fan_count = float(rows * nx * ny * taps)
    wide = 2 if ex % 2 == 0 else 1
    reach = wide + 2
    planes = 2 * wide if ex % (2 * wide) == 0 else wide

    turned = {axis: [lax.rem(me[axis] + k, count[axis]) for k in range(count[axis])] for axis in AXES}

    def peer(axis, k):
        return turned[axis][k]

    def plane_peer(k):
        flat = lax.rem(me["gx"] * ny + me["gy"] + k, nx * ny)
        return {"gx": lax.div(flat, ny), "gy": lax.rem(flat, ny)}

    def remote(src, dst, send_sem, recv_sem, where):
        return pltpu.make_async_remote_copy(
            src_ref=src, dst_ref=dst, send_sem=send_sem, recv_sem=recv_sem,
            device_id=where, device_id_type=MESH,
        )

    def arrived(ref, sem):
        remote(ref, ref, sem, sem, plane_peer(1)).wait_recv()

    def departed(ref, sem):
        remote(ref, ref, sem, sem, plane_peer(1)).wait_send()

    def inside(step):
        within = None
        for axis, d in zip(AXES, step):
            if d:
                near = me[axis] + d
                ok = near >= 0 if d < 0 else near < count[axis]
                within = ok if within is None else jnp.logical_and(within, ok)
        return within

    def neighbour(step):
        return {axis: lax.min(lax.max(me[axis] + d, 0), count[axis] - 1) for axis, d in zip(AXES, step)}

    body = pl.ds(1, ey)
    load_cot = pltpu.make_async_copy(cot_hbm, plain.at[1, pl.ds(1, ex), body], load_sem.at[1])
    load_more = pltpu.make_async_copy(cot_hbm, shifted.at[1, pl.ds(1, ex), body], load_sem.at[3])
    load_raw = pltpu.make_async_copy(raw_hbm, raw_ref, load_sem.at[0])
    load_in = pltpu.make_async_copy(in_hbm, in_ref, load_sem.at[2])
    load_cot.start()
    load_raw.start()
    load_in.start()
    load_more.start()

    barrier = pltpu.get_barrier_semaphore()
    greeted = jnp.int32(nx * ny - 1 + nz - 1)
    steps = [[(dx, dy, dz) for dx in xs for dy in ys for dz in zs]
             for xs, ys, zs in [((-1, 1), (0,), (0,)), ((0, -1, 1), (0,), (-1, 1)), ((0, -1, 1), (-1, 1), (0,)),
                                ((0, -1, 1), (-1, 1), (-1, 1))]]
    for step in reversed(steps[1] + steps[3]):
        if step[0] or step[1]:
            near = inside(step)

            @pl.when(near)
            def _(step=step):
                pl.semaphore_signal(barrier, inc=1, device_id=neighbour(step), device_id_type=MESH)

            greeted = greeted + near.astype(jnp.int32)

    for k in range(1, nz):
        pl.semaphore_signal(barrier, inc=1, device_id={"gz": peer("gz", k)}, device_id_type=MESH)
    for k in range(1, nx * ny):
        pl.semaphore_signal(barrier, inc=1, device_id=plane_peer(k), device_id_type=MESH)
    for u in range(0, taps, 3):
        for j in range(wide):
            for p in range(reach):
                if not 0 <= p - j <= 2:
                    w_cat[j * chan:(j + 1) * chan, (u // 3 * reach + p) * chan:(u // 3 * reach + p + 1) * chan] = (
                        jnp.zeros((chan, chan), BF16))
    for slot in range(3):
        plain[slot, :, 0] = jnp.zeros((ex + 2, ez, chan), BF16)
        plain[slot, :, ey + 1] = jnp.zeros((ex + 2, ez, chan), BF16)
    zero_col = jnp.zeros((ex + 2, ez, chan), BF16)
    for axis, edge, x in [("gx", 0, 0), ("gx", nx - 1, ex + 1)]:
        @pl.when(me[axis] == edge)
        def _(x=x):
            plain[1, x, 1:ey + 1] = jnp.zeros((ey, ez, chan), BF16)
            shifted[1, x, 0] = jnp.zeros((ez, chan), BF16)
            shifted[1, x, ey + 1] = jnp.zeros((ez, chan), BF16)
            face_in[0, x] = jnp.zeros((ey, chan), BF16)
            face_in[1, x] = jnp.zeros((ey, chan), BF16)
            edge_in[:, :, x] = jnp.zeros((2, 2, 1, chan), F32)

    for axis, edge, y, side in [("gy", 0, 0, 0), ("gy", ny - 1, ey + 1, 1)]:
        @pl.when(me[axis] == edge)
        def _(y=y, side=side):
            shifted[1, :, y] = zero_col
            edge_in[:, side] = jnp.zeros((2, ex + 2, 1, chan), F32)

    for side, edge in [(0, 0), (1, nz - 1)]:
        @pl.when(me["gz"] == edge)
        def _(side=side):
            face_in[side] = jnp.zeros((ex + 2, ey, chan), BF16)
            edge_in[side] = jnp.zeros((2, ex + 2, 1, chan), F32)

    for base, first, many, size in groups:
        for v in range(base + many, base + size * nz):
            send_z[v] = jnp.zeros((rows, chan), BF16)
            total_z[v] = jnp.zeros((rows, chan), F32)
            std[v] = jnp.zeros((rows, chan), F32)

    def per_output(value):
        return jnp.sum(jnp.sum(value, axis=0), axis=0, keepdims=True)

    load_raw.wait()
    raw = raw_ref[...]
    stats[0, 0] = per_output(raw)
    stats[0, 1] = per_output(raw * raw)
    stats[0, 2] = jnp.zeros((1, chan), F32)
    load_cot.wait()
    for x in range(ex):
        plane = plain[1, x + 1, 1:ey + 1].astype(F32)
        for side, z in [(0, 0), (1, ez - 1)]:
            face_out[side, x] = plane[:, z, :].astype(BF16)
            edge_out[side, 0, x] = plane[0, z:z + 1, :]
            edge_out[side, 1, x] = plane[ey - 1, z:z + 1, :]
    pl.semaphore_wait(barrier, greeted)
    for k in range(1, nx * ny):
        remote(stats.at[0], stats_in.at[k - 1], st_send.at[0], st_recv.at[0], plane_peer(k)).start()

    odd = lax.rem(me["gy"], 2) == 1

    def own_cells(d, extent, base):
        return {-1: pl.ds(base, 1), 0: pl.ds(base, extent), 1: pl.ds(base + extent - 1, 1)}[d]

    def beyond(d, extent):
        return {-1: pl.ds(extent + 1, 1), 0: pl.ds(1, extent), 1: pl.ds(0, 1)}[d]

    def halo_copy(phase, step):
        dx, dy, dz = step
        side = {-1: 0, 0: None, 1: 1}
        if phase == 1:
            pair = face_out.at[side[dz], own_cells(dx, ex, 0)], face_in.at[1 - side[dz], beyond(dx, ex)]
        elif phase == 3:
            pair = (edge_out.at[side[dz], side[dy], own_cells(dx, ex, 0)],
                    edge_in.at[1 - side[dz], 1 - side[dy], beyond(dx, ex)])
        else:
            land = plain if phase == 0 else shifted
            pair = (plain.at[1, own_cells(dx, ex, 1), own_cells(dy, ey, 1)],
                    land.at[1, beyond(dx, ex), beyond(dy, ey)])
        return remote(*pair, halo_send.at[phase], halo_recv.at[phase], neighbour(step))

    def halo_start(phase, far):
        for step in steps[phase]:
            near = inside(step)
            if far is not None:
                up = odd if step[1] > 0 else jnp.logical_not(odd)
                near = jnp.logical_and(near, up if far else jnp.logical_not(up))
            pl.when(near)(halo_copy(phase, step).start)

    def neighbours(axis):
        total = (me[axis] > 0).astype(jnp.int32) + (me[axis] < count[axis] - 1).astype(jnp.int32)
        return [(n, total == n) for n in ([count[axis] - 1] if count[axis] < 3 else [1, 2])]

    def halo_wait(phase):
        for (i, on_x), (j, on_y), (k, on_z) in itertools.product(*[neighbours(axis) for axis in AXES]):
            along = pl.ds(0, ex + i)
            if phase == 0:
                size, active, others = i, on_x, j == neighbours("gy")[0][0] and k == neighbours("gz")[0][0]
                ref = plain.at[1, pl.ds(0, i), body]
            elif phase == 1:
                size, active, others = k, jnp.logical_and(on_x, on_z), j == neighbours("gy")[0][0]
                ref = face_in.at[pl.ds(0, k), along]
            elif phase == 2:
                size, active, others = j, jnp.logical_and(on_x, on_y), k == neighbours("gz")[0][0]
                ref = shifted.at[1, along, pl.ds(0, j)]
            else:
                size, active, others = j * k, jnp.logical_and(on_x, jnp.logical_and(on_y, on_z)), True
                ref = edge_in.at[pl.ds(0, k), pl.ds(0, j), along]
            if size and others:
                @pl.when(active)
                def _(ref=ref):
                    departed(ref, halo_send.at[phase])
                    arrived(ref, halo_recv.at[phase])

    halo_start(2, True)
    halo_start(2, False)
    halo_start(0, None)
    halo_start(1, None)
    halo_start(3, True)
    halo_start(3, False)
    load_in.wait()
    for x in range(ex):
        in_t[:, x * ey * ez:(x + 1) * ey * ez] = in_ref[x].reshape(ey * ez, chan).T

    own = std_all.at[me["gx"], me["gy"]]
    spans = [pl.ds(low, high - low) for low, high in parts]

    def gather_y_start(n):
        mine = own.at[spans[n]]
        for k in range(1, ny):
            remote(mine, mine, ay_send.at[0], ay_recv.at[n], {"gy": peer("gy", k)}).start()

    def gather_x_start(n):
        arrived(std_all.at[0, pl.ds(0, ny - 1), spans[n]], ay_recv.at[n])
        mine = std_all.at[me["gx"], :, spans[n]]
        for k in range(1, nx):
            remote(mine, mine, ax_send.at[0], ax_recv.at[n], {"gx": peer("gx", k)}).start()

    def gather_wait(n):
        arrived(std_all.at[pl.ds(0, nx - 1), :, spans[n]], ax_recv.at[n])


    def view(t):
        a, b, c = t // 9, (t // 3) % 3, t % 3
        return plain[2 - c, 2 - a:2 - a + ex, 2 - b:2 - b + ey].reshape(ex * ey * ez, chan)

    def blocks():
        return [(gx, gy, (gx * ny + gy) * rows) for gx in range(nx) for gy in range(ny)]

    def interior(first, last):
        for u in range(first, last, 2):
            group = list(range(u, min(u + 2, last)))
            views = [view(order[v]) for v in group]
            right = jnp.concatenate(views, axis=1) if len(views) > 1 else views[0]
            product = jnp.dot(in_t[...], right, preferred_element_type=F32)
            for j, v in enumerate(group):
                for gx, gy, low in blocks():
                    value = product[low:low + rows, j * chan:(j + 1) * chan]
                    part[gx, gy, v] = value
                    if v < 3:
                        part_x[gx, gy, v] = value.astype(BF16)

    def correct(triple):
        b, c = (order[3 * triple] // 3) % 3, order[3 * triple] % 3
        left, right = [], [[] for a in range(3)]
        if b != 1:
            end = b // 2
            left.append(in_y[1 - end])
            for a in range(3):
                right[a].append(shifted[2 - c, 2 - a:2 - a + ex, (1 - end) * (ey + 1)].reshape(ex * ez, chan))
        if c != 1:
            end = c // 2
            left.append(in_z[1 - end])
            for a in range(3):
                face = face_in[1 - end, 2 - a:2 - a + ex] if b == 1 else face_turn[1 - end, b // 2, 2 - a:2 - a + ex]
                right[a].append(face.reshape(ex * ey, chan))
        left = jnp.concatenate(left, axis=1)
        right = jnp.concatenate([jnp.concatenate(strip, axis=0) for strip in right], axis=1)
        return jnp.dot(left, right, preferred_element_type=F32)

    def correct_all(triples):
        products = [correct(triple) for triple in triples]
        for triple, product in zip(triples, products):
            for a in range(3):
                for gx, gy, low in blocks():
                    value = part[gx, gy, 3 * triple + a] + product[low:low + rows, a * chan:(a + 1) * chan]
                    part[gx, gy, 3 * triple + a] = value
                    part_x[gx, gy, 3 * triple + a] = value.astype(BF16)

    def rows_send(g):
        base, first, many, size = groups[g]
        span = pl.ds(first, many)
        for k in range(1, nx):
            remote(part_x.at[peer("gx", k), :, span], recv_x.at[k - 1, :, span], x_send.at[0], x_recv.at[g],
                   {"gx": peer("gx", k)}).start()

    def rows_total(gy, span):
        total = part[me["gx"], gy, span]
        for k in range(1, nx):
            total = total + recv_x[k - 1, gy, span].astype(F32)
        return total

    def rows_chunk(g):
        base, first, many, size = groups[g]
        span = pl.ds(first, many)
        arrived(recv_x.at[:, :, span], x_recv.at[g])
        if g == depth_first:
            for gy in range(ny):
                send_a[gy, 0:many] = rows_total(gy, span).astype(BF16)
                for v in range(many, size * nz):
                    send_a[gy, v] = jnp.zeros((rows, chan), BF16)
            for k in range(1, nz):
                remote(send_a.at[:, pl.ds(peer("gz", k) * size, size)], recv_a.at[k - 1], y_send.at[1], y_recv.at[g],
                       {"gz": peer("gz", k)}).start()
            return
        for gy in range(ny):
            send_y[gy, span] = rows_total(gy, span).astype(BF16)
        for k in range(1, ny):
            remote(send_y.at[peer("gy", k), span], recv_y.at[k - 1, span], y_send.at[0], y_recv.at[g],
                   {"gy": peer("gy", k)}).start()

    def depth_middle():
        g = depth_first
        base, first, many, size = groups[g]
        arrived(recv_a, y_recv.at[g])
        mine = pl.ds(me["gz"] * size, size)
        for gy in range(ny):
            total = send_a[gy, mine].astype(F32)
            for k in range(1, nz):
                total = total + recv_a[k - 1, gy].astype(F32)
            own_b[gy] = total
            send_b[gy] = total.astype(BF16)
        for k in range(1, ny):
            remote(send_b.at[peer("gy", k)], recv_b.at[k - 1], z_send.at[1], z_recv.at[g], {"gy": peer("gy", k)}).start()

    def middle_sums():
        base, first, many, size = groups[depth_first]
        mine_std = pl.ds(first + me["gz"] * size, size)
        plain_sum, cross_sum = 0.0, 0.0
        for gy in range(ny):
            plain_sum = plain_sum + own_b[gy]
            cross_sum = cross_sum + own_b[gy] * std_all[me["gx"], gy, mine_std].astype(F32)
        return [per_output(plain_sum), per_output(cross_sum)]

    depth_index = lax.broadcasted_iota(jnp.int32, (ey, ez, chan), 1)
    edge_index = lax.broadcasted_iota(jnp.int32, (ex + 2, ez, chan), 1)
    row_index = lax.broadcasted_iota(jnp.int32, (ex + 2, ey, chan), 1)
    turns = [(2, 1, ez - 1, ez - 1), (0, 0, 1, 0)]

    def turn_plain(xs):
        for x in xs:
            value = plain[1, x, 1:ey + 1].astype(F32)
            for slot, side, amount, last in turns:
                plane = pltpu.roll(value, amount, 1)
                plain[slot, x, 1:ey + 1] = jnp.where(depth_index == last, 0.0, plane).astype(BF16)

    def turn_faces():
        for side in range(2):
            face = face_in[side].astype(F32)
            for n, amount, last in [(0, ey - 1, ey - 1), (1, 1, 0)]:
                face_turn[side, n] = jnp.where(row_index == last, 0.0, pltpu.roll(face, amount, 1)).astype(BF16)

    def shift_faces():
        for x in (0, ex + 1):
            shifted[1, x, 1:ey + 1] = plain[1, x, 1:ey + 1]
        for slot, side, amount, last in turns:
            for x in range(ex + 2):
                outer = face_in[side, x].astype(F32)[:, None, :]
                plane = plain[slot, x, 1:ey + 1].astype(F32)
                shifted[slot, x, 1:ey + 1] = jnp.where(depth_index == last, outer, plane).astype(BF16)

    def shift_edges():
        for slot, side, amount, last in turns:
            for end, y in [(0, 0), (1, ey + 1)]:
                plane = pltpu.roll(shifted[1, :, y].astype(F32), amount, 1)
                shifted[slot, :, y] = jnp.where(edge_index == last, edge_in[side, end], plane).astype(BF16)

    def depth_start(g):
        base, first, many, size = groups[g]
        span = pl.ds(first, many)
        arrived(recv_y.at[:, span], y_recv.at[g])
        total = rows_total(me["gy"], span)
        for k in range(1, ny):
            total = total + recv_y[k - 1, span].astype(F32)
        total_z[base:base + many] = total
        send_z[base:base + many] = total.astype(BF16)
        for k in range(1, nz):
            remote(send_z.at[pl.ds(base + peer("gz", k) * size, size)], recv_z.at[k - 1, pl.ds(base // nz, size)],
                   z_send.at[0], z_recv.at[g], {"gz": peer("gz", k)}).start()
        return [per_output(total), per_output(total * std[base:base + many])]

    def depth_sum(g):
        base, first, many, size = groups[g]
        mine = pl.ds(base + me["gz"] * size, size)
        if g == depth_first:
            arrived(recv_b, z_recv.at[g])
            grad = own_b[me["gy"]]
            for k in range(1, ny):
                grad = grad + recv_b[k - 1].astype(F32)
        else:
            arrived(recv_z.at[:, pl.ds(base // nz, size)], z_recv.at[g])
            grad = total_z[mine]
            for k in range(1, nz):
                grad = grad + recv_z[k - 1, pl.ds(base // nz, size)].astype(F32)
        full[mine] = grad.astype(BF16)
        return per_output(grad * grad)

    def gather_start(g):
        base, first, many, size = groups[g]
        mine = pl.ds(base + me["gz"] * size, size)
        for k in range(1, nz):
            remote(full.at[mine], full.at[mine], g_send.at[0], g_recv.at[0], {"gz": peer("gz", k)}).start()

    turn_plain(range(1, ex + 1))
    for end, y, z in [(0, 0, 0), (1, ey - 1, ez - 1)]:
        in_y[end] = in_ref[:, y].reshape(ex * ez, chan).T
        in_z[end] = jnp.concatenate([in_ref[x].astype(F32)[:, z, :] for x in range(ex)], axis=0).astype(BF16).T
    halo_wait(0)
    interior(0, 3)
    rows_send(0)
    turn_plain((0, ex + 1))
    interior(3, taps)
    rows_chunk(0)
    halo_wait(1)
    turn_faces()
    correct_all(range(1, 3))
    rows_send(1)
    arrived(stats_in, st_recv.at[0])
    sums = stats[0]
    for k in range(nx * ny - 1):
        sums = sums + stats_in[k]
    mean_out = sums[0] / fan_count
    var_out = sums[1] / fan_count - mean_out * mean_out
    inv_std = lax.rsqrt(var_out + var_eps)
    for u, t in enumerate(order):
        value = (raw_ref[t] - mean_out) * inv_std
        std[slots[u]] = value
        own[u] = value.astype(BF16)
    gather_y_start(0)
    halo_wait(2)
    correct_all(range(3, 5))
    halo_wait(3)
    shift_edges()
    correct_all(range(5, 9))
    for g in range(2, len(groups)):
        rows_send(g)
    for g in range(1, len(groups)):
        rows_chunk(g)
    gather_y_start(1)
    linear = [depth_start(0)]
    gather_x_start(0)
    load_more.wait()
    shift_faces()

    def dx_pass(n):
        low, high = parts[n]
        span = slice(low * reach * chan // 3, high * reach * chan // 3)
        for u in range(low, high):
            a = order[u] // 9
            for j in range(wide):
                at = (u // 3 * reach + j + 2 - a) * chan
                w_cat[j * chan:(j + 1) * chan, at:at + chan] = std_all[:, :, u].reshape(nx * ny * rows, chan)

        def dx_step(m, carry):
            start = m * planes
            left = []
            for x in range(0, planes, wide):
                strips = []
                for t in order[low:high:3]:
                    b, c = (t // 3) % 3, t % 3
                    for p in range(reach):
                        strips.append(shifted[2 - c, start + x + p, 2 - b:2 - b + ey].reshape(ey * ez, chan))
                left.append(jnp.concatenate(strips, axis=1))
            left = jnp.concatenate(left, axis=0)
            product = lax.dot_general(left, w_cat[:, span], (((1,), (1,)), ((), ())), preferred_element_type=F32)
            for x in range(0, planes, wide):
                for j in range(wide):
                    plane = product[x // wide * ey * ez:(x // wide + 1) * ey * ez, j * chan:(j + 1) * chan]
                    plane = plane.reshape(ey, ez, chan)
                    if n > 0:
                        plane = plane + dx_part[start + x + j]
                    if n == len(parts) - 1:
                        dx_ref[start + x + j] = plane.astype(BF16)
                    else:
                        dx_part[start + x + j] = plane
            return carry

        lax.fori_loop(0, ex // planes, dx_step, 0)

    for g in range(1, len(groups)):
        if g != depth_first:
            linear.append(depth_start(g))
    depth_middle()
    gather_y_start(2)
    gather_wait(0)
    dx_pass(0)
    late = [g for g in range(len(groups)) if g != depth_first]
    late.append(depth_first)
    flat = (me["gx"] * ny + me["gy"]) * nz + me["gz"]

    def everywhere(span, n):
        mine = total_in.at[flat, span]
        for dz in sorted(range(nz), key=lambda k: -min(k, nz - k)):
            for dx in range(nx):
                for dy in range(ny):
                    if dx or dy or dz:
                        where = {"gx": peer("gx", dx), "gy": peer("gy", dy), "gz": peer("gz", dz)}
                        remote(stats.at[1, span], mine, t_send.at[n], t_recv.at[n], where).start()

    squares = None
    for g in late:
        new = depth_sum(g)
        squares = new if squares is None else squares + new
        if g == 1:
            gather_x_start(1)
            linear.append(middle_sums())
            for n in range(2):
                stats[1, n] = sum(pair[n] for pair in linear)
            everywhere(pl.ds(0, 2), 0)
        if g != late[-1]:
            gather_start(g)
    stats[1, 2] = squares
    total_in[flat] = stats[1]
    everywhere(pl.ds(2, 1), 1)
    gather_start(late[-1])
    gather_x_start(2)
    gather_wait(1)
    dx_pass(1)
    gather_wait(2)
    dx_pass(2)
    departed(stats_in, st_send.at[0])
    departed(part_x.at[pl.ds(0, nx - 1)], x_send.at[0])
    base, first, many, size = groups[depth_first]
    departed(recv_a, y_send.at[1])
    departed(recv_b, z_send.at[1])
    departed(send_y.at[pl.ds(0, ny - 1), pl.ds(0, taps - many)], y_send.at[0])
    departed(recv_z.at[:, pl.ds(0, recv_z.shape[1] - size)], z_send.at[0])
    departed(recv_z, g_send.at[0])
    departed(std_all.at[0, pl.ds(0, ny - 1)], ay_send.at[0])
    departed(std_all.at[pl.ds(0, nx - 1)], ax_send.at[0])
    others = [total_in.at[pl.ds(0, nx * ny * nz - 1), pl.ds(0, 2)], total_in.at[pl.ds(0, nx * ny * nz - 1), pl.ds(2, 1)]]
    departed(others[0], t_send.at[0])
    departed(others[1], t_send.at[1])
    arrived(others[0], t_recv.at[0])
    sums = total_in[0, 0:2]
    for k in range(1, nx * ny * nz):
        sums = sums + total_in[k, 0:2]
    sum_grad, sum_cross = sums[0], sums[1]
    arrived(others[1], t_recv.at[1])
    sum_square = total_in[0, 2]
    for k in range(1, nx * ny * nz):
        sum_square = sum_square + total_in[k, 2]
    mean_grad = sum_grad / fan_count
    mean_cross = sum_cross / fan_count
    spread = sum_square - 2.0 * mean_grad * sum_grad - 2.0 * mean_cross * sum_cross
    spread = (
        spread
        + fan_count * mean_grad * mean_grad
        + fan_count * mean_cross * mean_cross * var_out / (var_out + var_eps)
    )
    square_sum = jnp.sum(inv_std * inv_std * spread, axis=1, keepdims=True)
    scale = jnp.minimum(1.0, clip_norm * lax.rsqrt(square_sum + norm_eps))
    coef_ref[0:1] = inv_std * scale
    coef_ref[1:2] = mean_grad
    coef_ref[2:3] = mean_cross
    arrived(recv_z, g_recv.at[0])


def finish_kernel(nz, dx_in, full, std, coef_ref, dx_hbm, wg_hbm, wg_ref, sem):
    for x in range(dx_in.shape[0]):
        pltpu.make_async_copy(dx_in.at[x], dx_hbm.at[x], sem.at[0]).start()
    factor, mean_grad, mean_cross = coef_ref[0:1], coef_ref[1:2], coef_ref[2:3]
    third = wg_ref.shape[0] // 3
    for t, slot in sorted(tap_slots(nz)):
        wg_ref[t] = factor * (full[slot].astype(F32) - mean_grad - std[slot] * mean_cross)
        if t % third == third - 1:
            span = pl.ds(t + 1 - third, third)
            pltpu.make_async_copy(wg_ref.at[span], wg_hbm.at[span], sem.at[1]).start()
    pltpu.make_async_copy(dx_in, dx_hbm, sem.at[0]).wait()
    pltpu.make_async_copy(wg_ref, wg_hbm, sem.at[1]).wait()


def on_device(dims, raw_weight, inputs, cotangent):
    nx, ny, nz = dims
    rows, taps, chan = raw_weight.shape
    ex, ey, ez = inputs.shape[:3]
    groups = z_groups(nz)
    wide = 2 if ex % 2 == 0 else 1
    many = len(groups)
    piece = sum(size for base, first, number, size in groups)
    padded_taps = piece * nz
    alone = groups[depth_first][3]
    stat_slots = nx * ny - 1
    dma = pltpu.SemaphoreType.DMA

    def pair(n, m):
        return [dma((n,)), dma((m,))]

    scratch = [
        pltpu.VMEM((taps, rows, chan), F32),
        pltpu.VMEM(inputs.shape, BF16),
        pltpu.VMEM((3, ex + 2, ey + 2, ez, chan), BF16),
        pltpu.VMEM((3, ex + 2, ey + 2, ez, chan), BF16),
        pltpu.VMEM((2, chan, ex * ez), BF16),
        pltpu.VMEM((2, chan, ex * ey), BF16),
        pltpu.VMEM((2, 2, ex + 2, ey, chan), BF16),
        pltpu.VMEM((ny, alone * nz, rows, chan), BF16),
        pltpu.VMEM((nz - 1, ny, alone, rows, chan), BF16),
        pltpu.VMEM((ny, alone, rows, chan), BF16),
        pltpu.VMEM((ny - 1, alone, rows, chan), BF16),
        pltpu.VMEM((ny, alone, rows, chan), F32),
        pltpu.VMEM((2, ex, ey, chan), BF16),
        pltpu.VMEM((2, ex + 2, ey, chan), BF16),
        pltpu.VMEM((2, 2, ex, 1, chan), F32),
        pltpu.VMEM((2, 2, ex + 2, 1, chan), F32),
        pltpu.VMEM((chan, ex * ey * ez), BF16),
        pltpu.VMEM((nx, ny, taps, rows, chan), F32),
        pltpu.VMEM((nx, ny, taps, rows, chan), BF16),
        pltpu.VMEM((nx - 1, ny, taps, rows, chan), BF16),
        pltpu.VMEM((ny, taps, rows, chan), BF16),
        pltpu.VMEM((ny - 1, taps, rows, chan), BF16),
        pltpu.VMEM((padded_taps, rows, chan), BF16),
        pltpu.VMEM((padded_taps, rows, chan), F32),
        pltpu.VMEM((nz - 1, piece, rows, chan), BF16),
        pltpu.VMEM((nx, ny, taps, rows, chan), BF16),
        pltpu.VMEM((wide * chan, taps // 3 * (wide + 2) * chan), BF16),
        pltpu.VMEM((ex, ey, ez, chan), F32),
        pltpu.VMEM((2, 3, 1, chan), F32),
        pltpu.VMEM((stat_slots, 3, 1, chan), F32),
        pltpu.VMEM((nx * ny * nz, 3, 1, chan), F32),
        dma((4,)), *pair(4, 4), *pair(1, many), *pair(2, many), *pair(2, many), *pair(1, 1), *pair(1, 3), *pair(1, 3),
        *pair(1, 1), *pair(2, 2),
    ]
    vmem = pl.BlockSpec(memory_space=pltpu.VMEM)
    anywhere = pl.BlockSpec(memory_space=pl.ANY)
    operands = (jnp.transpose(raw_weight, (1, 0, 2)), inputs, cotangent)
    dx, full, std, coef = pl.pallas_call(
        functools.partial(kernel, dims),
        out_shape=(
            pltpu.VMEM(cotangent.shape, BF16),
            pltpu.VMEM((padded_taps, rows, chan), BF16),
            pltpu.VMEM((padded_taps, rows, chan), F32),
            pltpu.VMEM((8, chan), F32),
        ),
        in_specs=[anywhere] * 3,
        out_specs=(vmem,) * 4,
        scratch_shapes=scratch,
        compiler_params=pltpu.CompilerParams(
            collective_id=0, has_side_effects=True, vmem_limit_bytes=40 * 1024 * 1024
        ),
    )(*[pltpu.with_memory_space_constraint(v, pltpu.HBM) for v in operands])
    input_grad, weight_grad = pl.pallas_call(
        functools.partial(finish_kernel, nz),
        out_shape=(
            jax.ShapeDtypeStruct(cotangent.shape, BF16),
            jax.ShapeDtypeStruct((taps, rows, chan), F32),
        ),
        in_specs=[vmem] * 4,
        out_specs=(anywhere,) * 2,
        scratch_shapes=[pltpu.VMEM((taps, rows, chan), F32), dma((2,))],
        compiler_params=pltpu.CompilerParams(vmem_limit_bytes=8 * 1024 * 1024),
    )(dx, full, std, coef)
    return input_grad, jnp.transpose(weight_grad, (1, 0, 2))


def solution(mesh):
    dims = tuple(mesh.shape[axis] for axis in AXES)
    in_specs = (P(("gx", "gy"), None, None), P("gx", "gy", "gz", None), P("gx", "gy", "gz", None))
    out_specs = (P("gx", "gy", "gz", None), P(("gx", "gy"), None, None))
    return jax.shard_map(
        functools.partial(on_device, dims), mesh=mesh, in_specs=in_specs, out_specs=out_specs, check_vma=False
    )
```
